32 devices in a mesh: grp: 8 (over z, y), col: 4 (over x, core).
Axes of the slice: x: 2, y: 2, z: 4, core: 2. Of those that a mesh axis runs over, the one named last changes fastest.
Arguments:
- features: bfloat16 [65536, 256], P(('grp', 'col')), may hold values from -6 to 6
- adj_tiles: bfloat16 [1536, 256, 256], P('grp'), may hold values from 0 to 1.5
- block_pairs: int32 [8, 192, 2], P('grp'), may hold values from 0 to 31, as said below
- tile_count: int32 [8], P('grp'), may hold values from 32 to 192, as said below
- degree: int32 [65536], P('grp'), may hold values from 1 to 769
- labels: int32 [65536], P(('grp', 'col')), may hold values from 0 to 63
- loss_mask: int32 [65536], P(('grp', 'col')), may hold values from 0 to 1
- slot_piece: int32 [8, 79], replicated, may hold values from -1 to 416, as said below
- master: float32 [632, 2, 256], P('grp', None, 'col'), may hold values from -4 to 4
- moment_one: float32 [632, 2, 256], P('grp', None, 'col'), may hold values from -0.125 to 0.125
- moment_two: float32 [632, 2, 256], P('grp', None, 'col'), may hold values from 3.0517579e-06 to 0.00030517578
Outputs:
- mean_loss: float32 [], replicated
- new_master: float32 [632, 2, 256], P('grp', None, 'col')
- new_moment_one: float32 [632, 2, 256], P('grp', None, 'col')
- new_moment_two: float32 [632, 2, 256], P('grp', None, 'col')
- new_weights: bfloat16 [632, 2, 256], P('grp', None, 'col')
The draws below stay inside these ranges and needn't reach their ends.
Inputs may be any that keep to these rules, and one draw needn't show every extreme that they name: `block_pairs`: of each group, the first tile_count entries are distinct pairs of blocks and include every diagonal pair (r, r); later entries are padding. `tile_count`: some group has 192 live tiles in every draw. `slot_piece`: each piece 0 to 416 sits in exactly one slot; a group holds at most 79 pieces, and some group holds 79 in every draw.
All inputs are finite; a program needn't handle non-finite values.
Results may differ from the reference program's by a relative error of at most 0.0079.
Values may be sent and summed in bfloat16 or wider, within the bound.
A program may use at most 128 MiB of HBM per device.

```python
import math
import jax
import jax.numpy as jnp
from jax import lax

F = 256
HID = 256
CLS = 64
B = 256
PR = 2
STEP = 7
NG = 8192
GROUPS = 8
NODES = 65536
R = 32
MAXT = 192
PROWS = 834
PIECES = 417
SLOTS = 79


community_count = 8


def community(key):
    return jax.random.randint(jax.random.fold_in(key, 41), (NODES,), 0, community_count).astype(jnp.int32)


def pair_table(key):
    base_key = jax.random.fold_in(key, 11)
    key_full, key_count, key_pick, key_order = jax.random.split(base_key, 4)
    heavy_group = jax.random.randint(key_full, (), 0, GROUPS)
    least_count = max(R, (MAXT + 1) // 2)
    counts = jax.random.randint(key_count, (GROUPS,), least_count, MAXT + 1)
    counts = jnp.where(jnp.arange(GROUPS) == heavy_group, MAXT, counts).astype(jnp.int32)
    extra_tiles = MAXT - R
    choose = jax.vmap(lambda sub_key: jax.random.permutation(sub_key, R * R - R)[:extra_tiles])(jax.random.split(key_pick, GROUPS)).astype(jnp.int32)
    first_block = choose // (R - 1)
    other_block = choose % (R - 1)
    second = other_block + (other_block >= first_block).astype(jnp.int32)
    diagonal = jnp.broadcast_to(jnp.arange(R, dtype=jnp.int32), (GROUPS, R))
    row_ids = jnp.concatenate([diagonal, first_block], axis=1)
    col_ids = jnp.concatenate([diagonal, second], axis=1)
    places = jnp.arange(MAXT, dtype=jnp.int32)
    shuffle = jax.vmap(lambda sub_key: jax.random.permutation(sub_key, MAXT))(jax.random.split(key_order, GROUPS)).astype(jnp.int32)
    live_slot = places[None, :] < counts[:, None]
    sort_key = jnp.where(live_slot, shuffle, MAXT + places[None, :])
    ordering = jnp.argsort(sort_key, axis=1)
    row_ids = jnp.where(live_slot, jnp.take_along_axis(row_ids, ordering, axis=1), 0)
    col_ids = jnp.where(live_slot, jnp.take_along_axis(col_ids, ordering, axis=1), 0)
    return (jnp.stack([row_ids, col_ids], axis=-1).astype(jnp.int32), counts)


def draw_block_pairs(key, part):
    return pair_table(key)[0]


def draw_tile_count(key, part):
    return pair_table(key)[1]


def draw_degree(key, part):
    pairs, counts = pair_table(key)
    live_slot = jnp.arange(MAXT, dtype=jnp.int32)[None, :] < counts[:, None]
    row_match = (pairs[:, :, 0][:, None, :] == jnp.arange(R, dtype=jnp.int32)[None, :, None]) & live_slot[:, None, :]
    row_hits = jnp.sum(row_match.astype(jnp.int32), axis=2)
    per_node = jnp.repeat(row_hits, B, axis=1).reshape(NODES)
    lowest = jnp.maximum(1, per_node * B // 32)
    highest = per_node * 3 * B // 32 + 2
    values = jax.random.randint(jax.random.fold_in(key, 13), (NODES,), lowest, highest).astype(jnp.int32)
    return values.at[0].set(3 * R * B // 32 + 1).astype(jnp.int32)


def draw_features(key, part):
    groups_of = community(key)
    key_noise, key_direction = jax.random.split(jax.random.fold_in(key, 43))
    noise = jnp.clip(jax.random.normal(key_noise, (NODES, F), jnp.float32), -4.0, 4.0)
    direction = jnp.clip(jax.random.normal(key_direction, (community_count, F), jnp.float32), -4.0, 4.0)
    return (0.8 * noise + 0.6 * direction[groups_of]).astype(jnp.bfloat16)


def draw_labels(key, part):
    groups_of = community(key)
    key_within, key_ticket, key_other = jax.random.split(jax.random.fold_in(key, 47), 3)
    share = CLS // community_count
    within = jax.random.randint(key_within, (NODES,), 0, share)
    ticket = jax.random.randint(key_ticket, (NODES,), 0, 10)
    other = jax.random.randint(key_other, (NODES,), 0, CLS)
    return jnp.where(ticket < 8, groups_of * share + within, other).astype(jnp.int32)


def draw_adj_tiles(key, part):
    pairs, counts = pair_table(key)
    groups_of = community(key).reshape(GROUPS, R, B)
    row_group = jax.vmap(lambda table, index: table[index])(groups_of, pairs[:, :, 0])
    col_group = jax.vmap(lambda table, index: table[index])(groups_of, pairs[:, :, 1])
    same_group = row_group[:, :, :, None] == col_group[:, :, None, :]
    same_chance = min(0.9, 11.0 * community_count / B)
    other_chance = min(0.05, 2.5 / B)
    chance = jnp.where(same_group, same_chance, other_chance)
    key_edge, key_weight = jax.random.split(jax.random.fold_in(key, 17))
    tile_shape = (GROUPS, MAXT, B, B)
    present = jax.random.uniform(key_edge, tile_shape, jnp.float32) < chance
    weight = jax.random.uniform(key_weight, tile_shape, jnp.float32, 0.5, 1.5)
    return jnp.where(present, weight, 0.0).reshape(GROUPS * MAXT, B, B).astype(jnp.bfloat16)


def draw_loss_mask(key, part):
    node_index = jnp.arange(NODES, dtype=jnp.int32)
    ticket = jax.random.randint(jax.random.fold_in(key, 19), (NODES,), 0, 4 * NODES)
    return (ticket < NODES + 3 * node_index + 3).astype(jnp.int32)


def slot_table(key):
    base_key = jax.random.fold_in(key, 23)
    key_full, key_piece, key_rank = jax.random.split(base_key, 3)
    slot_total = GROUPS * SLOTS
    full_group = jax.random.randint(key_full, (), 0, GROUPS)
    pieces = jax.random.permutation(key_piece, PIECES).astype(jnp.int32)
    places = jnp.arange(slot_total, dtype=jnp.int32)
    layout = jnp.full((slot_total,), -1, jnp.int32)
    layout = layout.at[full_group * SLOTS + jnp.arange(SLOTS, dtype=jnp.int32)].set(pieces[:SLOTS])
    random_rank = jax.random.permutation(key_rank, slot_total).astype(jnp.int32)
    sort_key = jnp.where(places // SLOTS == full_group, slot_total + places, random_rank)
    ordering = jnp.argsort(sort_key)
    layout = layout.at[ordering[:PIECES - SLOTS]].set(pieces[SLOTS:])
    return layout


def draw_slot_piece(key, part):
    return slot_table(key).reshape(GROUPS, SLOTS)


def draw_master(key, part):
    layout = slot_table(key)
    table_rows = jnp.maximum(layout, 0)[:, None, None] * PR + jnp.arange(PR, dtype=jnp.int32)[None, :, None]
    row_scale = jnp.where(table_rows < F, 1.0 / F ** 0.5, jnp.where(table_rows < F + 2 * HID, 0.7 / HID ** 0.5, jnp.where(table_rows < F + 2 * HID + CLS, 4.5 / HID ** 0.5, 0.5)))
    value_shape = (GROUPS * SLOTS, PR, HID)
    draw_key = jax.random.fold_in(key, 31)
    unit_draw = jnp.clip(jax.random.normal(draw_key, value_shape, jnp.float32), -4.0, 4.0)
    return (unit_draw * row_scale).astype(jnp.float32)


def levels(key, dims, cuts, least, top_value):
    def one(dim, blocks):
        steps = jax.random.uniform(jax.random.fold_in(jax.random.fold_in(key, 6), dim), (blocks,), jnp.float32, least / len(cuts), top_value / len(cuts))
        return jnp.repeat(jnp.exp(steps), dims[dim] // blocks).reshape((-1,) + (1,) * (len(dims) - dim - 1))

    factor_of = one(*cuts[0])
    for cut in cuts[1:]:
        factor_of = factor_of * one(*cut)
    return factor_of


def scatter_about(stream_key, shape, scale, reach, cuts=(), kind=jnp.bfloat16):
    values = jax.random.normal(stream_key, shape, jnp.float32) * scale
    if len(cuts) > 0:
        values = levels(stream_key, shape, cuts, -0.22, 0.18) * values
    return jnp.clip(values, min=-reach, max=reach).astype(kind)


def setup_inputs(seed: int = 0) -> dict:
    streams_of = jax.random.split(jax.random.key(seed), 12)
    features = draw_features(jax.random.fold_in(streams_of[11], 71), 0)
    adj_tiles = draw_adj_tiles(jax.random.fold_in(streams_of[11], 71), 0)
    block_pairs = draw_block_pairs(jax.random.fold_in(streams_of[11], 71), 0)
    tile_count = draw_tile_count(jax.random.fold_in(streams_of[11], 71), 0)
    degree = draw_degree(jax.random.fold_in(streams_of[11], 71), 0)
    labels = draw_labels(jax.random.fold_in(streams_of[11], 71), 0)
    loss_mask = draw_loss_mask(jax.random.fold_in(streams_of[11], 71), 0)
    slot_piece = draw_slot_piece(jax.random.fold_in(streams_of[11], 71), 0)
    master = draw_master(jax.random.fold_in(streams_of[11], 71), 0)
    moment_one = scatter_about(streams_of[9], (GROUPS * SLOTS, PR, HID), (2.0 / NODES ** 0.5), 0.125, ((0, 8), (2, 4)), jnp.float32)
    moment_two = jnp.clip(jnp.exp(math.log(0.00030517578) - 4.6051702 * jax.random.uniform(streams_of[10], (GROUPS * SLOTS, PR, HID), jnp.float32) ** levels(streams_of[10], (GROUPS * SLOTS, PR, HID), ((0, 8), (2, 4)), -0.2, 0.2)), 3.051757857974735e-06, 0.00030517578)
    return {"features": features, "adj_tiles": adj_tiles, "block_pairs": block_pairs, "tile_count": tile_count, "degree": degree, "labels": labels, "loss_mask": loss_mask, "slot_piece": slot_piece, "master": master, "moment_one": moment_one, "moment_two": moment_two}


@jax.custom_vjp
def low(v):
    return lax.optimization_barrier(v.astype(jnp.bfloat16)).astype(jnp.float32)

@jax.custom_vjp
def low_back(v):
    return v

def low_keep(v):
    return (low(v), None)

def low_pass(kept, grad):
    return (grad,)

def back_keep(v):
    return (v, None)

def back_low(kept, grad):
    return (low(grad),)
low.defvjp(low_keep, low_pass)
low_back.defvjp(back_keep, back_low)
learn_rate = 0.01
beta_one = 0.5
beta_two = 0.5
adam_epsilon = 1e-08
decay_rate = 0.1

def silu_value(value):
    return value * jax.nn.sigmoid(value)

def table_from_slots(slot_values, slot_piece):
    flat_slots = slot_piece.reshape(-1)
    positions = jnp.arange(flat_slots.shape[0], dtype=jnp.int32)
    target = jnp.where(flat_slots >= 0, flat_slots, PIECES).astype(jnp.int32)
    piece_slot = jnp.zeros((PIECES + 1,), jnp.int32).at[target].set(positions)[:PIECES]
    return slot_values[piece_slot].reshape(PROWS, HID)

def aggregate(encoded, tiles, pairs, counts):

    def one_group(packed):
        group_rows, group_tiles, group_pairs, group_count = packed
        blocks = group_rows.reshape(R, B, HID)
        picked = blocks[group_pairs[:, 1]]
        products = jnp.einsum('tij,tjc->tic', group_tiles, picked, precision=lax.Precision.HIGHEST)
        live_tiles = jnp.arange(MAXT, dtype=jnp.int32) < group_count
        places = (group_pairs[:, 0][None, :] == jnp.arange(R, dtype=jnp.int32)[:, None]) & live_tiles[None, :]
        summed = jnp.einsum('rt,tic->ric', places.astype(jnp.float32), products, precision=lax.Precision.HIGHEST)
        return summed.reshape(NG, HID)
    packed_all = (encoded.reshape(GROUPS, NG, HID), tiles.reshape(GROUPS, MAXT, B, B), pairs, counts)
    return lax.map(jax.checkpoint(one_group), packed_all).reshape(NODES, HID)

def forward(weight_table, features, tiles, pairs, counts, degree, labels, mask_values):
    weights = low(weight_table)
    encoder_weight = weights[:F]
    self_weight = weights[F:F + HID]
    neigh_weight = weights[F + HID:F + 2 * HID]
    head_weight = weights[F + 2 * HID:F + 2 * HID + CLS]
    encoder_bias = weights[PROWS - 2]
    sage_bias = weights[PROWS - 1]
    preact = low_back(jnp.dot(features, encoder_weight, precision=lax.Precision.HIGHEST) + encoder_bias)
    encoded = low(silu_value(preact))
    block_sum = low_back(aggregate(encoded, tiles, pairs, counts))
    neigh_mean = low(block_sum / degree[:, None])
    sage_pre = low_back(jnp.dot(encoded, self_weight, precision=lax.Precision.HIGHEST) + jnp.dot(neigh_mean, neigh_weight, precision=lax.Precision.HIGHEST) + sage_bias)
    hidden = low(silu_value(sage_pre))
    logits = low_back(jnp.dot(hidden, head_weight.T, precision=lax.Precision.HIGHEST))
    row_max = lax.optimization_barrier(jnp.max(logits, axis=1, keepdims=True))
    log_total = row_max[:, 0] + jnp.log(lax.optimization_barrier(jnp.sum(jnp.exp(logits - row_max), axis=1)))
    target_logit = jnp.take_along_axis(logits, labels[:, None], axis=1)[:, 0]
    count = jnp.sum(mask_values)
    return jnp.sum(mask_values * (log_total - target_logit)) / count

def reference(features, adj_tiles, block_pairs, tile_count, degree, labels, loss_mask, slot_piece, master, moment_one, moment_two):
    weight_table = table_from_slots(master, slot_piece)
    feature_values = features.astype(jnp.float32)
    tile_values = adj_tiles.astype(jnp.float32)
    degree_values = degree.astype(jnp.float32)
    mask_values = loss_mask.astype(jnp.float32)

    def loss_of(table_values):
        return forward(table_values, feature_values, tile_values, block_pairs, tile_count, degree_values, labels, mask_values)
    mean_loss, pullback = jax.vjp(loss_of, weight_table)
    grad_table = pullback(jnp.ones_like(mean_loss))[0]
    flat_slots = slot_piece.reshape(-1)
    is_owned = flat_slots >= 0
    safe_pieces = jnp.where(is_owned, flat_slots, 0).astype(jnp.int32)
    owned_values = is_owned[:, None, None]
    slot_grad = grad_table.reshape(PIECES, PR, HID)[safe_pieces]
    slot_grad = jnp.where(owned_values, slot_grad, 0.0)
    table_rows = safe_pieces[:, None] * PR + jnp.arange(PR, dtype=jnp.int32)[None, :]
    decay_values = jnp.where(table_rows < PROWS - 2, decay_rate, 0.0)[:, :, None]
    first_moment = beta_one * moment_one + (1.0 - beta_one) * slot_grad
    second_moment = beta_two * moment_two + (1.0 - beta_two) * slot_grad * slot_grad
    first_hat = first_moment / (1.0 - beta_one ** STEP)
    second_hat = second_moment / (1.0 - beta_two ** STEP)
    updated = master - learn_rate * (first_hat / (jnp.sqrt(second_hat) + adam_epsilon) + decay_values * master)
    updated = jnp.where(owned_values, updated, 0.0)
    first_moment = jnp.where(owned_values, first_moment, 0.0)
    second_moment = jnp.where(owned_values, second_moment, 0.0)
    return (mean_loss, updated, first_moment, second_moment, updated.astype(jnp.bfloat16))
```

```python
import functools
import jax
import jax.numpy as jnp
from jax import lax
from jax.experimental import pallas as pl
from jax.experimental.pallas import tpu as pltpu
from jax.sharding import PartitionSpec as P

F = 256
HID = 256
CLS = 64
B = 256
PR = 2
STEP = 7
PROWS = 834
TROWS = 848
HALF = 128
UNROLL = 8

learn_rate = 0.01
beta_one = 0.5
beta_two = 0.5
adam_epsilon = 1e-08
decay_rate = 0.1

f32 = jnp.float32
bf16 = jnp.bfloat16
MESH = pl.DeviceIdType.MESH
VM = pl.BlockSpec(memory_space=pltpu.VMEM)
SM = pl.BlockSpec(memory_space=pltpu.SMEM)
ANY = pl.BlockSpec(memory_space=pl.ANY)


def sds(shape, dtype):
    return jax.ShapeDtypeStruct(shape, dtype)


def dot_nn(a, b):
    return lax.dot_general(a, b, (((1,), (0,)), ((), ())), preferred_element_type=f32)


def dot_nt(a, b):
    return lax.dot_general(a, b, (((1,), (1,)), ((), ())), preferred_element_type=f32)


def dot_tn(a, b):
    return lax.dot_general(a, b, (((0,), (0,)), ((), ())), preferred_element_type=f32)


def column_of(rows16, row):
    pick = (lax.broadcasted_iota(jnp.int32, (16, HALF), 0) == row).astype(bf16)
    return dot_tn(rows16, pick)


def place():
    g = lax.axis_index("grp")
    q = lax.axis_index("col")
    k = q % 2
    x = q // 2
    partner = q + 1 - 2 * k
    across = q + 2 - 4 * x
    return g, q, k, x, partner, across


def sigmoid(v):
    return jax.nn.sigmoid(v)


def gather_kernel(
    ng,
    feat,
    wmsg,
    srow,
    labels,
    mask,
    pairs,
    tcount,
    fbuf,
    enc,
    table,
    wtrans,
    hot,
    marks,
    lists,
    pmsg,
    wbuf,
    prow,
    local_sem,
    core_sem,
    mark_sem,
    ws_core,
    ws_x,
    ws_send,
    ws_recv,
    wr_send,
    wr_recv,
    xs_send,
    xs_recv,
    rl_send,
    rl_recv,
):
    g, q, k, x, partner, across = place()
    rows = feat.shape[0]
    chunks = rows // B
    blocks = chunks
    sp = wmsg.shape[1]
    tiles = pairs.shape[1]
    tpad = lists.shape[1]

    load = pltpu.make_async_copy(feat, fbuf.at[q], local_sem)
    load.start()
    marks[x] = jnp.where(mask[...] > 0, labels[...], -1)

    barrier = pltpu.get_barrier_semaphore()
    pl.semaphore_signal(barrier, inc=1, device_id=(g, partner), device_id_type=MESH)
    pl.semaphore_signal(barrier, inc=1, device_id=(g, across), device_id_type=MESH)

    def greet(d, c):
        pl.semaphore_signal(barrier, inc=1, device_id=((g + d) % ng, q), device_id_type=MESH)
        return c

    lax.fori_loop(1, ng, greet, 0)
    pl.semaphore_wait(barrier, ng + 1)

    def remote(src, dst, send, recv, dev):
        return pltpu.make_async_remote_copy(
            src_ref=src, dst_ref=dst, send_sem=send, recv_sem=recv, device_id=dev, device_id_type=MESH
        )

    first = remote(wmsg, pmsg, ws_core.at[0], ws_core.at[1], (g, partner))
    first.start()
    mark_copy = remote(marks.at[x], marks.at[x], mark_sem.at[0], mark_sem.at[1], (g, across))
    mark_copy.start()
    load.wait()

    def cross(i):
        piece = fbuf.at[q, pl.ds(pl.multiple_of(i * B, B), B)]
        return remote(piece, piece, xs_send.at[i], xs_recv.at[i], (g, across))

    cross(0).start()
    share = remote(fbuf.at[q], fbuf.at[q], core_sem.at[0], core_sem.at[1], (g, partner))
    share.start()

    first.wait()
    wbuf[k, g, x] = wmsg[k] + pmsg[k]
    second = remote(wbuf.at[k, g, x], wbuf.at[k, g, x], ws_x.at[0], ws_x.at[1], (g, across))
    second.start()

    def cross_all(i, c):
        cross(i).start()
        return c

    lax.fori_loop(1, chunks, cross_all, 0)
    second.wait()

    def to_group(d):
        return remote(
            wbuf.at[k, g], wbuf.at[k, g], ws_send.at[d], ws_recv.at[d], ((g + d) % ng, q)
        )

    def from_group(d):
        src = (g + ng - d) % ng
        return remote(wbuf.at[k, src], wbuf.at[k, src], ws_send.at[d], ws_recv.at[d], (src, q))

    def hand_over(d):
        src = (g + ng - d) % ng
        return remote(
            wbuf.at[k, src], wbuf.at[k, src], wr_send.at[d], wr_recv.at[d], (g, partner)
        )

    def handed(d):
        src = (g + ng - d) % ng
        return remote(
            wbuf.at[1 - k, src], wbuf.at[1 - k, src], wr_send.at[d], wr_recv.at[d], (g, partner)
        )

    def send_group(d, c):
        to_group(d).start()
        return c

    lax.fori_loop(1, ng, send_group, 0)
    hand_over(0).start()

    shift = blocks.bit_length() - 1
    prow[...] = jnp.zeros_like(prow)
    pick = (
        lax.broadcasted_iota(jnp.int32, (8, 2), 0) == lax.broadcasted_iota(jnp.int32, (8, 2), 1)
    ).astype(bf16)
    prow[:, :tiles] = dot_nt(pick, pairs[0].astype(f32).astype(bf16))
    rvec = prow[0:1, :].astype(jnp.int32)
    cvec = prow[1:2, :].astype(jnp.int32)
    tvec = lax.broadcasted_iota(jnp.int32, (1, tpad), 1)
    live = tvec < tcount[0]

    def split(v):
        quarter = lax.shift_right_logical(v, shift)
        local = lax.shift_right_logical(quarter, 1) * blocks + (v & (blocks - 1))
        return (quarter & 1) == k, local

    fmine, frow = split(rvec)
    bmine, bcol = split(cvec)
    fmine = fmine & live
    bmine = bmine & live
    upto = (
        lax.broadcasted_iota(jnp.int32, (tpad, tpad), 0)
        <= lax.broadcasted_iota(jnp.int32, (tpad, tpad), 1)
    ).astype(bf16)
    order = lax.broadcasted_iota(jnp.int32, (tpad, tpad), 0)
    zero = jnp.zeros((1, tpad), jnp.int32)

    def compact(mine, one, two):
        flag = mine.astype(f32)
        seen = dot_nn(jnp.broadcast_to(flag, (8, tpad)).astype(bf16), upto)[0:1].astype(jnp.int32)
        spot = jnp.where(mine, seen - 1, -1)
        chosen = (order == spot).astype(f32).astype(bf16)
        values = jnp.concatenate([tvec, one, two, zero, zero, zero, zero, zero], axis=0)
        packed = dot_nt(values.astype(f32).astype(bf16), chosen).astype(jnp.int32)
        total = jnp.sum(flag, axis=1, keepdims=True).astype(jnp.int32)
        past = tvec >= total
        return packed[0:1], jnp.where(past, 2 * blocks, packed[1:2]), packed[2:3], zero + total

    ft, fr, fc, fn = compact(fmine, frow, cvec)
    bt, bc, br, bn = compact(bmine, bcol, rvec)
    lists[...] = jnp.concatenate([ft, fr, fc, bt, bc, br, fn, bn], axis=0)

    hot[...] = (
        (lax.broadcasted_iota(jnp.int32, hot.shape, 0) == srow[...]).astype(f32).astype(bf16)
    )

    def pass_on(d, c):
        from_group(d).wait_recv()
        hand_over(d).start()
        return c

    lax.fori_loop(1, ng, pass_on, 0)

    def take(d, c):
        handed(d).wait_recv()
        return c

    lax.fori_loop(0, ng, take, 0)

    left = wbuf[:, :, 0].reshape(2 * ng * sp, HALF)
    right = wbuf[:, :, 1].reshape(2 * ng * sp, HALF)
    full = dot_nn(hot[...], jnp.concatenate([left, right], axis=1))
    table[...] = full.astype(bf16)
    for i in range(3):
        wtrans[i] = jnp.transpose(full[i * B : (i + 1) * B]).astype(bf16)
    bias = column_of(table[PROWS - 2 : PROWS + 14], 0)
    bias = jnp.concatenate([bias, bias], axis=1)

    def encode(quarter, i):
        piece = fbuf[quarter, pl.ds(pl.multiple_of(i * B, B), B)]
        pre = dot_nt(wtrans[0], piece) + bias
        enc[quarter * blocks + i] = (pre * sigmoid(pre)).astype(bf16)

    def own(i, c):
        encode(q, i)
        return c

    lax.fori_loop(0, blocks, own, 0)
    share.wait_recv()

    def near(i, c):
        encode(partner, i)
        return c

    lax.fori_loop(0, blocks, near, 0)
    mine_far = across
    near_far = partner + 2 - 4 * x

    def crossed(i):
        piece = fbuf.at[mine_far, pl.ds(pl.multiple_of(i * B, B), B)]
        return remote(piece, piece, xs_send.at[i], xs_recv.at[i], (g, across))

    def relay(i):
        piece = fbuf.at[mine_far, pl.ds(pl.multiple_of(i * B, B), B)]
        return remote(piece, piece, rl_send.at[i], rl_recv.at[i], (g, partner))

    def relayed(i):
        piece = fbuf.at[near_far, pl.ds(pl.multiple_of(i * B, B), B)]
        return remote(piece, piece, rl_send.at[i], rl_recv.at[i], (g, partner))

    def far(i, c):
        crossed(i).wait_recv()
        relay(i).start()
        encode(mine_far, i)

        @pl.when(i > 0)
        def _():
            relayed(i - 1).wait_recv()
            encode(near_far, i - 1)

        return c

    lax.fori_loop(0, chunks, far, 0)
    relayed(chunks - 1).wait_recv()
    encode(near_far, chunks - 1)

    mark_copy.wait()
    share.wait_send()

    def drain(i, c):
        cross(i).wait_send()
        relay(i).wait_send()
        return c

    lax.fori_loop(0, chunks, drain, 0)

    def drain_group(d, c):
        to_group(d).wait_send()
        hand_over(d).wait_send()
        return c

    lax.fori_loop(1, ng, drain_group, 0)
    hand_over(0).wait_send()


def forward_kernel(lists, tiles, enc, degree, mean, acc):
    k = lax.axis_index("col") % 2
    local = mean.shape[0]
    blocks = local // 2

    def clear(i, c):
        acc[i] = jnp.zeros((B, B), f32)
        return c

    lax.fori_loop(0, local + 1, clear, 0)
    count = lists[6, 0]

    def step(i, c):
        for u in range(UNROLL):
            j = i * UNROLL + u
            r = lists[1, j]
            acc[r] += dot_nt(enc[lists[2, j]], tiles[lists[0, j]])
        return c

    lax.fori_loop(0, (count + UNROLL - 1) // UNROLL, step, 0)

    def finish(i, c):
        scale = 1.0 / degree[(i // blocks) * 2 + k, :, pl.ds(pl.multiple_of((i % blocks) * B, B), B)].astype(f32)
        mean[i] = (acc[i] * scale).astype(bf16)
        return c

    lax.fori_loop(0, local, finish, 0)


def sage_kernel(
    enc,
    mean,
    table,
    wtrans,
    marks,
    degree,
    sums,
    self_back,
    self_grad,
    neigh_grad,
    head_grad,
    bias_grad,
    stats,
    sage,
    hid,
    lgrad,
    send,
    recv,
):
    g, q, k, x, partner, across = place()
    local = mean.shape[0]
    blocks = local // 2
    width = 2 * B
    steps = local // 2
    barrier = pltpu.get_barrier_semaphore()
    pl.semaphore_signal(barrier, inc=1, device_id=(g, partner), device_id_type=MESH)
    pl.semaphore_wait(barrier, 1)
    half = pl.ds(pl.multiple_of(x * HALF, HALF), HALF)
    head = table[F + 2 * HID : F + 2 * HID + CLS]
    bias = column_of(table[PROWS - 2 : PROWS + 14], 1)
    bias = jnp.concatenate([bias] * 4, axis=1)
    neigh_half = table[pl.ds(pl.multiple_of(F + HID + x * HALF, HALF), HALF)]
    self_half = table[pl.ds(pl.multiple_of(F + x * HALF, HALF), HALF)]
    stats[...] = jnp.zeros_like(stats)

    def slot(i, core):
        return (i // (steps // 2)) * 2 * blocks + core * blocks + (i % (steps // 2)) * 2

    def exchange(i, core):
        piece = sums.at[pl.ds(slot(i, core), 2)]
        return pltpu.make_async_remote_copy(
            src_ref=piece,
            dst_ref=piece,
            send_sem=send.at[i],
            recv_sem=recv.at[i],
            device_id=(g, partner),
            device_id_type=MESH,
        )

    def step(i, c):
        at = slot(i, k)
        e = jnp.concatenate([enc[at], enc[at + 1]], axis=1)
        m = jnp.concatenate([mean[2 * i], mean[2 * i + 1]], axis=1)
        pre = dot_nn(wtrans[1], e) + dot_nn(wtrans[2], m) + bias
        sig = sigmoid(pre)
        hidden = (pre * sig).astype(bf16)
        logits = dot_nn(head, hidden)
        top = jnp.max(logits, axis=0, keepdims=True)
        expd = jnp.exp(logits - top)
        total = jnp.sum(expd, axis=0, keepdims=True)
        cols = pl.ds(pl.multiple_of((i % (steps // 2)) * width, width), width)
        mark = marks[i // (steps // 2), :, cols]
        valid = (mark >= 0).astype(f32)
        onehot = (lax.broadcasted_iota(jnp.int32, (CLS, width), 0) == mark).astype(f32)
        target = jnp.sum(logits * onehot, axis=0, keepdims=True)
        loss = valid * (top + jnp.log(total) - target)
        stats[0:1, :] += loss
        stats[1:2, :] += valid
        grad = ((expd * (1.0 / total) - onehot) * valid).astype(bf16)
        back = dot_tn(head, grad) * (sig * (1.0 + pre * (1.0 - sig)))
        sgrad = back.astype(bf16)
        scale = 1.0 / degree[(i // (steps // 2)) * 2 + k, :, cols].astype(f32)
        out = (dot_nn(neigh_half, sgrad) * scale).astype(bf16)
        for b in range(2):
            lanes = slice(b * B, (b + 1) * B)
            sums[at + b] = out[:, lanes]
            sage[2 * i + b] = sgrad[:, lanes]
            hid[2 * i + b] = hidden[:, lanes]
            lgrad[2 * i + b] = grad[:, lanes]
        exchange(i, k).start()
        return c

    lax.fori_loop(0, steps, step, 0)

    ones = jnp.ones((B, HALF), bf16)
    sg = ng_ = hg = bg = None
    for b in range(local):
        at = (b // blocks) * 2 * blocks + k * blocks + b % blocks
        s = sage[b, half]
        t1 = dot_nt(s, enc[at])
        t2 = dot_nt(s, mean[b])
        t3 = dot_nt(lgrad[b], hid[b, half])
        t4 = dot_nn(s, ones)
        sg = t1 if sg is None else sg + t1
        ng_ = t2 if ng_ is None else ng_ + t2
        hg = t3 if hg is None else hg + t3
        bg = t4 if bg is None else bg + t4
        self_back[b] = dot_nn(self_half, sage[b])
    self_grad[...] = sg
    neigh_grad[...] = ng_
    head_grad[...] = hg
    bias_grad[...] = bg

    def done(i, c):
        exchange(i, 1 - k).wait_recv()
        exchange(i, k).wait_send()
        return c

    lax.fori_loop(0, steps, done, 0)


def backward_kernel(lists, tiles, sums, self_back, fbuf, table, wtrans, enc_grad, bias_grad, acc):
    q = lax.axis_index("col")
    k = q % 2
    x = q // 2
    local = self_back.shape[0]
    blocks = local // 2

    def clear(i, c):
        acc[i] = jnp.zeros((HALF, B), f32)
        return c

    lax.fori_loop(0, local + 1, clear, 0)
    count = lists[7, 0]

    def step(i, c):
        for u in range(UNROLL):
            j = i * UNROLL + u
            acc[lists[4, j]] += dot_nn(sums[lists[5, j]], tiles[lists[3, j]])
        return c

    lax.fori_loop(0, (count + UNROLL - 1) // UNROLL, step, 0)

    half = pl.ds(pl.multiple_of(x * HALF, HALF), HALF)
    wide = column_of(table[PROWS - 2 : PROWS + 14, half], 0)
    wide = jnp.concatenate([wide, wide], axis=1)
    weight = wtrans[0, half]
    eg = bg = None
    for b in range(local):
        piece = fbuf[(b // blocks) * 2 + k, (b % blocks) * B : (b % blocks + 1) * B]
        pre = dot_nt(weight, piece) + wide
        sig = sigmoid(pre)
        grad = ((self_back[b] + acc[b]) * (sig * (1.0 + pre * (1.0 - sig)))).astype(bf16)
        t1 = dot_nn(grad, piece)
        gf = grad.astype(f32)
        t2 = gf[:, :HALF] + gf[:, HALF:]
        eg = t1 if eg is None else eg + t1
        bg = t2 if bg is None else bg + t2
    enc_grad[...] = eg
    bias_grad[...] = bg


def reduce_kernel(
    ng,
    enc_grad,
    benc_grad,
    self_grad,
    neigh_grad,
    head_grad,
    bsage_grad,
    hot,
    stats,
    slot_grad,
    loss,
    gtab,
    pbuf,
    rbuf,
    qbuf,
    inbox,
    sbuf,
    srecv,
    sbox,
    core_sem,
    stat_sem,
    g_send,
    g_recv,
    s_send,
    s_recv,
):
    g, q, k, x, partner, across = place()
    barrier = pltpu.get_barrier_semaphore()
    pl.semaphore_signal(barrier, inc=1, device_id=(g, partner), device_id_type=MESH)

    def greet(d, c):
        pl.semaphore_signal(barrier, inc=1, device_id=((g + d) % ng, q), device_id_type=MESH)
        return c

    lax.fori_loop(1, ng, greet, 0)
    sp = inbox.shape[1]
    slots = ng * sp

    both = jnp.sum(stats[...], axis=1, keepdims=True)
    sbuf[...] = jnp.broadcast_to(both, sbuf.shape)
    gtab[0:B] = jnp.transpose(enc_grad[...])
    gtab[B : 2 * B] = jnp.transpose(self_grad[...])
    gtab[2 * B : 3 * B] = jnp.transpose(neigh_grad[...])
    gtab[3 * B : 3 * B + CLS] = head_grad[...]
    tail = lax.broadcasted_iota(jnp.int32, (16, HALF), 0)
    row_one = jnp.sum(jnp.transpose(benc_grad[...]), axis=0, keepdims=True)
    row_two = jnp.transpose(bsage_grad[...])[0:1]
    gtab[PROWS - 2 : PROWS + 14] = jnp.where(tail == 0, row_one, jnp.where(tail == 1, row_two, 0.0))
    whole = gtab[...]
    rolled = pltpu.roll(whole, HALF // 2, 1)
    low = lax.broadcasted_iota(jnp.int32, (TROWS, HALF), 1) < HALF // 2

    def spread(first, second):
        one = jnp.where(low, first, 0.0).astype(bf16)
        two = jnp.where(low, 0.0, second).astype(bf16)
        both = dot_tn(hot[:, :slots], one) + dot_tn(hot[:, slots:], two)
        return both.astype(bf16)

    pbuf[0] = spread(whole, rolled)
    pbuf[1] = spread(rolled, whole)
    pl.semaphore_wait(barrier, ng)

    def remote(src, dst, send, recv, dev):
        return pltpu.make_async_remote_copy(
            src_ref=src, dst_ref=dst, send_sem=send, recv_sem=recv, device_id=dev, device_id_type=MESH
        )

    one = remote(pbuf.at[1 - k], rbuf, core_sem.at[0], core_sem.at[1], (g, partner))
    one.start()
    two = remote(sbuf, srecv, stat_sem.at[0], stat_sem.at[1], (g, partner))
    two.start()
    one.wait()
    two.wait()
    qbuf[...] = (
        (pbuf[k].astype(f32) + rbuf[...].astype(f32)).astype(bf16).reshape(ng, sp, HALF)
    )
    sbox[g] = sbuf[...] + srecv[...]

    def out(d):
        to = (g + d) % ng
        return remote(qbuf.at[to], inbox.at[g], g_send.at[d], g_recv.at[d], (to, q))

    def got(d):
        src = (g + ng - d) % ng
        return remote(qbuf.at[src], inbox.at[src], g_send.at[d], g_recv.at[d], (src, q))

    def stat_out(d):
        to = (g + d) % ng
        return remote(sbox.at[g], sbox.at[g], s_send.at[d], s_recv.at[d], (to, q))

    def stat_got(d):
        src = (g + ng - d) % ng
        return remote(sbox.at[src], sbox.at[src], s_send.at[d], s_recv.at[d], (src, q))

    def start(d, c):
        stat_out(d).start()
        out(d).start()
        return c

    lax.fori_loop(1, ng, start, 0)
    inbox[g] = qbuf[g]

    def arrive(d, c):
        stat_got(d).wait_recv()
        got(d).wait_recv()
        return c

    lax.fori_loop(1, ng, arrive, 0)

    def add_stat(i, c):
        return c + sbox[i]

    sums = lax.fori_loop(0, ng, add_stat, jnp.zeros(sbuf.shape, f32))
    loss_sum = sums[0:1]
    count = sums[1:2]
    loss[...] = jnp.broadcast_to(loss_sum / count, loss.shape)

    def add(i, c):
        return c + inbox[i].astype(f32)

    total = lax.fori_loop(0, ng, add, jnp.zeros((sp, HALF), f32))
    slot_grad[...] = total / count

    def finish(d, c):
        stat_out(d).wait_send()
        out(d).wait_send()
        return c

    lax.fori_loop(1, ng, finish, 0)


def params(limit, collective=None):
    return pltpu.CompilerParams(
        vmem_limit_bytes=limit << 20, collective_id=collective, has_side_effects=collective is not None
    )


DMA = pltpu.SemaphoreType.DMA


def body(
    features,
    adj_tiles,
    block_pairs,
    tile_count,
    degree,
    labels,
    loss_mask,
    slot_piece,
    master,
    moment_one,
    moment_two,
):
    nc = lax.axis_size("col")
    ng = lax.axis_size("grp")
    q = lax.axis_index("col")
    grp_index = lax.axis_index("grp")
    rows = features.shape[0]
    blocks = rows // B
    nb = nc * blocks
    local = 2 * blocks
    tile_slots = adj_tiles.shape[0]
    tpad = -(-tile_slots // HALF) * HALF
    slots = slot_piece.shape[1]
    sp = -(-slots // 16) * 16
    width = master.shape[2]
    chunks = blocks

    flat = jnp.transpose(master.astype(bf16), (1, 0, 2))
    flat = jnp.pad(flat, ((0, 0), (0, sp - slots), (0, 0)))
    empty = jnp.zeros_like(flat)
    wmsg = jnp.where(
        q % 2 == 0,
        jnp.concatenate([flat, empty], axis=2),
        jnp.concatenate([empty, flat], axis=2),
    )
    piece = jnp.pad(slot_piece, ((0, 0), (0, sp - slots)), constant_values=-1).reshape(1, -1)
    srow = jnp.concatenate(
        [jnp.where(piece >= 0, piece * PR + j, -1) for j in range(PR)], axis=1
    )
    degree_rows = degree.reshape(nc, 1, rows)

    fbuf, enc, table, wtrans, hot, marks, lists = pl.pallas_call(
        functools.partial(gather_kernel, ng),
        out_shape=(
            sds((nc, rows, F), bf16),
            sds((nb, HID, B), bf16),
            sds((TROWS, HID), bf16),
            sds((3, HID, HID), bf16),
            sds((TROWS, 2 * ng * sp), bf16),
            sds((2, 1, rows), jnp.int32),
            sds((8, tpad), jnp.int32),
        ),
        in_specs=[ANY, VM, VM, VM, VM, VM, SM],
        out_specs=(VM,) * 7,
        scratch_shapes=[
            pltpu.VMEM((2, sp, HALF), bf16),
            pltpu.VMEM((2, ng, 2, sp, HALF), bf16),
            pltpu.VMEM((8, tpad), f32),
            DMA,
            DMA((2,)),
            DMA((2,)),
            DMA((2,)),
            DMA((2,)),
            DMA((ng,)),
            DMA((ng,)),
            DMA((ng,)),
            DMA((ng,)),
            DMA((chunks,)),
            DMA((chunks,)),
            DMA((chunks,)),
            DMA((chunks,)),
        ],
        compiler_params=params(24, 0),
        name="gather",
    )(
        features,
        wmsg,
        srow,
        labels.reshape(1, rows),
        loss_mask.reshape(1, rows),
        block_pairs,
        tile_count,
    )

    mean = pl.pallas_call(
        forward_kernel,
        out_shape=sds((local, HID, B), bf16),
        in_specs=[SM, VM, VM, VM],
        out_specs=VM,
        scratch_shapes=[pltpu.VMEM((local + 1, HID, B), f32)],
        compiler_params=params(56),
        name="forward",
    )(lists, adj_tiles, enc, degree_rows)

    sums, self_back, self_grad, neigh_grad, head_grad, bsage, stats = pl.pallas_call(
        sage_kernel,
        out_shape=(
            sds((nb, HALF, B), bf16),
            sds((local, HALF, B), f32),
            sds((HALF, HID), f32),
            sds((HALF, HID), f32),
            sds((CLS, HALF), f32),
            sds((HALF, HALF), f32),
            sds((8, 2 * B), f32),
        ),
        in_specs=[VM] * 6,
        out_specs=(VM,) * 7,
        scratch_shapes=[
            pltpu.VMEM((local, HID, B), bf16),
            pltpu.VMEM((local, HID, B), bf16),
            pltpu.VMEM((local, CLS, B), bf16),
            DMA((blocks,)),
            DMA((blocks,)),
        ],
        compiler_params=params(24, 1),
        name="sage",
    )(enc, mean, table, wtrans, marks, degree_rows)

    enc_grad, benc = pl.pallas_call(
        backward_kernel,
        out_shape=(sds((HALF, F), f32), sds((HALF, HALF), f32)),
        in_specs=[SM, VM, VM, VM, VM, VM, VM],
        out_specs=(VM,) * 2,
        scratch_shapes=[pltpu.VMEM((local + 1, HALF, B), f32)],
        compiler_params=params(56),
        name="backward",
    )(lists, adj_tiles, sums, self_back, fbuf, table, wtrans)

    packed, loss = pl.pallas_call(
        functools.partial(reduce_kernel, ng),
        out_shape=(sds((sp, HALF), f32), sds((8, HALF), f32)),
        in_specs=[VM] * 8,
        out_specs=(VM,) * 2,
        scratch_shapes=[
            pltpu.VMEM((TROWS, HALF), f32),
            pltpu.VMEM((2, ng * sp, HALF), bf16),
            pltpu.VMEM((ng * sp, HALF), bf16),
            pltpu.VMEM((ng, sp, HALF), bf16),
            pltpu.VMEM((ng, sp, HALF), bf16),
            pltpu.VMEM((8, HALF), f32),
            pltpu.VMEM((8, HALF), f32),
            pltpu.VMEM((ng, 8, HALF), f32),
            DMA((2,)),
            DMA((2,)),
            DMA((ng,)),
            DMA((ng,)),
            DMA((ng,)),
            DMA((ng,)),
        ],
        compiler_params=params(24, 2),
        name="reduce",
    )(enc_grad, benc, self_grad, neigh_grad, head_grad, bsage, hot, stats)

    mean_loss = loss[0, 0]
    my_pieces = lax.dynamic_slice_in_dim(slot_piece, grp_index, 1, 0)[0]
    is_owned = my_pieces >= 0
    safe_pieces = jnp.where(is_owned, my_pieces, 0)
    owned_values = is_owned[:, None, None]
    slot_grad = jnp.where(owned_values, packed[:slots].reshape(slots, PR, width), 0.0)
    table_rows = safe_pieces[:, None] * PR + jnp.arange(PR, dtype=jnp.int32)[None, :]
    decay_values = jnp.where(table_rows < PROWS - 2, decay_rate, 0.0)[:, :, None]
    first_moment = beta_one * moment_one + (1.0 - beta_one) * slot_grad
    second_moment = beta_two * moment_two + (1.0 - beta_two) * slot_grad * slot_grad
    first_hat = first_moment / (1.0 - beta_one**STEP)
    second_hat = second_moment / (1.0 - beta_two**STEP)
    updated = master - learn_rate * (
        first_hat / (jnp.sqrt(second_hat) + adam_epsilon) + decay_values * master
    )
    updated = jnp.where(owned_values, updated, 0.0)
    first_moment = jnp.where(owned_values, first_moment, 0.0)
    second_moment = jnp.where(owned_values, second_moment, 0.0)
    return (mean_loss, updated, first_moment, second_moment, updated.astype(jnp.bfloat16))


def solution(mesh):
    in_specs = (
        P(("grp", "col"), None),
        P("grp", None, None),
        P("grp", None, None),
        P("grp"),
        P("grp"),
        P(("grp", "col")),
        P(("grp", "col")),
        P(),
        P("grp", None, "col"),
        P("grp", None, "col"),
        P("grp", None, "col"),
    )
    out_specs = (
        P(),
        P("grp", None, "col"),
        P("grp", None, "col"),
        P("grp", None, "col"),
        P("grp", None, "col"),
    )
    return jax.shard_map(body, mesh=mesh, in_specs=in_specs, out_specs=out_specs, check_vma=False)
```

```python
import functools
import jax
import jax.numpy as jnp
from jax import lax
from jax.experimental import pallas as pl
from jax.experimental.pallas import tpu as pltpu
from jax.sharding import PartitionSpec as P

F = 256
HID = 256
CLS = 64
B = 256
PR = 2
STEP = 7
PROWS = 834
TROWS = 848
HALF = 128
UNROLL = 8

learn_rate = 0.01
beta_one = 0.5
beta_two = 0.5
adam_epsilon = 1e-08
decay_rate = 0.1

f32 = jnp.float32
bf16 = jnp.bfloat16
MESH = pl.DeviceIdType.MESH
VM = pl.BlockSpec(memory_space=pltpu.VMEM)
SM = pl.BlockSpec(memory_space=pltpu.SMEM)
HBM = pl.BlockSpec(memory_space=pltpu.HBM)


def sds(shape, dtype):
    return jax.ShapeDtypeStruct(shape, dtype)


def dot_nn(a, b):
    return lax.dot_general(a, b, (((1,), (0,)), ((), ())), preferred_element_type=f32)


def dot_nt(a, b):
    return lax.dot_general(a, b, (((1,), (1,)), ((), ())), preferred_element_type=f32)


def dot_tn(a, b):
    return lax.dot_general(a, b, (((0,), (0,)), ((), ())), preferred_element_type=f32)


def column_of(rows16, row):
    pick = (lax.broadcasted_iota(jnp.int32, (16, HALF), 0) == row).astype(bf16)
    return dot_tn(rows16, pick)


def place():
    g = lax.axis_index("grp")
    q = lax.axis_index("col")
    k = q % 2
    x = q // 2
    partner = q + 1 - 2 * k
    across = q + 2 - 4 * x
    return g, q, k, x, partner, across


def sigmoid(v):
    return jax.nn.sigmoid(v)


def remote(src, dst, send, recv, dev):
    return pltpu.make_async_remote_copy(
        src_ref=src, dst_ref=dst, send_sem=send, recv_sem=recv, device_id=dev, device_id_type=MESH
    )


def gather_kernel(
    ng,
    feat,
    master,
    pieces,
    labels,
    mask,
    pairs,
    degree,
    tcount,
    fbuf,
    enc,
    table,
    wtrans,
    hot,
    marks,
    inverse,
    lists,
    mbuf,
    pcs,
    lab,
    msk,
    prs,
    deg,
    lbuf,
    wmsg,
    pmsg,
    wbuf,
    local_sem,
    small_sem,
    mark_sem,
    ws_core,
    ws_x,
    ws_send,
    ws_recv,
    wr_send,
    wr_recv,
    xs_send,
    xs_recv,
    en_send,
    en_recv,
):
    g, q, k, x, partner, across = place()
    rows = feat.shape[0]
    blocks = rows // B
    sp = wmsg.shape[1]
    slots = pieces.shape[1]
    count = pairs.shape[2]
    tpad = lists.shape[1]
    width = master.shape[1]

    load = pltpu.make_async_copy(feat, fbuf.at[x], local_sem)
    load.start()
    small = [
        pltpu.make_async_copy(a, b, small_sem.at[i])
        for i, (a, b) in enumerate(
            [
                (master, mbuf),
                (pieces, pcs),
                (labels, lab),
                (mask, msk),
                (pairs, prs),
                (degree.at[k], deg.at[0]),
                (degree.at[2 + k], deg.at[1]),
            ]
        )
    ]
    for copy in small:
        copy.start()

    barrier = pltpu.get_barrier_semaphore()
    pl.semaphore_signal(barrier, inc=1, device_id=(g, across), device_id_type=MESH)
    pl.semaphore_signal(barrier, inc=1, device_id=(g, partner), device_id_type=MESH)

    def greet(d, c):
        pl.semaphore_signal(barrier, inc=1, device_id=((g + d) % ng, q), device_id_type=MESH)
        return c

    lax.fori_loop(1, ng, greet, 0)

    for copy in small:
        copy.wait()
    for j in range(PR):
        cols = jnp.concatenate(
            [mbuf[j], jnp.zeros((width, HALF - slots), f32)], axis=1
        )
        turned = jnp.transpose(jnp.concatenate([cols, jnp.zeros_like(cols)], axis=0))
        other = pltpu.roll(turned, width, 1)
        wmsg[j] = jnp.where(k == 0, turned, other)[:sp].astype(bf16)
    marks[x] = jnp.where(msk[...] > 0, lab[...], -1)
    pl.semaphore_wait(barrier, ng + 1)

    first = remote(wmsg, pmsg, ws_core.at[0], ws_core.at[1], (g, partner))
    first.start()
    mark_copy = remote(marks.at[x], marks.at[x], mark_sem.at[0], mark_sem.at[1], (g, across))
    mark_copy.start()
    load.wait()

    def cross(i):
        piece = fbuf.at[x, pl.ds(pl.multiple_of(i * B, B), B)]
        return remote(piece, piece, xs_send.at[i], xs_recv.at[i], (g, across))

    cross(0).start()
    first.wait()
    wbuf[k, g, x] = wmsg[k] + pmsg[k]
    second = remote(wbuf.at[k, g, x], wbuf.at[k, g, x], ws_x.at[0], ws_x.at[1], (g, across))
    second.start()

    def cross_all(i, c):
        cross(i).start()
        return c

    lax.fori_loop(1, blocks, cross_all, 0)
    second.wait()

    def to_group(d):
        return remote(
            wbuf.at[k, g], wbuf.at[k, g], ws_send.at[d], ws_recv.at[d], ((g + d) % ng, q)
        )

    def from_group(d):
        src = (g + ng - d) % ng
        return remote(wbuf.at[k, src], wbuf.at[k, src], ws_send.at[d], ws_recv.at[d], (src, q))

    def hand_over(d):
        src = (g + ng - d) % ng
        return remote(
            wbuf.at[k, src], wbuf.at[k, src], wr_send.at[d], wr_recv.at[d], (g, partner)
        )

    def handed(d):
        src = (g + ng - d) % ng
        return remote(
            wbuf.at[1 - k, src], wbuf.at[1 - k, src], wr_send.at[d], wr_recv.at[d], (g, partner)
        )

    def send_group(d, c):
        to_group(d).start()
        return c

    lax.fori_loop(1, ng, send_group, 0)
    hand_over(0).start()

    shift = blocks.bit_length() - 1
    fill = jnp.zeros((2, tpad - count), jnp.int32)
    both = jnp.concatenate([prs[0], fill], axis=1)
    rvec = both[0:1]
    cvec = both[1:2]
    tvec = lax.broadcasted_iota(jnp.int32, (1, tpad), 1)
    live = tvec < tcount[0]

    def split(v):
        quarter = lax.shift_right_logical(v, shift)
        local = lax.shift_right_logical(quarter, 1) * blocks + (v & (blocks - 1))
        return (quarter & 1) == k, local

    fmine, frow = split(rvec)
    bmine, bcol = split(cvec)
    fmine = fmine & live
    bmine = bmine & live
    upto = (
        lax.broadcasted_iota(jnp.int32, (tpad, tpad), 0)
        <= lax.broadcasted_iota(jnp.int32, (tpad, tpad), 1)
    ).astype(bf16)
    order = lax.broadcasted_iota(jnp.int32, (tpad, tpad), 0)
    zero = jnp.zeros((1, tpad), jnp.int32)

    def compact(mine, one, two):
        flag = mine.astype(f32)
        seen = dot_nn(jnp.broadcast_to(flag, (8, tpad)).astype(bf16), upto)[0:1].astype(jnp.int32)
        spot = jnp.where(mine, seen - 1, -1)
        chosen = (order == spot).astype(f32).astype(bf16)
        values = jnp.concatenate([tvec, one, two, zero, zero, zero, zero, zero], axis=0)
        packed = dot_nt(values.astype(f32).astype(bf16), chosen).astype(jnp.int32)
        total = jnp.sum(flag, axis=1, keepdims=True).astype(jnp.int32)
        past = tvec >= total
        return packed[0:1], jnp.where(past, 2 * blocks, packed[1:2]), packed[2:3], zero + total

    ft, fr, fc, fn = compact(fmine, frow, cvec)
    bt, bc, br, bn = compact(bmine, bcol, rvec)
    lbuf[...] = jnp.concatenate([ft, fr, fc, bt, bc, br, fn, bn], axis=0)
    put = pltpu.make_async_copy(lbuf, lists, local_sem)
    put.start()
    inverse[...] = 1.0 / deg[...].astype(f32)

    lanes = ng * sp
    piece = jnp.concatenate([pcs[...], jnp.full((ng, HALF - slots), -1, jnp.int32)], axis=1)
    high = lax.shift_right_logical(piece + 1, 4).astype(f32).astype(bf16)
    low = ((piece + 1) & 15).astype(f32).astype(bf16)
    lane = lax.broadcasted_iota(jnp.int32, (1, lanes), 1)
    owner = jnp.floor((lane.astype(f32) + 0.5) * (1.0 / sp)).astype(jnp.int32)
    within = lane - owner * sp
    pick = (lax.broadcasted_iota(jnp.int32, (HALF, lanes), 0) == within).astype(f32).astype(bf16)
    wide = dot_nn(high, pick) * 16.0 + dot_nn(low, pick)
    keep = lax.broadcasted_iota(jnp.int32, (ng, lanes), 0) == owner
    flat = jnp.sum(jnp.where(keep, wide, 0.0), axis=0, keepdims=True).astype(jnp.int32) - 1
    line = lax.broadcasted_iota(jnp.int32, (TROWS, lanes), 0)
    for j in range(PR):
        at = jnp.where(flat >= 0, flat * PR + j, -1)
        hot[:, j * lanes : (j + 1) * lanes] = (line == at).astype(f32).astype(bf16)

    def pass_on(d, c):
        from_group(d).wait_recv()
        hand_over(d).start()
        return c

    lax.fori_loop(1, ng, pass_on, 0)

    def take(d, c):
        handed(d).wait_recv()
        return c

    lax.fori_loop(0, ng, take, 0)

    left = wbuf[:, :, 0].reshape(2 * ng * sp, HALF)
    right = wbuf[:, :, 1].reshape(2 * ng * sp, HALF)
    full = dot_nn(hot[...], jnp.concatenate([left, right], axis=1))
    table[...] = full.astype(bf16)
    for i in range(3):
        wtrans[i] = jnp.transpose(full[i * B : (i + 1) * B]).astype(bf16)
    bias = column_of(table[PROWS - 2 : PROWS + 14], 0)
    bias = jnp.concatenate([bias] * 4, axis=1)

    def share(i, core):
        away = i // (blocks // 2)
        quarter = (x + away * (1 - 2 * x)) * 2 + core
        piece = enc.at[pl.ds(quarter * blocks + (i % (blocks // 2)) * 2, 2)]
        return remote(piece, piece, en_send.at[i], en_recv.at[i], (g, partner))

    def encode(i):
        away = i // (blocks // 2)
        side = x + away * (1 - 2 * x)
        base = (i % (blocks // 2)) * 2
        piece = fbuf[side, pl.ds(pl.multiple_of(base * B, 2 * B), 2 * B)]
        pre = dot_nt(wtrans[0], piece) + bias
        out = (pre * sigmoid(pre)).astype(bf16)
        at = (side * 2 + k) * blocks + base
        enc[at] = out[:, :B]
        enc[at + 1] = out[:, B:]
        share(i, k).start()

    def own(i, c):
        encode(i)
        return c

    lax.fori_loop(0, blocks // 2, own, 0)

    def crossed(i):
        piece = fbuf.at[1 - x, pl.ds(pl.multiple_of(i * B, B), B)]
        return remote(piece, piece, xs_send.at[i], xs_recv.at[i], (g, across))

    def far(i, c):
        crossed(2 * i).wait_recv()
        crossed(2 * i + 1).wait_recv()
        encode(blocks // 2 + i)
        return c

    lax.fori_loop(0, blocks // 2, far, 0)

    def settle(i, c):
        share(i, 1 - k).wait_recv()
        share(i, k).wait_send()
        cross(i).wait_send()
        return c

    lax.fori_loop(0, blocks, settle, 0)
    mark_copy.wait()

    def drain_group(d, c):
        to_group(d).wait_send()
        hand_over(d).wait_send()
        return c

    lax.fori_loop(1, ng, drain_group, 0)
    hand_over(0).wait_send()
    put.wait()


RING = 32


def each_tile(tiles, order, count, ring, sems, use):
    def fetch(j):
        return pltpu.make_async_copy(tiles.at[order(j)], ring.at[j % RING], sems.at[j % RING])

    def ask(j):
        @pl.when(j < count)
        def _():
            fetch(j).start()

    def first(j, c):
        ask(j)
        return c

    lax.fori_loop(0, RING, first, 0)

    def step(i, c):
        for u in range(UNROLL):
            j = i * UNROLL + u

            @pl.when(j < count)
            def _():
                fetch(j).wait()

        for u in range(UNROLL):
            j = i * UNROLL + u
            use(j, ring[j % RING])
        for u in range(UNROLL):
            ask(i * UNROLL + u + RING)
        return c

    return lambda: lax.fori_loop(0, (count + UNROLL - 1) // UNROLL, step, 0)


def forward_kernel(lists, tiles, enc, inverse, mean, acc, ring, sems):
    local = mean.shape[0]
    blocks = local // 2

    def use(j, tile):
        acc[lists[1, j]] += dot_nt(enc[lists[2, j]], tile)

    run = each_tile(tiles, lambda j: lists[0, j], lists[6, 0], ring, sems, use)

    def clear(i, c):
        acc[i] = jnp.zeros((B, B), f32)
        return c

    lax.fori_loop(0, local + 1, clear, 0)
    run()

    def finish(i, c):
        scale = inverse[i // blocks, :, pl.ds(pl.multiple_of((i % blocks) * B, B), B)]
        mean[i] = (acc[i] * scale).astype(bf16)
        return c

    lax.fori_loop(0, local, finish, 0)


def sage_kernel(
    enc,
    mean,
    table,
    wtrans,
    marks,
    inverse,
    sums,
    self_back,
    self_grad,
    neigh_grad,
    head_grad,
    bias_grad,
    stats,
    sage,
    hid,
    lgrad,
    send,
    recv,
):
    g, q, k, x, partner, across = place()
    local = mean.shape[0]
    blocks = local // 2
    width = 2 * B
    steps = local // 2
    barrier = pltpu.get_barrier_semaphore()
    pl.semaphore_signal(barrier, inc=1, device_id=(g, partner), device_id_type=MESH)
    pl.semaphore_wait(barrier, 1)
    half = pl.ds(pl.multiple_of(x * HALF, HALF), HALF)
    head = table[F + 2 * HID : F + 2 * HID + CLS]
    bias = column_of(table[PROWS - 2 : PROWS + 14], 1)
    bias = jnp.concatenate([bias] * 4, axis=1)
    neigh_half = table[pl.ds(pl.multiple_of(F + HID + x * HALF, HALF), HALF)]
    self_half = table[pl.ds(pl.multiple_of(F + x * HALF, HALF), HALF)]
    stats[...] = jnp.zeros_like(stats)

    def slot(i, core):
        return (i // (steps // 2)) * 2 * blocks + core * blocks + (i % (steps // 2)) * 2

    def exchange(i, core):
        piece = sums.at[pl.ds(slot(i, core), 2)]
        return pltpu.make_async_remote_copy(
            src_ref=piece,
            dst_ref=piece,
            send_sem=send.at[i],
            recv_sem=recv.at[i],
            device_id=(g, partner),
            device_id_type=MESH,
        )

    def step(i, c):
        at = slot(i, k)
        e = jnp.concatenate([enc[at], enc[at + 1]], axis=1)
        m = jnp.concatenate([mean[2 * i], mean[2 * i + 1]], axis=1)
        pre = dot_nn(wtrans[1], e) + dot_nn(wtrans[2], m) + bias
        sig = sigmoid(pre)
        hidden = (pre * sig).astype(bf16)
        logits = dot_nn(head, hidden)
        top = jnp.max(logits, axis=0, keepdims=True)
        expd = jnp.exp(logits - top)
        total = jnp.sum(expd, axis=0, keepdims=True)
        cols = pl.ds(pl.multiple_of((i % (steps // 2)) * width, width), width)
        mark = marks[i // (steps // 2), :, cols]
        valid = (mark >= 0).astype(f32)
        onehot = (lax.broadcasted_iota(jnp.int32, (CLS, width), 0) == mark).astype(f32)
        target = jnp.sum(logits * onehot, axis=0, keepdims=True)
        loss = valid * (top + jnp.log(total) - target)
        stats[0:1, :] += loss
        stats[1:2, :] += valid
        grad = ((expd * (1.0 / total) - onehot) * valid).astype(bf16)
        back = dot_tn(head, grad) * (sig * (1.0 + pre * (1.0 - sig)))
        sgrad = back.astype(bf16)
        scale = inverse[i // (steps // 2), :, cols]
        out = (dot_nn(neigh_half, sgrad) * scale).astype(bf16)
        for b in range(2):
            lanes = slice(b * B, (b + 1) * B)
            sums[at + b] = out[:, lanes]
            sage[2 * i + b] = sgrad[:, lanes]
            hid[2 * i + b] = hidden[:, lanes]
            lgrad[2 * i + b] = grad[:, lanes]
        exchange(i, k).start()
        return c

    lax.fori_loop(0, steps, step, 0)

    ones = jnp.ones((B, HALF), bf16)
    sg = ng_ = hg = bg = None
    for b in range(local):
        at = (b // blocks) * 2 * blocks + k * blocks + b % blocks
        s = sage[b, half]
        t1 = dot_nt(s, enc[at])
        t2 = dot_nt(s, mean[b])
        t3 = dot_nt(lgrad[b], hid[b, half])
        t4 = dot_nn(s, ones)
        sg = t1 if sg is None else sg + t1
        ng_ = t2 if ng_ is None else ng_ + t2
        hg = t3 if hg is None else hg + t3
        bg = t4 if bg is None else bg + t4
        self_back[b] = dot_nn(self_half, sage[b])
    self_grad[...] = sg
    neigh_grad[...] = ng_
    head_grad[...] = hg
    bias_grad[...] = bg

    def done(i, c):
        exchange(i, 1 - k).wait_recv()
        exchange(i, k).wait_send()
        return c

    lax.fori_loop(0, steps, done, 0)


def backward_kernel(lists, tiles, sums, self_back, fbuf, table, wtrans, enc_grad, bias_grad, acc, ring, sems):
    x = lax.axis_index("col") // 2
    local = self_back.shape[0]
    blocks = local // 2

    def use(j, tile):
        acc[lists[4, j]] += dot_nn(sums[lists[5, j]], tile)

    run = each_tile(tiles, lambda j: lists[3, j], lists[7, 0], ring, sems, use)

    def clear(i, c):
        acc[i] = jnp.zeros((HALF, B), f32)
        return c

    lax.fori_loop(0, local + 1, clear, 0)
    run()
    half = pl.ds(pl.multiple_of(x * HALF, HALF), HALF)
    wide = column_of(table[PROWS - 2 : PROWS + 14, half], 0)
    wide = jnp.concatenate([wide, wide], axis=1)
    weight = wtrans[0, half]
    eg = bg = None
    for b in range(local):
        piece = fbuf[b // blocks, (b % blocks) * B : (b % blocks + 1) * B]
        pre = dot_nt(weight, piece) + wide
        sig = sigmoid(pre)
        grad = ((self_back[b] + acc[b]) * (sig * (1.0 + pre * (1.0 - sig)))).astype(bf16)
        t1 = dot_nn(grad, piece)
        gf = grad.astype(f32)
        t2 = gf[:, :HALF] + gf[:, HALF:]
        eg = t1 if eg is None else eg + t1
        bg = t2 if bg is None else bg + t2
    enc_grad[...] = eg
    bias_grad[...] = bg


def reduce_kernel(
    ng,
    enc_grad,
    benc_grad,
    self_grad,
    neigh_grad,
    head_grad,
    bsage_grad,
    hot,
    stats,
    slot_grad,
    loss,
    gtab,
    pbuf,
    rbuf,
    qbuf,
    inbox,
    sbuf,
    srecv,
    sbox,
    core_sem,
    stat_sem,
    g_send,
    g_recv,
    s_send,
    s_recv,
):
    g, q, k, x, partner, across = place()
    barrier = pltpu.get_barrier_semaphore()
    pl.semaphore_signal(barrier, inc=1, device_id=(g, partner), device_id_type=MESH)

    def greet(d, c):
        pl.semaphore_signal(barrier, inc=1, device_id=((g + d) % ng, q), device_id_type=MESH)
        return c

    lax.fori_loop(1, ng, greet, 0)
    sp = inbox.shape[1]
    slots = ng * sp

    both = jnp.sum(stats[...], axis=1, keepdims=True)
    sbuf[...] = jnp.broadcast_to(both, sbuf.shape)
    gtab[0:B] = jnp.transpose(enc_grad[...])
    gtab[B : 2 * B] = jnp.transpose(self_grad[...])
    gtab[2 * B : 3 * B] = jnp.transpose(neigh_grad[...])
    gtab[3 * B : 3 * B + CLS] = head_grad[...]
    tail = lax.broadcasted_iota(jnp.int32, (16, HALF), 0)
    row_one = jnp.sum(jnp.transpose(benc_grad[...]), axis=0, keepdims=True)
    row_two = jnp.transpose(bsage_grad[...])[0:1]
    gtab[PROWS - 2 : PROWS + 14] = jnp.where(tail == 0, row_one, jnp.where(tail == 1, row_two, 0.0))
    whole = gtab[...]
    rolled = pltpu.roll(whole, HALF // 2, 1)
    low = lax.broadcasted_iota(jnp.int32, (TROWS, HALF), 1) < HALF // 2

    def spread(first, second):
        one = jnp.where(low, first, 0.0).astype(bf16)
        two = jnp.where(low, 0.0, second).astype(bf16)
        both = dot_tn(hot[:, :slots], one) + dot_tn(hot[:, slots:], two)
        return both.astype(bf16)

    pbuf[0] = spread(whole, rolled)
    pbuf[1] = spread(rolled, whole)
    pl.semaphore_wait(barrier, ng)

    one = remote(pbuf.at[1 - k], rbuf, core_sem.at[0], core_sem.at[1], (g, partner))
    one.start()
    two = remote(sbuf, srecv, stat_sem.at[0], stat_sem.at[1], (g, partner))
    two.start()
    one.wait()
    two.wait()
    qbuf[...] = (
        (pbuf[k].astype(f32) + rbuf[...].astype(f32)).astype(bf16).reshape(ng, sp, HALF)
    )
    sbox[g] = sbuf[...] + srecv[...]

    def out(d):
        to = (g + d) % ng
        return remote(qbuf.at[to], inbox.at[g], g_send.at[d], g_recv.at[d], (to, q))

    def got(d):
        src = (g + ng - d) % ng
        return remote(qbuf.at[src], inbox.at[src], g_send.at[d], g_recv.at[d], (src, q))

    def stat_out(d):
        to = (g + d) % ng
        return remote(sbox.at[g], sbox.at[g], s_send.at[d], s_recv.at[d], (to, q))

    def stat_got(d):
        src = (g + ng - d) % ng
        return remote(sbox.at[src], sbox.at[src], s_send.at[d], s_recv.at[d], (src, q))

    def start(d, c):
        stat_out(d).start()
        out(d).start()
        return c

    lax.fori_loop(1, ng, start, 0)
    inbox[g] = qbuf[g]

    def arrive(d, c):
        stat_got(d).wait_recv()
        got(d).wait_recv()
        return c

    lax.fori_loop(1, ng, arrive, 0)

    def add_stat(i, c):
        return c + sbox[i]

    sums = lax.fori_loop(0, ng, add_stat, jnp.zeros(sbuf.shape, f32))
    loss_sum = sums[0:1]
    count = sums[1:2]
    loss[...] = jnp.broadcast_to(loss_sum / count, loss.shape)

    def add(i, c):
        return c + inbox[i].astype(f32)

    total = lax.fori_loop(0, ng, add, jnp.zeros((sp, HALF), f32))
    slot_grad[...] = total / count

    def finish(d, c):
        stat_out(d).wait_send()
        out(d).wait_send()
        return c

    lax.fori_loop(1, ng, finish, 0)


def update_kernel(packed, loss, pieces, master, first, second, new_master, new_first, new_second, low, mean_loss):
    g = lax.axis_index("grp")
    slots = pieces.shape[1]
    width = master.shape[1]
    sp = packed.shape[0]
    rows = packed[...]
    if sp < HALF:
        rows = jnp.concatenate([rows, jnp.zeros((HALF - sp, HALF), f32)], axis=0)
    turned = jnp.transpose(rows)
    piece = pieces[pl.ds(g, 1), :]
    owned = piece >= 0
    for j in range(PR):
        grad = turned[j * width : (j + 1) * width, :slots]
        decay = jnp.where(piece * PR + j < PROWS - 2, decay_rate, 0.0)
        old = master[j]
        one = beta_one * first[j] + (1.0 - beta_one) * grad
        two = beta_two * second[j] + (1.0 - beta_two) * grad * grad
        one_hat = one / (1.0 - beta_one**STEP)
        two_hat = two / (1.0 - beta_two**STEP)
        new = old - learn_rate * (one_hat / (jnp.sqrt(two_hat) + adam_epsilon) + decay * old)
        new = jnp.where(owned, new, 0.0)
        new_master[j] = new
        new_first[j] = jnp.where(owned, one, 0.0)
        new_second[j] = jnp.where(owned, two, 0.0)
        low[j] = new.astype(bf16)
    mean_loss[0, 0] = loss[0, 0]


def far(v):
    return pltpu.with_memory_space_constraint(v, pltpu.HBM)


def params(limit, collective=None):
    return pltpu.CompilerParams(
        vmem_limit_bytes=limit << 20, collective_id=collective, has_side_effects=collective is not None
    )


DMA = pltpu.SemaphoreType.DMA


def body(
    features,
    adj_tiles,
    block_pairs,
    tile_count,
    degree,
    labels,
    loss_mask,
    slot_piece,
    master,
    moment_one,
    moment_two,
):
    nc = lax.axis_size("col")
    ng = lax.axis_size("grp")
    rows = features.shape[0]
    blocks = rows // B
    nb = nc * blocks
    local = 2 * blocks
    count = adj_tiles.shape[0]
    tpad = -(-count // HALF) * HALF
    slots = slot_piece.shape[1]
    sp = -(-slots // 16) * 16
    width = master.shape[2]
    master_t = jnp.transpose(master, (1, 2, 0))
    first_t = jnp.transpose(moment_one, (1, 2, 0))
    second_t = jnp.transpose(moment_two, (1, 2, 0))

    fbuf, enc, table, wtrans, hot, marks, inverse, lists = pl.pallas_call(
        functools.partial(gather_kernel, ng),
        out_shape=(
            pltpu.VMEM((2, rows, F), bf16),
            pltpu.VMEM((nb, HID, B), bf16),
            pltpu.VMEM((TROWS, HID), bf16),
            pltpu.VMEM((3, HID, HID), bf16),
            pltpu.VMEM((TROWS, 2 * ng * sp), bf16),
            pltpu.VMEM((2, 1, rows), jnp.int32),
            pltpu.VMEM((2, 1, rows), f32),
            sds((8, tpad), jnp.int32),
        ),
        in_specs=[HBM] * 7 + [SM],
        out_specs=(VM,) * 7 + (HBM,),
        scratch_shapes=[
            pltpu.VMEM((PR, width, slots), f32),
            pltpu.VMEM((ng, slots), jnp.int32),
            pltpu.VMEM((1, rows), jnp.int32),
            pltpu.VMEM((1, rows), jnp.int32),
            pltpu.VMEM((1, 2, count), jnp.int32),
            pltpu.VMEM((2, 1, rows), jnp.int32),
            pltpu.VMEM((8, tpad), jnp.int32),
            pltpu.VMEM((2, sp, HALF), bf16),
            pltpu.VMEM((2, sp, HALF), bf16),
            pltpu.VMEM((2, ng, 2, sp, HALF), bf16),
            DMA,
            DMA((7,)),
            DMA((2,)),
            DMA((2,)),
            DMA((2,)),
            DMA((ng,)),
            DMA((ng,)),
            DMA((ng,)),
            DMA((ng,)),
            DMA((blocks,)),
            DMA((blocks,)),
            DMA((blocks,)),
            DMA((blocks,)),
        ],
        compiler_params=params(12, 0),
        name="gather",
    )(
        far(features),
        far(master_t),
        far(slot_piece),
        far(labels.reshape(1, rows)),
        far(loss_mask.reshape(1, rows)),
        far(jnp.transpose(block_pairs, (0, 2, 1))),
        far(degree.reshape(nc, 1, rows)),
        tile_count,
    )

    adj = far(adj_tiles)
    mean = pl.pallas_call(
        forward_kernel,
        out_shape=pltpu.VMEM((local, HID, B), bf16),
        in_specs=[SM, HBM, VM, VM],
        out_specs=VM,
        scratch_shapes=[pltpu.VMEM((local + 1, HID, B), f32), pltpu.VMEM((RING, B, B), bf16), DMA((RING,))],
        compiler_params=params(14),
        name="forward",
    )(lists, adj, enc, inverse)

    sums, self_back, self_grad, neigh_grad, head_grad, bsage, stats = pl.pallas_call(
        sage_kernel,
        out_shape=(
            pltpu.VMEM((nb, HALF, B), bf16),
            pltpu.VMEM((local, HALF, B), f32),
            pltpu.VMEM((HALF, HID), f32),
            pltpu.VMEM((HALF, HID), f32),
            pltpu.VMEM((CLS, HALF), f32),
            pltpu.VMEM((HALF, HALF), f32),
            pltpu.VMEM((8, 2 * B), f32),
        ),
        in_specs=[VM] * 6,
        out_specs=(VM,) * 7,
        scratch_shapes=[
            pltpu.VMEM((local, HID, B), bf16),
            pltpu.VMEM((local, HID, B), bf16),
            pltpu.VMEM((local, CLS, B), bf16),
            DMA((blocks,)),
            DMA((blocks,)),
        ],
        compiler_params=params(12, 1),
        name="sage",
    )(enc, mean, table, wtrans, marks, inverse)

    enc_grad, benc = pl.pallas_call(
        backward_kernel,
        out_shape=(pltpu.VMEM((HALF, F), f32), pltpu.VMEM((HALF, HALF), f32)),
        in_specs=[SM, HBM, VM, VM, VM, VM, VM],
        out_specs=(VM,) * 2,
        scratch_shapes=[pltpu.VMEM((local + 1, HALF, B), f32), pltpu.VMEM((RING, B, B), bf16), DMA((RING,))],
        compiler_params=params(12),
        name="backward",
    )(lists, adj, sums, self_back, fbuf, table, wtrans)

    packed, loss = pl.pallas_call(
        functools.partial(reduce_kernel, ng),
        out_shape=(pltpu.VMEM((sp, HALF), f32), pltpu.VMEM((8, HALF), f32)),
        in_specs=[VM] * 8,
        out_specs=(VM,) * 2,
        scratch_shapes=[
            pltpu.VMEM((TROWS, HALF), f32),
            pltpu.VMEM((2, ng * sp, HALF), bf16),
            pltpu.VMEM((ng * sp, HALF), bf16),
            pltpu.VMEM((ng, sp, HALF), bf16),
            pltpu.VMEM((ng, sp, HALF), bf16),
            pltpu.VMEM((8, HALF), f32),
            pltpu.VMEM((8, HALF), f32),
            pltpu.VMEM((ng, 8, HALF), f32),
            DMA((2,)),
            DMA((2,)),
            DMA((ng,)),
            DMA((ng,)),
            DMA((ng,)),
            DMA((ng,)),
        ],
        compiler_params=params(12, 2),
        name="reduce",
    )(enc_grad, benc, self_grad, neigh_grad, head_grad, bsage, hot, stats)

    shape = (PR, width, slots)
    new_master, new_first, new_second, low, mean_loss = pl.pallas_call(
        update_kernel,
        out_shape=(sds(shape, f32), sds(shape, f32), sds(shape, f32), sds(shape, bf16), sds((1, 1), f32)),
        in_specs=[VM] * 6,
        out_specs=(VM,) * 4 + (SM,),
        compiler_params=params(4),
        name="update",
    )(packed, loss, slot_piece, master_t, first_t, second_t)

    def back(v):
        return jnp.transpose(v, (2, 0, 1))

    return mean_loss[0, 0], back(new_master), back(new_first), back(new_second), back(low)


def solution(mesh):
    in_specs = (
        P(("grp", "col"), None),
        P("grp", None, None),
        P("grp", None, None),
        P("grp"),
        P("grp"),
        P(("grp", "col")),
        P(("grp", "col")),
        P(),
        P("grp", None, "col"),
        P("grp", None, "col"),
        P("grp", None, "col"),
    )
    out_specs = (
        P(),
        P("grp", None, "col"),
        P("grp", None, "col"),
        P("grp", None, "col"),
        P("grp", None, "col"),
    )
    return jax.shard_map(body, mesh=mesh, in_specs=in_specs, out_specs=out_specs, check_vma=False)
```

```python
import functools
import jax
import jax.numpy as jnp
from jax import lax
from jax.experimental import pallas as pl
from jax.experimental.pallas import tpu as pltpu
from jax.sharding import PartitionSpec as P

F = 256
HID = 256
CLS = 64
B = 256
PR = 2
STEP = 7
PROWS = 834
TROWS = 848
HALF = 128
UNROLL = 8

learn_rate = 0.01
beta_one = 0.5
beta_two = 0.5
adam_epsilon = 1e-08
decay_rate = 0.1

f32 = jnp.float32
bf16 = jnp.bfloat16
MESH = pl.DeviceIdType.MESH
VM = pl.BlockSpec(memory_space=pltpu.VMEM)
SM = pl.BlockSpec(memory_space=pltpu.SMEM)
HBM = pl.BlockSpec(memory_space=pltpu.HBM)


def sds(shape, dtype):
    return jax.ShapeDtypeStruct(shape, dtype)


def dot_nn(a, b):
    return lax.dot_general(a, b, (((1,), (0,)), ((), ())), preferred_element_type=f32)


def dot_nt(a, b):
    return lax.dot_general(a, b, (((1,), (1,)), ((), ())), preferred_element_type=f32)


def dot_tn(a, b):
    return lax.dot_general(a, b, (((0,), (0,)), ((), ())), preferred_element_type=f32)


def column_of(rows16, row):
    pick = (lax.broadcasted_iota(jnp.int32, (16, HALF), 0) == row).astype(bf16)
    return dot_tn(rows16, pick)


def place():
    g = lax.axis_index("grp")
    q = lax.axis_index("col")
    k = q % 2
    x = q // 2
    partner = q + 1 - 2 * k
    across = q + 2 - 4 * x
    return g, q, k, x, partner, across


def sigmoid(v):
    return jax.nn.sigmoid(v)


def remote(src, dst, send, recv, dev):
    return pltpu.make_async_remote_copy(
        src_ref=src, dst_ref=dst, send_sem=send, recv_sem=recv, device_id=dev, device_id_type=MESH
    )


def enter(ng, g, q, others):
    barrier = pltpu.get_barrier_semaphore()
    line, last = g // 2, ng // 2 - 1
    for c in others:
        pl.semaphore_signal(barrier, inc=1, device_id=(g, c), device_id_type=MESH)
    pair = g + 1 - 2 * (g % 2)
    pl.semaphore_signal(barrier, inc=1, device_id=(pair, q), device_id_type=MESH)

    @pl.when(line > 0)
    def _():
        pl.semaphore_signal(barrier, inc=1, device_id=(g - 2, q), device_id_type=MESH)

    @pl.when(line < last)
    def _():
        pl.semaphore_signal(barrier, inc=1, device_id=(g + 2, q), device_id_type=MESH)

    ends = jnp.minimum(line, 1) + jnp.minimum(last - line, 1)
    return lambda: pl.semaphore_wait(barrier, len(others) + 1 + ends)


def all_in(ng, g, q, up, down):
    line, last = g // 2, ng // 2 - 1

    @pl.when(line == last)
    def _():
        @pl.when(line > 0)
        def _():
            pl.semaphore_signal(down, inc=1, device_id=(g - 2, q), device_id_type=MESH)

    @pl.when(line > 0)
    def _():
        pl.semaphore_wait(up, 1)

    @pl.when(line < last)
    def _():
        pl.semaphore_signal(up, inc=1, device_id=(g + 2, q), device_id_type=MESH)
        pl.semaphore_wait(down, 1)

        @pl.when(line > 0)
        def _():
            pl.semaphore_signal(down, inc=1, device_id=(g - 2, q), device_id_type=MESH)


def gather_kernel(
    ng,
    feat,
    master,
    pieces,
    labels,
    mask,
    pairs,
    degree,
    adj,
    tcount,
    tiles,
    fbuf,
    enc,
    table,
    wtrans,
    srow,
    marks,
    inverse,
    lists,
    mbuf,
    pcs,
    lab,
    msk,
    prs,
    deg,
    lbuf,
    wmsg,
    pmsg,
    wbuf,
    hot,
    up,
    down,
    local_sem,
    tile_sem,
    small_sem,
    mark_sem,
    ws_core,
    ws_x,
    ws_send,
    ws_recv,
    wr_send,
    wr_recv,
    xs_send,
    xs_recv,
    en_send,
    en_recv,
):
    g, q, k, x, partner, across = place()
    rows = feat.shape[0]
    blocks = rows // B
    sp = wmsg.shape[1]
    slots = pieces.shape[1]
    count = pairs.shape[2]
    tpad = lists.shape[1]
    width = master.shape[1]

    load = pltpu.make_async_copy(feat, fbuf.at[x], local_sem)
    load.start()
    small = [
        pltpu.make_async_copy(a, b, small_sem.at[i])
        for i, (a, b) in enumerate(
            [
                (master, mbuf),
                (pieces, pcs),
                (labels, lab),
                (mask, msk),
                (pairs, prs),
                (degree.at[k], deg.at[0]),
                (degree.at[2 + k], deg.at[1]),
            ]
        )
    ]
    for copy in small:
        copy.start()

    entered = enter(ng, g, q, (across, partner))
    for copy in small:
        copy.wait()
    for j in range(PR):
        cols = jnp.concatenate(
            [mbuf[j], jnp.zeros((width, HALF - slots), f32)], axis=1
        )
        turned = jnp.transpose(jnp.concatenate([cols, jnp.zeros_like(cols)], axis=0))
        other = pltpu.roll(turned, width, 1)
        wmsg[j] = jnp.where(k == 0, turned, other)[:sp].astype(bf16)
    marks[x] = jnp.where(msk[...] > 0, lab[...], -1)
    entered()

    first = remote(wmsg, pmsg, ws_core.at[0], ws_core.at[1], (g, partner))
    first.start()
    mark_copy = remote(marks.at[x], marks.at[x], mark_sem.at[0], mark_sem.at[1], (g, across))
    mark_copy.start()
    load.wait()

    def cross(i):
        piece = fbuf.at[x, pl.ds(pl.multiple_of(i * B, B), B)]
        return remote(piece, piece, xs_send.at[i], xs_recv.at[i], (g, across))

    cross(0).start()
    first.wait()
    wbuf[k, g, x] = wmsg[k] + pmsg[k]
    second = remote(wbuf.at[k, g, x], wbuf.at[k, g, x], ws_x.at[0], ws_x.at[1], (g, across))
    second.start()

    def cross_all(i, c):
        cross(i).start()
        return c

    lax.fori_loop(1, blocks, cross_all, 0)
    fetch = pltpu.make_async_copy(adj, tiles, tile_sem)
    fetch.start()
    all_in(ng, g, q, up, down)
    second.wait()

    def to_group(d):
        return remote(
            wbuf.at[k, g], wbuf.at[k, g], ws_send.at[d], ws_recv.at[d], ((g + d) % ng, q)
        )

    def from_group(d):
        src = (g + ng - d) % ng
        return remote(wbuf.at[k, src], wbuf.at[k, src], ws_send.at[d], ws_recv.at[d], (src, q))

    def hand_over(d):
        src = (g + ng - d) % ng
        return remote(
            wbuf.at[k, src], wbuf.at[k, src], wr_send.at[d], wr_recv.at[d], (g, partner)
        )

    def handed(d):
        src = (g + ng - d) % ng
        return remote(
            wbuf.at[1 - k, src], wbuf.at[1 - k, src], wr_send.at[d], wr_recv.at[d], (g, partner)
        )

    def send_group(d, c):
        to_group(d).start()
        return c

    lax.fori_loop(1, ng, send_group, 0)
    hand_over(0).start()

    shift = blocks.bit_length() - 1
    fill = jnp.zeros((2, tpad - count), jnp.int32)
    both = jnp.concatenate([prs[0], fill], axis=1)
    rvec = both[0:1]
    cvec = both[1:2]
    tvec = lax.broadcasted_iota(jnp.int32, (1, tpad), 1)
    live = tvec < tcount[0]

    def split(v):
        quarter = lax.shift_right_logical(v, shift)
        local = lax.shift_right_logical(quarter, 1) * blocks + (v & (blocks - 1))
        return (quarter & 1) == k, local

    fmine, frow = split(rvec)
    bmine, bcol = split(cvec)
    fmine = fmine & live
    bmine = bmine & live
    upto = (
        lax.broadcasted_iota(jnp.int32, (tpad, tpad), 0)
        <= lax.broadcasted_iota(jnp.int32, (tpad, tpad), 1)
    ).astype(bf16)
    order = lax.broadcasted_iota(jnp.int32, (tpad, tpad), 0)
    zero = jnp.zeros((1, tpad), jnp.int32)

    def compact(mine, one, two):
        flag = mine.astype(f32)
        seen = dot_nn(jnp.broadcast_to(flag, (8, tpad)).astype(bf16), upto)[0:1].astype(jnp.int32)
        spot = jnp.where(mine, seen - 1, -1)
        chosen = (order == spot).astype(f32).astype(bf16)
        values = jnp.concatenate([tvec, one, two, zero, zero, zero, zero, zero], axis=0)
        packed = dot_nt(values.astype(f32).astype(bf16), chosen).astype(jnp.int32)
        total = jnp.sum(flag, axis=1, keepdims=True).astype(jnp.int32)
        past = tvec >= total
        return packed[0:1], jnp.where(past, 2 * blocks, packed[1:2]), packed[2:3], zero + total

    ft, fr, fc, fn = compact(fmine, frow, cvec)
    bt, bc, br, bn = compact(bmine, bcol, rvec)
    lbuf[...] = jnp.concatenate([ft, fr, fc, bt, bc, br, fn, bn], axis=0)
    put = pltpu.make_async_copy(lbuf, lists, local_sem)
    put.start()
    inverse[...] = 1.0 / deg[...].astype(f32)

    lanes = ng * sp
    piece = jnp.concatenate([pcs[...], jnp.full((ng, HALF - slots), -1, jnp.int32)], axis=1)
    high = lax.shift_right_logical(piece + 1, 4).astype(f32).astype(bf16)
    low = ((piece + 1) & 15).astype(f32).astype(bf16)
    lane = lax.broadcasted_iota(jnp.int32, (1, lanes), 1)
    owner = jnp.floor((lane.astype(f32) + 0.5) * (1.0 / sp)).astype(jnp.int32)
    within = lane - owner * sp
    pick = (lax.broadcasted_iota(jnp.int32, (HALF, lanes), 0) == within).astype(f32).astype(bf16)
    wide = dot_nn(high, pick) * 16.0 + dot_nn(low, pick)
    keep = lax.broadcasted_iota(jnp.int32, (ng, lanes), 0) == owner
    flat = jnp.sum(jnp.where(keep, wide, 0.0), axis=0, keepdims=True).astype(jnp.int32) - 1
    line = lax.broadcasted_iota(jnp.int32, (TROWS, lanes), 0)
    for j in range(PR):
        at = jnp.where(flat >= 0, flat * PR + j, -1)
        srow[:, j * lanes : (j + 1) * lanes] = at
        hot[:, j * lanes : (j + 1) * lanes] = (line == at).astype(f32).astype(bf16)

    def pass_on(d, c):
        from_group(d).wait_recv()
        hand_over(d).start()
        return c

    lax.fori_loop(1, ng, pass_on, 0)

    def take(d, c):
        handed(d).wait_recv()
        return c

    lax.fori_loop(0, ng, take, 0)

    left = wbuf[:, :, 0].reshape(2 * ng * sp, HALF)
    right = wbuf[:, :, 1].reshape(2 * ng * sp, HALF)
    full = dot_nn(hot[...], jnp.concatenate([left, right], axis=1))
    table[...] = full.astype(bf16)
    for i in range(3):
        wtrans[i] = jnp.transpose(full[i * B : (i + 1) * B]).astype(bf16)
    bias = column_of(table[PROWS - 2 : PROWS + 14], 0)

    def share(i, core):
        away = i // blocks
        quarter = (x + away * (1 - 2 * x)) * 2 + core
        piece = enc.at[quarter * blocks + i % blocks]
        return remote(piece, piece, en_send.at[i], en_recv.at[i], (g, partner))

    def encode(i, many):
        away = i // blocks
        side = x + away * (1 - 2 * x)
        base = i % blocks
        piece = fbuf[side, pl.ds(pl.multiple_of(base * B, B), many * B)]
        pre = dot_nt(wtrans[0], piece) + jnp.concatenate([bias] * (2 * many), axis=1)
        out = (pre * sigmoid(pre)).astype(bf16)
        at = (side * 2 + k) * blocks + base
        for n in range(many):
            enc[at + n] = out[:, n * B : (n + 1) * B]
        for n in range(many):
            share(i + n, k).start()

    def own(i, c):
        encode(i * 4, 4)
        return c

    lax.fori_loop(0, blocks // 4, own, 0)

    def crossed(i):
        piece = fbuf.at[1 - x, pl.ds(pl.multiple_of(i * B, B), B)]
        return remote(piece, piece, xs_send.at[i], xs_recv.at[i], (g, across))

    def far_block(i, c):
        crossed(i).wait_recv()
        encode(blocks + i, 1)
        return c

    lax.fori_loop(0, blocks, far_block, 0)

    def settle(i, c):
        for n in (i, blocks + i):
            share(n, 1 - k).wait_recv()
            share(n, k).wait_send()
        cross(i).wait_send()
        return c

    lax.fori_loop(0, blocks, settle, 0)
    mark_copy.wait()

    def drain_group(d, c):
        to_group(d).wait_send()
        hand_over(d).wait_send()
        return c

    lax.fori_loop(1, ng, drain_group, 0)
    hand_over(0).wait_send()
    put.wait()
    fetch.wait()


def each_tile(count, use):
    def step(i, c):
        for u in range(UNROLL):
            use(i * UNROLL + u)
        return c

    lax.fori_loop(0, (count + UNROLL - 1) // UNROLL, step, 0)


def forward_kernel(lists, tiles, enc, inverse, mean, acc):
    local = mean.shape[0]
    blocks = local // 2

    def use(j):
        acc[lists[1, j]] += dot_nt(enc[lists[2, j]], tiles[lists[0, j]])

    def clear(i, c):
        acc[i] = jnp.zeros((B, B), f32)
        return c

    lax.fori_loop(0, local + 1, clear, 0)
    each_tile(lists[6, 0], use)

    def finish(i, c):
        scale = inverse[i // blocks, :, pl.ds(pl.multiple_of((i % blocks) * B, B), B)]
        mean[i] = (acc[i] * scale).astype(bf16)
        return c

    lax.fori_loop(0, local, finish, 0)


def sage_kernel(
    enc,
    mean,
    table,
    wtrans,
    marks,
    inverse,
    sums,
    self_back,
    self_grad,
    neigh_grad,
    head_grad,
    bias_grad,
    stats,
    sage,
    hid,
    lgrad,
    send,
    recv,
):
    g, q, k, x, partner, across = place()
    local = mean.shape[0]
    blocks = local // 2
    width = 2 * B
    steps = local // 2
    barrier = pltpu.get_barrier_semaphore()
    pl.semaphore_signal(barrier, inc=1, device_id=(g, partner), device_id_type=MESH)
    pl.semaphore_wait(barrier, 1)
    half = pl.ds(pl.multiple_of(x * HALF, HALF), HALF)
    head = table[F + 2 * HID : F + 2 * HID + CLS]
    bias = column_of(table[PROWS - 2 : PROWS + 14], 1)
    bias = jnp.concatenate([bias] * 4, axis=1)
    neigh_half = table[pl.ds(pl.multiple_of(F + HID + x * HALF, HALF), HALF)]
    self_half = table[pl.ds(pl.multiple_of(F + x * HALF, HALF), HALF)]
    stats[...] = jnp.zeros_like(stats)

    def slot(i, core):
        return (i // (steps // 2)) * 2 * blocks + core * blocks + (i % (steps // 2)) * 2

    def exchange(i, core):
        piece = sums.at[pl.ds(slot(i, core), 2)]
        return pltpu.make_async_remote_copy(
            src_ref=piece,
            dst_ref=piece,
            send_sem=send.at[i],
            recv_sem=recv.at[i],
            device_id=(g, partner),
            device_id_type=MESH,
        )

    def step(i, c):
        at = slot(i, k)
        e = jnp.concatenate([enc[at], enc[at + 1]], axis=1)
        m = jnp.concatenate([mean[2 * i], mean[2 * i + 1]], axis=1)
        pre = dot_nn(wtrans[1], e) + dot_nn(wtrans[2], m) + bias
        sig = sigmoid(pre)
        hidden = (pre * sig).astype(bf16)
        logits = dot_nn(head, hidden)
        top = jnp.max(logits, axis=0, keepdims=True)
        expd = jnp.exp(logits - top)
        total = jnp.sum(expd, axis=0, keepdims=True)
        cols = pl.ds(pl.multiple_of((i % (steps // 2)) * width, width), width)
        mark = marks[i // (steps // 2), :, cols]
        valid = (mark >= 0).astype(f32)
        onehot = (lax.broadcasted_iota(jnp.int32, (CLS, width), 0) == mark).astype(f32)
        target = jnp.sum(logits * onehot, axis=0, keepdims=True)
        loss = valid * (top + jnp.log(total) - target)
        stats[0:1, :] += loss
        stats[1:2, :] += valid
        grad = ((expd * (1.0 / total) - onehot) * valid).astype(bf16)
        back = dot_tn(head, grad) * (sig * (1.0 + pre * (1.0 - sig)))
        sgrad = back.astype(bf16)
        scale = inverse[i // (steps // 2), :, cols]
        out = (dot_nn(neigh_half, sgrad) * scale).astype(bf16)
        for b in range(2):
            lanes = slice(b * B, (b + 1) * B)
            sums[at + b] = out[:, lanes]
            sage[2 * i + b] = sgrad[:, lanes]
            hid[2 * i + b] = jnp.where(x == 0, hidden[:HALF, lanes], hidden[HALF:, lanes])
            lgrad[2 * i + b] = grad[:, lanes]
        exchange(i, k).start()
        return c

    lax.fori_loop(0, steps, step, 0)

    ones = jnp.ones((B, HALF), bf16)
    sg = ng_ = hg = bg = None
    for b in range(local):
        at = (b // blocks) * 2 * blocks + k * blocks + b % blocks
        s = sage[b, half]
        t1 = dot_nt(s, enc[at])
        t2 = dot_nt(s, mean[b])
        t3 = dot_nt(lgrad[b], hid[b])
        t4 = dot_nn(s, ones)
        sg = t1 if sg is None else sg + t1
        ng_ = t2 if ng_ is None else ng_ + t2
        hg = t3 if hg is None else hg + t3
        bg = t4 if bg is None else bg + t4
        self_back[b] = dot_nn(self_half, sage[b])
    self_grad[...] = sg
    neigh_grad[...] = ng_
    head_grad[...] = hg
    bias_grad[...] = bg

    def done(i, c):
        exchange(i, 1 - k).wait_recv()
        exchange(i, k).wait_send()
        return c

    lax.fori_loop(0, steps, done, 0)


def backward_kernel(lists, tiles, sums, self_back, fbuf, table, wtrans, enc_grad, bias_grad, acc):
    x = lax.axis_index("col") // 2
    local = self_back.shape[0]
    blocks = local // 2

    def use(j):
        acc[lists[4, j]] += dot_nn(sums[lists[5, j]], tiles[lists[3, j]])

    def clear(i, c):
        acc[i] = jnp.zeros((HALF, B), f32)
        return c

    lax.fori_loop(0, local + 1, clear, 0)
    each_tile(lists[7, 0], use)
    half = pl.ds(pl.multiple_of(x * HALF, HALF), HALF)
    wide = column_of(table[PROWS - 2 : PROWS + 14, half], 0)
    wide = jnp.concatenate([wide, wide], axis=1)
    weight = wtrans[0, half]
    eg = bg = None
    for b in range(local):
        piece = fbuf[b // blocks, (b % blocks) * B : (b % blocks + 1) * B]
        pre = dot_nt(weight, piece) + wide
        sig = sigmoid(pre)
        grad = ((self_back[b] + acc[b]) * (sig * (1.0 + pre * (1.0 - sig)))).astype(bf16)
        t1 = dot_nn(grad, piece)
        gf = grad.astype(f32)
        t2 = gf[:, :HALF] + gf[:, HALF:]
        eg = t1 if eg is None else eg + t1
        bg = t2 if bg is None else bg + t2
    enc_grad[...] = eg
    bias_grad[...] = bg


def reduce_kernel(
    ng,
    enc_grad,
    benc_grad,
    self_grad,
    neigh_grad,
    head_grad,
    bsage_grad,
    srow,
    stats,
    slot_grad,
    loss,
    gtab,
    rtab,
    qbuf,
    inbox,
    sbuf,
    srecv,
    sbox,
    up,
    down,
    core_sem,
    stat_sem,
    g_send,
    g_recv,
    s_send,
    s_recv,
):
    g, q, k, x, partner, across = place()
    entered = enter(ng, g, q, (partner,))
    sp = inbox.shape[1]
    slots = ng * sp

    both = jnp.sum(stats[...], axis=1, keepdims=True)
    sbuf[...] = jnp.broadcast_to(both, sbuf.shape)
    gtab[0:B] = jnp.transpose(enc_grad[...]).astype(bf16)
    gtab[B : 2 * B] = jnp.transpose(self_grad[...]).astype(bf16)
    gtab[2 * B : 3 * B] = jnp.transpose(neigh_grad[...]).astype(bf16)
    gtab[3 * B : 3 * B + CLS] = head_grad[...].astype(bf16)
    tail = lax.broadcasted_iota(jnp.int32, (16, HALF), 0)
    row_one = jnp.sum(jnp.transpose(benc_grad[...]), axis=0, keepdims=True)
    row_two = jnp.transpose(bsage_grad[...])[0:1]
    last = jnp.where(tail == 0, row_one, jnp.where(tail == 1, row_two, 0.0))
    gtab[PROWS - 2 : PROWS + 14] = last.astype(bf16)
    entered()
    one = remote(gtab, rtab, core_sem.at[0], core_sem.at[1], (g, partner))
    one.start()
    two = remote(sbuf, srecv, stat_sem.at[0], stat_sem.at[1], (g, partner))
    two.start()
    all_in(ng, g, q, up, down)
    one.wait()
    two.wait()
    sbox[g] = sbuf[...] + srecv[...]

    def stat_out(d):
        to = (g + d) % ng
        return remote(sbox.at[g], sbox.at[g], s_send.at[d], s_recv.at[d], (to, q))

    def stat_got(d):
        src = (g + ng - d) % ng
        return remote(sbox.at[src], sbox.at[src], s_send.at[d], s_recv.at[d], (src, q))

    def start_stat(d, c):
        stat_out(d).start()
        return c

    lax.fori_loop(1, ng, start_stat, 0)

    whole = gtab[...].astype(f32) + rtab[...].astype(f32)
    rolled = pltpu.roll(whole, HALF // 2, 1)
    low = lax.broadcasted_iota(jnp.int32, (TROWS, HALF), 1) < HALF // 2
    line = lax.broadcasted_iota(jnp.int32, (TROWS, slots), 0)
    even = jnp.where(low, jnp.where(k == 0, whole, rolled), 0.0).astype(bf16)
    odd = jnp.where(low, 0.0, jnp.where(k == 0, rolled, whole)).astype(bf16)
    hot_even = (line == srow[:, :slots]).astype(f32).astype(bf16)
    hot_odd = (line == srow[:, slots:]).astype(f32).astype(bf16)
    spread = dot_tn(hot_even, even) + dot_tn(hot_odd, odd)
    qbuf[...] = spread.astype(bf16).reshape(ng, sp, HALF)

    def out(d):
        to = (g + d) % ng
        return remote(qbuf.at[to], inbox.at[g], g_send.at[d], g_recv.at[d], (to, q))

    def got(d):
        src = (g + ng - d) % ng
        return remote(qbuf.at[src], inbox.at[src], g_send.at[d], g_recv.at[d], (src, q))

    def start(d, c):
        out(d).start()
        return c

    lax.fori_loop(1, ng, start, 0)
    inbox[g] = qbuf[g]

    def arrive(d, c):
        stat_got(d).wait_recv()
        got(d).wait_recv()
        return c

    lax.fori_loop(1, ng, arrive, 0)

    def add_stat(i, c):
        return c + sbox[i]

    sums = lax.fori_loop(0, ng, add_stat, jnp.zeros(sbuf.shape, f32))
    loss_sum = sums[0:1]
    count = sums[1:2]
    loss[...] = jnp.broadcast_to(loss_sum / count, loss.shape)

    def add(i, c):
        return c + inbox[i].astype(f32)

    total = lax.fori_loop(0, ng, add, jnp.zeros((sp, HALF), f32))
    slot_grad[...] = total / count

    def finish(d, c):
        stat_out(d).wait_send()
        out(d).wait_send()
        return c

    lax.fori_loop(1, ng, finish, 0)


def update_kernel(packed, loss, pieces, master, first, second, new_master, new_first, new_second, low, mean_loss):
    g = lax.axis_index("grp")
    slots = pieces.shape[1]
    width = master.shape[1]
    sp = packed.shape[0]
    rows = packed[...]
    if sp < HALF:
        rows = jnp.concatenate([rows, jnp.zeros((HALF - sp, HALF), f32)], axis=0)
    turned = jnp.transpose(rows)
    piece = pieces[pl.ds(g, 1), :]
    owned = piece >= 0
    for j in range(PR):
        grad = turned[j * width : (j + 1) * width, :slots]
        decay = jnp.where(piece * PR + j < PROWS - 2, decay_rate, 0.0)
        old = master[j]
        one = beta_one * first[j] + (1.0 - beta_one) * grad
        two = beta_two * second[j] + (1.0 - beta_two) * grad * grad
        one_hat = one / (1.0 - beta_one**STEP)
        two_hat = two / (1.0 - beta_two**STEP)
        new = old - learn_rate * (one_hat / (jnp.sqrt(two_hat) + adam_epsilon) + decay * old)
        new = jnp.where(owned, new, 0.0)
        new_master[j] = new
        new_first[j] = jnp.where(owned, one, 0.0)
        new_second[j] = jnp.where(owned, two, 0.0)
        low[j] = new.astype(bf16)
    mean_loss[0, 0] = loss[0, 0]


def far(v):
    return pltpu.with_memory_space_constraint(v, pltpu.HBM)


def params(limit, collective=None):
    return pltpu.CompilerParams(
        vmem_limit_bytes=limit << 20, collective_id=collective, has_side_effects=collective is not None
    )


DMA = pltpu.SemaphoreType.DMA


def body(
    features,
    adj_tiles,
    block_pairs,
    tile_count,
    degree,
    labels,
    loss_mask,
    slot_piece,
    master,
    moment_one,
    moment_two,
):
    nc = lax.axis_size("col")
    ng = lax.axis_size("grp")
    rows = features.shape[0]
    blocks = rows // B
    nb = nc * blocks
    local = 2 * blocks
    count = adj_tiles.shape[0]
    tpad = -(-count // HALF) * HALF
    slots = slot_piece.shape[1]
    sp = -(-slots // 16) * 16
    width = master.shape[2]
    master_t = jnp.transpose(master, (1, 2, 0))
    first_t = jnp.transpose(moment_one, (1, 2, 0))
    second_t = jnp.transpose(moment_two, (1, 2, 0))

    tiles, fbuf, enc, table, wtrans, srow, marks, inverse, lists = pl.pallas_call(
        functools.partial(gather_kernel, ng),
        out_shape=(
            pltpu.VMEM((count, B, B), bf16),
            pltpu.VMEM((2, rows, F), bf16),
            pltpu.VMEM((nb, HID, B), bf16),
            pltpu.VMEM((TROWS, HID), bf16),
            pltpu.VMEM((3, HID, HID), bf16),
            pltpu.VMEM((1, 2 * ng * sp), jnp.int32),
            pltpu.VMEM((2, 1, rows), jnp.int32),
            pltpu.VMEM((2, 1, rows), f32),
            sds((8, tpad), jnp.int32),
        ),
        in_specs=[HBM] * 8 + [SM],
        out_specs=(VM,) * 8 + (HBM,),
        scratch_shapes=[
            pltpu.VMEM((PR, width, slots), f32),
            pltpu.VMEM((ng, slots), jnp.int32),
            pltpu.VMEM((1, rows), jnp.int32),
            pltpu.VMEM((1, rows), jnp.int32),
            pltpu.VMEM((1, 2, count), jnp.int32),
            pltpu.VMEM((2, 1, rows), jnp.int32),
            pltpu.VMEM((8, tpad), jnp.int32),
            pltpu.VMEM((2, sp, HALF), bf16),
            pltpu.VMEM((2, sp, HALF), bf16),
            pltpu.VMEM((2, ng, 2, sp, HALF), bf16),
            pltpu.VMEM((TROWS, 2 * ng * sp), bf16),
            pltpu.SemaphoreType.REGULAR,
            pltpu.SemaphoreType.REGULAR,
            DMA,
            DMA,
            DMA((7,)),
            DMA((2,)),
            DMA((2,)),
            DMA((2,)),
            DMA((ng,)),
            DMA((ng,)),
            DMA((ng,)),
            DMA((ng,)),
            DMA((blocks,)),
            DMA((blocks,)),
            DMA((2 * blocks,)),
            DMA((2 * blocks,)),
        ],
        compiler_params=params(6, 0),
        name="gather",
    )(
        far(features),
        far(master_t),
        far(slot_piece),
        far(labels.reshape(1, rows)),
        far(loss_mask.reshape(1, rows)),
        far(jnp.transpose(block_pairs, (0, 2, 1))),
        far(degree.reshape(nc, 1, rows)),
        far(adj_tiles),
        tile_count,
    )

    mean = pl.pallas_call(
        forward_kernel,
        out_shape=pltpu.VMEM((local, HID, B), bf16),
        in_specs=[SM, VM, VM, VM],
        out_specs=VM,
        scratch_shapes=[pltpu.VMEM((local + 1, HID, B), f32)],
        compiler_params=params(7),
        name="forward",
    )(lists, tiles, enc, inverse)

    sums, self_back, self_grad, neigh_grad, head_grad, bsage, stats = pl.pallas_call(
        sage_kernel,
        out_shape=(
            pltpu.VMEM((nb, HALF, B), bf16),
            pltpu.VMEM((local, HALF, B), f32),
            pltpu.VMEM((HALF, HID), f32),
            pltpu.VMEM((HALF, HID), f32),
            pltpu.VMEM((CLS, HALF), f32),
            pltpu.VMEM((HALF, HALF), f32),
            pltpu.VMEM((8, 2 * B), f32),
        ),
        in_specs=[VM] * 6,
        out_specs=(VM,) * 7,
        scratch_shapes=[
            pltpu.VMEM((local, HID, B), bf16),
            pltpu.VMEM((local, HALF, B), bf16),
            pltpu.VMEM((local, CLS, B), bf16),
            DMA((blocks,)),
            DMA((blocks,)),
        ],
        compiler_params=params(8, 1),
        name="sage",
    )(enc, mean, table, wtrans, marks, inverse)

    enc_grad, benc = pl.pallas_call(
        backward_kernel,
        out_shape=(pltpu.VMEM((HALF, F), f32), pltpu.VMEM((HALF, HALF), f32)),
        in_specs=[SM, VM, VM, VM, VM, VM, VM],
        out_specs=(VM,) * 2,
        scratch_shapes=[pltpu.VMEM((local + 1, HALF, B), f32)],
        compiler_params=params(6),
        name="backward",
    )(lists, tiles, sums, self_back, fbuf, table, wtrans)

    packed, loss = pl.pallas_call(
        functools.partial(reduce_kernel, ng),
        out_shape=(pltpu.VMEM((sp, HALF), f32), pltpu.VMEM((8, HALF), f32)),
        in_specs=[VM] * 8,
        out_specs=(VM,) * 2,
        scratch_shapes=[
            pltpu.VMEM((TROWS, HALF), bf16),
            pltpu.VMEM((TROWS, HALF), bf16),
            pltpu.VMEM((ng, sp, HALF), bf16),
            pltpu.VMEM((ng, sp, HALF), bf16),
            pltpu.VMEM((8, HALF), f32),
            pltpu.VMEM((8, HALF), f32),
            pltpu.VMEM((ng, 8, HALF), f32),
            pltpu.SemaphoreType.REGULAR,
            pltpu.SemaphoreType.REGULAR,
            DMA((2,)),
            DMA((2,)),
            DMA((ng,)),
            DMA((ng,)),
            DMA((ng,)),
            DMA((ng,)),
        ],
        compiler_params=params(12, 2),
        name="reduce",
    )(enc_grad, benc, self_grad, neigh_grad, head_grad, bsage, srow, stats)

    shape = (PR, width, slots)
    new_master, new_first, new_second, low, mean_loss = pl.pallas_call(
        update_kernel,
        out_shape=(sds(shape, f32), sds(shape, f32), sds(shape, f32), sds(shape, bf16), sds((1, 1), f32)),
        in_specs=[VM] * 6,
        out_specs=(VM,) * 4 + (SM,),
        compiler_params=params(4),
        name="update",
    )(packed, loss, slot_piece, master_t, first_t, second_t)

    def back(v):
        return jnp.transpose(v, (2, 0, 1))

    return mean_loss[0, 0], back(new_master), back(new_first), back(new_second), back(low)


def solution(mesh):
    in_specs = (
        P(("grp", "col"), None),
        P("grp", None, None),
        P("grp", None, None),
        P("grp"),
        P("grp"),
        P(("grp", "col")),
        P(("grp", "col")),
        P(),
        P("grp", None, "col"),
        P("grp", None, "col"),
        P("grp", None, "col"),
    )
    out_specs = (
        P(),
        P("grp", None, "col"),
        P("grp", None, "col"),
        P("grp", None, "col"),
        P("grp", None, "col"),
    )
    return jax.shard_map(body, mesh=mesh, in_specs=in_specs, out_specs=out_specs, check_vma=False)
```

```python
import functools
import jax
import jax.numpy as jnp
from jax import lax
from jax.experimental import pallas as pl
from jax.experimental.pallas import tpu as pltpu
from jax.sharding import PartitionSpec as P

F = 256
HID = 256
CLS = 64
B = 256
PR = 2
STEP = 7
PROWS = 834
TROWS = 848
HALF = 128
WIDE = 8

learn_rate = 0.01
beta_one = 0.5
beta_two = 0.5
adam_epsilon = 1e-08
decay_rate = 0.1

f32 = jnp.float32
bf16 = jnp.bfloat16
MESH = pl.DeviceIdType.MESH
VM = pl.BlockSpec(memory_space=pltpu.VMEM)
SM = pl.BlockSpec(memory_space=pltpu.SMEM)
HBM = pl.BlockSpec(memory_space=pltpu.HBM)


def sds(shape, dtype):
    return jax.ShapeDtypeStruct(shape, dtype)


def dot_nn(a, b):
    return lax.dot_general(a, b, (((1,), (0,)), ((), ())), preferred_element_type=f32)


def dot_nt(a, b):
    return lax.dot_general(a, b, (((1,), (1,)), ((), ())), preferred_element_type=f32)


def dot_tn(a, b):
    return lax.dot_general(a, b, (((0,), (0,)), ((), ())), preferred_element_type=f32)


def column_of(rows16, row):
    pick = (lax.broadcasted_iota(jnp.int32, (16, HALF), 0) == row).astype(bf16)
    return dot_tn(rows16, pick)


def place():
    g = lax.axis_index("grp")
    q = lax.axis_index("col")
    k = q % 2
    x = q // 2
    partner = q + 1 - 2 * k
    across = q + 2 - 4 * x
    return g, q, k, x, partner, across


def sigmoid(v):
    return jax.nn.sigmoid(v)


def remote(src, dst, send, recv, dev):
    return pltpu.make_async_remote_copy(
        src_ref=src, dst_ref=dst, send_sem=send, recv_sem=recv, device_id=dev, device_id_type=MESH
    )


def enter(ng, g, q, others):
    barrier = pltpu.get_barrier_semaphore()
    line, last = g // 2, ng // 2 - 1
    for c in others:
        pl.semaphore_signal(barrier, inc=1, device_id=(g, c), device_id_type=MESH)
    pair = g + 1 - 2 * (g % 2)
    pl.semaphore_signal(barrier, inc=1, device_id=(pair, q), device_id_type=MESH)

    @pl.when(line > 0)
    def _():
        pl.semaphore_signal(barrier, inc=1, device_id=(g - 2, q), device_id_type=MESH)

    @pl.when(line < last)
    def _():
        pl.semaphore_signal(barrier, inc=1, device_id=(g + 2, q), device_id_type=MESH)

    ends = jnp.minimum(line, 1) + jnp.minimum(last - line, 1)
    return lambda: pl.semaphore_wait(barrier, len(others) + 1 + ends)


def all_in(ng, g, q, up, down):
    line, last = g // 2, ng // 2 - 1

    @pl.when(line == last)
    def _():
        @pl.when(line > 0)
        def _():
            pl.semaphore_signal(down, inc=1, device_id=(g - 2, q), device_id_type=MESH)

    @pl.when(line > 0)
    def _():
        pl.semaphore_wait(up, 1)

    @pl.when(line < last)
    def _():
        pl.semaphore_signal(up, inc=1, device_id=(g + 2, q), device_id_type=MESH)
        pl.semaphore_wait(down, 1)

        @pl.when(line > 0)
        def _():
            pl.semaphore_signal(down, inc=1, device_id=(g - 2, q), device_id_type=MESH)


def gather_kernel(
    ng,
    feat,
    master,
    pieces,
    labels,
    mask,
    pairs,
    degree,
    adj,
    tcount,
    tiles,
    fbuf,
    enc,
    table,
    wtrans,
    srow,
    marks,
    inverse,
    lists,
    mbuf,
    pcs,
    lab,
    msk,
    prs,
    deg,
    lbuf,
    wmsg,
    pmsg,
    wbuf,
    hot,
    up,
    down,
    local_sem,
    put_sem,
    tile_sem,
    small_sem,
    mark_sem,
    ws_core,
    ws_x,
    ws_send,
    ws_recv,
    wr_send,
    wr_recv,
    xs_send,
    xs_recv,
    en_send,
    en_recv,
):
    g, q, k, x, partner, across = place()
    rows = feat.shape[0]
    blocks = rows // B
    sp = wmsg.shape[1]
    slots = pieces.shape[1]
    count = pairs.shape[2]
    tpad = lists.shape[1]
    width = master.shape[1]

    load = pltpu.make_async_copy(feat, fbuf.at[x], local_sem)
    load.start()
    small = [
        pltpu.make_async_copy(a, b, small_sem.at[i])
        for i, (a, b) in enumerate(
            [
                (master, mbuf),
                (pieces, pcs),
                (labels, lab),
                (mask, msk),
                (pairs, prs),
                (degree.at[k], deg.at[0]),
                (degree.at[2 + k], deg.at[1]),
            ]
        )
    ]
    for copy in small:
        copy.start()

    entered = enter(ng, g, q, (across, partner))
    def cross(i):
        at = pl.ds(pl.multiple_of(i * B, B), B)
        return remote(feat.at[at], fbuf.at[x, at], xs_send.at[i], xs_recv.at[i], (g, across))

    entered()
    cross(0).start()
    cross(1).start()
    for copy in small:
        copy.wait()
    for j in range(PR):
        cols = jnp.concatenate(
            [mbuf[j], jnp.zeros((width, HALF - slots), f32)], axis=1
        )
        turned = jnp.transpose(jnp.concatenate([cols, jnp.zeros_like(cols)], axis=0))
        other = pltpu.roll(turned, width, 1)
        wmsg[j] = jnp.where(k == 0, turned, other)[:sp].astype(bf16)
    first = remote(wmsg, pmsg, ws_core.at[0], ws_core.at[1], (g, partner))
    first.start()
    marks[x] = jnp.where(msk[...] > 0, lab[...], -1)
    mark_copy = remote(marks.at[x], marks.at[x], mark_sem.at[0], mark_sem.at[1], (g, across))
    mark_copy.start()
    first.wait()
    wbuf[k, g, x] = wmsg[k] + pmsg[k]
    second = remote(wbuf.at[k, g, x], wbuf.at[k, g, x], ws_x.at[0], ws_x.at[1], (g, across))
    second.start()

    def cross_all(i, c):
        cross(i).start()
        return c

    lax.fori_loop(2, blocks, cross_all, 0)
    fetch = pltpu.make_async_copy(adj, tiles, tile_sem)
    fetch.start()
    all_in(ng, g, q, up, down)
    second.wait()

    def to_group(d):
        return remote(
            wbuf.at[k, g], wbuf.at[k, g], ws_send.at[d], ws_recv.at[d], ((g + d) % ng, q)
        )

    def from_group(d):
        src = (g + ng - d) % ng
        return remote(wbuf.at[k, src], wbuf.at[k, src], ws_send.at[d], ws_recv.at[d], (src, q))

    def hand_over(d):
        src = (g + ng - d) % ng
        return remote(
            wbuf.at[k, src], wbuf.at[k, src], wr_send.at[d], wr_recv.at[d], (g, partner)
        )

    def handed(d):
        src = (g + ng - d) % ng
        return remote(
            wbuf.at[1 - k, src], wbuf.at[1 - k, src], wr_send.at[d], wr_recv.at[d], (g, partner)
        )

    def send_group(d, c):
        to_group(d).start()
        return c

    lax.fori_loop(1, ng, send_group, 0)
    hand_over(0).start()

    shift = blocks.bit_length() - 1
    fill = jnp.zeros((2, tpad - count), jnp.int32)
    both = jnp.concatenate([prs[0], fill], axis=1)
    rvec = both[0:1]
    cvec = both[1:2]
    tvec = lax.broadcasted_iota(jnp.int32, (1, tpad), 1)
    live = tvec < tcount[0]

    def split(v):
        quarter = lax.shift_right_logical(v, shift)
        local = lax.shift_right_logical(quarter, 1) * blocks + (v & (blocks - 1))
        return (quarter & 1) == k, local

    fmine, frow = split(rvec)
    bmine, bcol = split(cvec)
    fmine = fmine & live
    bmine = bmine & live
    upto = (
        lax.broadcasted_iota(jnp.int32, (tpad, tpad), 0)
        <= lax.broadcasted_iota(jnp.int32, (tpad, tpad), 1)
    ).astype(bf16)
    order = lax.broadcasted_iota(jnp.int32, (tpad, tpad), 0)
    zero = jnp.zeros((1, tpad), jnp.int32)

    def compact(mine, one, two):
        flag = mine.astype(f32)
        seen = dot_nn(jnp.broadcast_to(flag, (8, tpad)).astype(bf16), upto)[0:1].astype(jnp.int32)
        spot = jnp.where(mine, seen - 1, -1)
        chosen = (order == spot).astype(f32).astype(bf16)
        values = jnp.concatenate([tvec, one, two, zero, zero, zero, zero, zero], axis=0)
        packed = dot_nt(values.astype(f32).astype(bf16), chosen).astype(jnp.int32)
        total = jnp.sum(flag, axis=1, keepdims=True).astype(jnp.int32)
        past = tvec >= total
        return packed[0:1], jnp.where(past, 2 * blocks, packed[1:2]), packed[2:3], zero + total

    ft, fr, fc, fn = compact(fmine, frow, cvec)
    bt, bc, br, bn = compact(bmine, bcol, rvec)
    lbuf[...] = jnp.concatenate([ft, fr, fc, bt, bc, br, fn, bn], axis=0)
    put = pltpu.make_async_copy(lbuf, lists, put_sem)
    put.start()
    inverse[...] = 1.0 / deg[...].astype(f32)

    lanes = ng * sp
    piece = jnp.concatenate([pcs[...], jnp.full((ng, HALF - slots), -1, jnp.int32)], axis=1)
    high = lax.shift_right_logical(piece + 1, 4).astype(f32).astype(bf16)
    low = ((piece + 1) & 15).astype(f32).astype(bf16)
    lane = lax.broadcasted_iota(jnp.int32, (1, lanes), 1)
    owner = jnp.floor((lane.astype(f32) + 0.5) * (1.0 / sp)).astype(jnp.int32)
    within = lane - owner * sp
    pick = (lax.broadcasted_iota(jnp.int32, (HALF, lanes), 0) == within).astype(f32).astype(bf16)
    wide = dot_nn(high, pick) * 16.0 + dot_nn(low, pick)
    keep = lax.broadcasted_iota(jnp.int32, (ng, lanes), 0) == owner
    flat = jnp.sum(jnp.where(keep, wide, 0.0), axis=0, keepdims=True).astype(jnp.int32) - 1
    line = lax.broadcasted_iota(jnp.int32, (TROWS, lanes), 0)
    for j in range(PR):
        at = jnp.where(flat >= 0, flat * PR + j, -1)
        srow[:, j * lanes : (j + 1) * lanes] = at
        hot[:, j * lanes : (j + 1) * lanes] = (line == at).astype(f32).astype(bf16)

    def pass_on(d, c):
        from_group(d).wait_recv()
        hand_over(d).start()
        return c

    lax.fori_loop(1, ng, pass_on, 0)

    def take(d, c):
        handed(d).wait_recv()
        return c

    lax.fori_loop(0, ng, take, 0)

    left = wbuf[:, :, 0].reshape(2 * ng * sp, HALF)
    right = wbuf[:, :, 1].reshape(2 * ng * sp, HALF)
    full = dot_nn(hot[...], jnp.concatenate([left, right], axis=1))
    table[...] = full.astype(bf16)
    for i in range(3):
        wtrans[i] = jnp.transpose(full[i * B : (i + 1) * B]).astype(bf16)
    bias = column_of(table[PROWS - 2 : PROWS + 14], 0)

    def share(i, core):
        away = i // blocks
        quarter = (x + away * (1 - 2 * x)) * 2 + core
        piece = enc.at[quarter * blocks + i % blocks]
        return remote(piece, piece, en_send.at[i], en_recv.at[i], (g, partner))

    def encode(i, many):
        away = i // blocks
        side = x + away * (1 - 2 * x)
        base = i % blocks
        piece = fbuf[side, pl.ds(pl.multiple_of(base * B, B), many * B)]
        pre = dot_nt(wtrans[0], piece) + jnp.concatenate([bias] * (2 * many), axis=1)
        out = (pre * sigmoid(pre)).astype(bf16)
        at = (side * 2 + k) * blocks + base
        for n in range(many):
            enc[at + n] = out[:, n * B : (n + 1) * B]
        for n in range(many):
            share(i + n, k).start()

    load.wait()

    def own(i, c):
        encode(i * 4, 4)
        return c

    lax.fori_loop(0, blocks // 4, own, 0)

    def crossed(i):
        at = pl.ds(pl.multiple_of(i * B, B), B)
        return remote(feat.at[at], fbuf.at[1 - x, at], xs_send.at[i], xs_recv.at[i], (g, across))

    def far_block(i, c):
        crossed(i).wait_recv()
        encode(blocks + i, 1)
        return c

    lax.fori_loop(0, blocks, far_block, 0)

    def settle(i, c):
        for n in (i, blocks + i):
            share(n, 1 - k).wait_recv()
            share(n, k).wait_send()
        cross(i).wait_send()
        return c

    lax.fori_loop(0, blocks, settle, 0)
    mark_copy.wait()

    def drain_group(d, c):
        to_group(d).wait_send()
        hand_over(d).wait_send()
        return c

    lax.fori_loop(1, ng, drain_group, 0)
    hand_over(0).wait_send()
    put.wait()
    fetch.wait()


def each_tile(count, use):
    def many(i, c):
        for u in range(32):
            use(i * 32 + u)
        return c

    whole = count // 32
    lax.fori_loop(0, whole, many, 0)
    done = whole * 32

    def few(i, c):
        for u in range(8):
            use(done + i * 8 + u)
        return c

    lax.fori_loop(0, (count - done + 7) // 8, few, 0)


def forward_kernel(lists, tiles, enc, inverse, mean, acc):
    local = mean.shape[0]
    blocks = local // 2

    def use(j):
        acc[lists[1, j]] += dot_nt(enc[lists[2, j]], tiles[lists[0, j]])

    def clear(i, c):
        acc[i] = jnp.zeros((B, B), f32)
        return c

    lax.fori_loop(0, local + 1, clear, 0)
    each_tile(lists[6, 0], use)

    def finish(i, c):
        scale = inverse[i // blocks, :, pl.ds(pl.multiple_of((i % blocks) * B, B), B)]
        mean[i] = (acc[i] * scale).astype(bf16)
        return c

    lax.fori_loop(0, local, finish, 0)


def sage_kernel(
    enc,
    mean,
    table,
    wtrans,
    marks,
    inverse,
    sums,
    self_back,
    self_grad,
    neigh_grad,
    head_grad,
    bias_grad,
    stats,
    sage,
    hid,
    lgrad,
    send,
    recv,
):
    g, q, k, x, partner, across = place()
    local = mean.shape[0]
    blocks = local // 2
    width = 2 * B
    steps = local // WIDE
    side = steps // 2
    barrier = pltpu.get_barrier_semaphore()
    pl.semaphore_signal(barrier, inc=1, device_id=(g, partner), device_id_type=MESH)
    head = table[F + 2 * HID : F + 2 * HID + CLS]
    bias = column_of(table[PROWS - 2 : PROWS + 14], 1)
    bias = jnp.concatenate([bias] * 4, axis=1)
    both_half = jnp.concatenate(
        [
            table[pl.ds(pl.multiple_of(F + HID + x * HALF, HALF), HALF)],
            table[pl.ds(pl.multiple_of(F + x * HALF, HALF), HALF)],
        ],
        axis=0,
    )

    def slot(i, core):
        return (i // side) * 2 * blocks + core * blocks + (i % side) * WIDE

    def exchange(i, core):
        piece = sums.at[pl.ds(slot(i, core), WIDE)]
        return remote(piece, piece, send.at[i], recv.at[i], (g, partner))

    loss_rows = jnp.zeros((1, width), f32)
    valid_rows = jnp.zeros((1, width), f32)
    bias_sum = jnp.zeros((HALF, HALF), f32)
    parts = range(WIDE // 2)
    grads = []

    def weight_grads(i):
        total = [None, None, None]
        for b in range(WIDE):
            n = i * WIDE + b
            here = (
                dot_nt(sage[n], enc[slot(i, k) + b]),
                dot_nt(sage[n], mean[n]),
                dot_nt(lgrad[n], hid[n]),
            )
            total = [h if t is None else t + h for t, h in zip(total, here)]
        for ref, t in zip((self_grad, neigh_grad, head_grad), total):
            ref[...] = t if i == 0 else ref[...] + t

    for i in range(steps):
        at = slot(i, k)
        pre, sig, hidden, grad = {}, {}, {}, {}
        for p in parts:
            e = jnp.concatenate([enc[at + 2 * p], enc[at + 2 * p + 1]], axis=1)
            n = i * WIDE + 2 * p
            m = jnp.concatenate([mean[n], mean[n + 1]], axis=1)
            pre[p] = dot_nn(wtrans[1], e) + dot_nn(wtrans[2], m) + bias
        for p in parts:
            sig[p] = sigmoid(pre[p])
            hidden[p] = (pre[p] * sig[p]).astype(bf16)
        if i > 0:
            weight_grads(i - 1)
        for p in parts:
            logits = dot_nn(head, hidden[p])
            top = jnp.max(logits, axis=0, keepdims=True)
            expd = jnp.exp(logits - top)
            total = jnp.sum(expd, axis=0, keepdims=True)
            base = (i % side) * WIDE * B + p * width
            mark = marks[i // side, :, base : base + width]
            valid = (mark >= 0).astype(f32)
            hot = lax.broadcasted_iota(jnp.int32, (CLS, width), 0) == mark
            onehot = hot.astype(f32)
            target = jnp.sum(logits * onehot, axis=0, keepdims=True)
            loss_rows = loss_rows + valid * (top + jnp.log(total) - target)
            valid_rows = valid_rows + valid
            grad[p] = ((expd * (1.0 / total) - onehot) * valid).astype(bf16)
        outs = {}
        for p in parts:
            back = dot_tn(head, grad[p]) * (sig[p] * (1.0 + pre[p] * (1.0 - sig[p])))
            sgrad = back.astype(bf16)
            base = (i % side) * WIDE * B + p * width
            outs[p] = dot_nn(both_half, sgrad)
            scale = inverse[i // side, :, base : base + width]
            out = (outs[p][:HALF] * scale).astype(bf16)
            mine = jnp.where(x == 0, sgrad[:HALF], sgrad[HALF:])
            own = jnp.where(x == 0, hidden[p][:HALF], hidden[p][HALF:])
            fine = mine.astype(f32)
            for v in range(4):
                bias_sum = bias_sum + fine[:, v * HALF : (v + 1) * HALF]
            for b in range(2):
                lanes = slice(b * B, (b + 1) * B)
                n = i * WIDE + 2 * p + b
                sums[at + 2 * p + b] = out[:, lanes]
                self_back[n] = outs[p][HALF:, lanes]
                sage[n] = mine[:, lanes]
                hid[n] = own[:, lanes]
                lgrad[n] = grad[p][:, lanes]
        if i == 0:
            pl.semaphore_wait(barrier, 1)
        exchange(i, k).start()

    weight_grads(steps - 1)
    bias_grad[...] = bias_sum
    stats[...] = jnp.concatenate([loss_rows, valid_rows, jnp.zeros((6, width), f32)], axis=0)
    for i in range(steps):
        exchange(i, 1 - k).wait_recv()
        exchange(i, k).wait_send()


def backward_kernel(lists, tiles, sums, self_back, fbuf, table, wtrans, enc_grad, bias_grad, acc):
    x = lax.axis_index("col") // 2
    local = self_back.shape[0]
    blocks = local // 2

    def use(j):
        acc[lists[4, j]] += dot_nn(sums[lists[5, j]], tiles[lists[3, j]])

    def clear(i, c):
        acc[i] = jnp.zeros((HALF, B), f32)
        return c

    lax.fori_loop(0, local + 1, clear, 0)
    each_tile(lists[7, 0], use)
    half = pl.ds(pl.multiple_of(x * HALF, HALF), HALF)
    wide = column_of(table[PROWS - 2 : PROWS + 14, half], 0)
    wide = jnp.concatenate([wide, wide], axis=1)
    weight = wtrans[0, half]
    eg = bg = None
    for b in range(local):
        piece = fbuf[b // blocks, (b % blocks) * B : (b % blocks + 1) * B]
        pre = dot_nt(weight, piece) + wide
        sig = sigmoid(pre)
        grad = ((self_back[b] + acc[b]) * (sig * (1.0 + pre * (1.0 - sig)))).astype(bf16)
        t1 = dot_nn(grad, piece)
        gf = grad.astype(f32)
        t2 = gf[:, :HALF] + gf[:, HALF:]
        eg = t1 if eg is None else eg + t1
        bg = t2 if bg is None else bg + t2
    enc_grad[...] = eg
    bias_grad[...] = bg


def reduce_kernel(
    ng,
    enc_grad,
    benc_grad,
    self_grad,
    neigh_grad,
    head_grad,
    bsage_grad,
    srow,
    stats,
    slot_grad,
    loss,
    gtab,
    rtab,
    qbuf,
    inbox,
    sbuf,
    srecv,
    sbox,
    up,
    down,
    core_sem,
    stat_sem,
    g_send,
    g_recv,
    s_send,
    s_recv,
):
    g, q, k, x, partner, across = place()
    entered = enter(ng, g, q, (partner,))
    sp = inbox.shape[1]
    slots = ng * sp

    both = jnp.sum(stats[...], axis=1, keepdims=True)
    sbuf[...] = jnp.broadcast_to(both, sbuf.shape)
    gtab[0:B] = jnp.transpose(enc_grad[...]).astype(bf16)
    gtab[B : 2 * B] = jnp.transpose(self_grad[...]).astype(bf16)
    gtab[2 * B : 3 * B] = jnp.transpose(neigh_grad[...]).astype(bf16)
    gtab[3 * B : 3 * B + CLS] = head_grad[...].astype(bf16)
    tail = lax.broadcasted_iota(jnp.int32, (16, HALF), 0)
    row_one = jnp.sum(jnp.transpose(benc_grad[...]), axis=0, keepdims=True)
    row_two = jnp.sum(jnp.transpose(bsage_grad[...]), axis=0, keepdims=True)
    last = jnp.where(tail == 0, row_one, jnp.where(tail == 1, row_two, 0.0))
    gtab[PROWS - 2 : PROWS + 14] = last.astype(bf16)
    entered()
    one = remote(gtab, rtab, core_sem.at[0], core_sem.at[1], (g, partner))
    one.start()
    two = remote(sbuf, srecv, stat_sem.at[0], stat_sem.at[1], (g, partner))
    two.start()
    all_in(ng, g, q, up, down)
    one.wait()
    two.wait()
    sbox[g] = sbuf[...] + srecv[...]

    def stat_out(d):
        to = (g + d) % ng
        return remote(sbox.at[g], sbox.at[g], s_send.at[d], s_recv.at[d], (to, q))

    def stat_got(d):
        src = (g + ng - d) % ng
        return remote(sbox.at[src], sbox.at[src], s_send.at[d], s_recv.at[d], (src, q))

    def start_stat(d, c):
        stat_out(d).start()
        return c

    lax.fori_loop(1, ng, start_stat, 0)

    whole = gtab[...].astype(f32) + rtab[...].astype(f32)
    rolled = pltpu.roll(whole, HALF // 2, 1)
    low = lax.broadcasted_iota(jnp.int32, (TROWS, HALF), 1) < HALF // 2
    line = lax.broadcasted_iota(jnp.int32, (TROWS, slots), 0)
    even = jnp.where(low, jnp.where(k == 0, whole, rolled), 0.0).astype(bf16)
    odd = jnp.where(low, 0.0, jnp.where(k == 0, rolled, whole)).astype(bf16)
    hot_even = (line == srow[:, :slots]).astype(f32).astype(bf16)
    hot_odd = (line == srow[:, slots:]).astype(f32).astype(bf16)
    spread = dot_tn(hot_even, even) + dot_tn(hot_odd, odd)
    qbuf[...] = spread.astype(bf16).reshape(ng, sp, HALF)

    def out(d):
        to = (g + d) % ng
        return remote(qbuf.at[to], inbox.at[g], g_send.at[d], g_recv.at[d], (to, q))

    def got(d):
        src = (g + ng - d) % ng
        return remote(qbuf.at[src], inbox.at[src], g_send.at[d], g_recv.at[d], (src, q))

    def start(d, c):
        out(d).start()
        return c

    lax.fori_loop(1, ng, start, 0)
    inbox[g] = qbuf[g]

    def arrive(d, c):
        stat_got(d).wait_recv()
        got(d).wait_recv()
        return c

    lax.fori_loop(1, ng, arrive, 0)

    def add_stat(i, c):
        return c + sbox[i]

    sums = lax.fori_loop(0, ng, add_stat, jnp.zeros(sbuf.shape, f32))
    loss_sum = sums[0:1]
    count = sums[1:2]
    loss[...] = jnp.broadcast_to(loss_sum / count, loss.shape)

    def add(i, c):
        return c + inbox[i].astype(f32)

    total = lax.fori_loop(0, ng, add, jnp.zeros((sp, HALF), f32))
    slot_grad[...] = total / count

    def finish(d, c):
        stat_out(d).wait_send()
        out(d).wait_send()
        return c

    lax.fori_loop(1, ng, finish, 0)


def update_kernel(packed, loss, pieces, master, first, second, new_master, new_first, new_second, low, mean_loss):
    g = lax.axis_index("grp")
    slots = pieces.shape[1]
    width = master.shape[1]
    sp = packed.shape[0]
    rows = packed[...]
    if sp < HALF:
        rows = jnp.concatenate([rows, jnp.zeros((HALF - sp, HALF), f32)], axis=0)
    turned = jnp.transpose(rows)
    piece = pieces[pl.ds(g, 1), :]
    owned = piece >= 0
    for j in range(PR):
        grad = turned[j * width : (j + 1) * width, :slots]
        decay = jnp.where(piece * PR + j < PROWS - 2, decay_rate, 0.0)
        old = master[j]
        one = beta_one * first[j] + (1.0 - beta_one) * grad
        two = beta_two * second[j] + (1.0 - beta_two) * grad * grad
        one_hat = one / (1.0 - beta_one**STEP)
        two_hat = two / (1.0 - beta_two**STEP)
        new = old - learn_rate * (one_hat / (jnp.sqrt(two_hat) + adam_epsilon) + decay * old)
        new = jnp.where(owned, new, 0.0)
        new_master[j] = new
        new_first[j] = jnp.where(owned, one, 0.0)
        new_second[j] = jnp.where(owned, two, 0.0)
        low[j] = new.astype(bf16)
    mean_loss[0, 0] = loss[0, 0]


def far(v):
    return pltpu.with_memory_space_constraint(v, pltpu.HBM)


def params(limit, collective=None):
    return pltpu.CompilerParams(
        vmem_limit_bytes=limit << 20, collective_id=collective, has_side_effects=collective is not None
    )


DMA = pltpu.SemaphoreType.DMA


def body(
    features,
    adj_tiles,
    block_pairs,
    tile_count,
    degree,
    labels,
    loss_mask,
    slot_piece,
    master,
    moment_one,
    moment_two,
):
    nc = lax.axis_size("col")
    ng = lax.axis_size("grp")
    rows = features.shape[0]
    blocks = rows // B
    nb = nc * blocks
    local = 2 * blocks
    count = adj_tiles.shape[0]
    tpad = -(-count // HALF) * HALF
    slots = slot_piece.shape[1]
    sp = -(-slots // 16) * 16
    width = master.shape[2]
    master_t = jnp.transpose(master, (1, 2, 0))
    first_t = jnp.transpose(moment_one, (1, 2, 0))
    second_t = jnp.transpose(moment_two, (1, 2, 0))

    tiles, fbuf, enc, table, wtrans, srow, marks, inverse, lists = pl.pallas_call(
        functools.partial(gather_kernel, ng),
        out_shape=(
            pltpu.VMEM((count, B, B), bf16),
            pltpu.VMEM((2, rows, F), bf16),
            pltpu.VMEM((nb, HID, B), bf16),
            pltpu.VMEM((TROWS, HID), bf16),
            pltpu.VMEM((3, HID, HID), bf16),
            pltpu.VMEM((1, 2 * ng * sp), jnp.int32),
            pltpu.VMEM((2, 1, rows), jnp.int32),
            pltpu.VMEM((2, 1, rows), f32),
            pltpu.SMEM((8, tpad), jnp.int32),
        ),
        in_specs=[HBM] * 8 + [SM],
        out_specs=(VM,) * 8 + (SM,),
        scratch_shapes=[
            pltpu.VMEM((PR, width, slots), f32),
            pltpu.VMEM((ng, slots), jnp.int32),
            pltpu.VMEM((1, rows), jnp.int32),
            pltpu.VMEM((1, rows), jnp.int32),
            pltpu.VMEM((1, 2, count), jnp.int32),
            pltpu.VMEM((2, 1, rows), jnp.int32),
            pltpu.VMEM((8, tpad), jnp.int32),
            pltpu.VMEM((2, sp, HALF), bf16),
            pltpu.VMEM((2, sp, HALF), bf16),
            pltpu.VMEM((2, ng, 2, sp, HALF), bf16),
            pltpu.VMEM((TROWS, 2 * ng * sp), bf16),
            pltpu.SemaphoreType.REGULAR,
            pltpu.SemaphoreType.REGULAR,
            DMA,
            DMA,
            DMA,
            DMA((7,)),
            DMA((2,)),
            DMA((2,)),
            DMA((2,)),
            DMA((ng,)),
            DMA((ng,)),
            DMA((ng,)),
            DMA((ng,)),
            DMA((blocks,)),
            DMA((blocks,)),
            DMA((2 * blocks,)),
            DMA((2 * blocks,)),
        ],
        compiler_params=params(6, 0),
        name="gather",
    )(
        far(features),
        far(master_t),
        far(slot_piece),
        far(labels.reshape(1, rows)),
        far(loss_mask.reshape(1, rows)),
        far(jnp.transpose(block_pairs, (0, 2, 1))),
        far(degree.reshape(nc, 1, rows)),
        far(adj_tiles),
        tile_count,
    )

    mean = pl.pallas_call(
        forward_kernel,
        out_shape=pltpu.VMEM((local, HID, B), bf16),
        in_specs=[SM, VM, VM, VM],
        out_specs=VM,
        scratch_shapes=[pltpu.VMEM((local + 1, HID, B), f32)],
        compiler_params=params(7),
        name="forward",
    )(lists, tiles, enc, inverse)

    sums, self_back, self_grad, neigh_grad, head_grad, bsage, stats = pl.pallas_call(
        sage_kernel,
        out_shape=(
            pltpu.VMEM((nb, HALF, B), bf16),
            pltpu.VMEM((local, HALF, B), f32),
            pltpu.VMEM((HALF, HID), f32),
            pltpu.VMEM((HALF, HID), f32),
            pltpu.VMEM((CLS, HALF), f32),
            pltpu.VMEM((HALF, HALF), f32),
            pltpu.VMEM((8, 2 * B), f32),
        ),
        in_specs=[VM] * 6,
        out_specs=(VM,) * 7,
        scratch_shapes=[
            pltpu.VMEM((local, HALF, B), bf16),
            pltpu.VMEM((local, HALF, B), bf16),
            pltpu.VMEM((local, CLS, B), bf16),
            DMA((local // WIDE,)),
            DMA((local // WIDE,)),
        ],
        compiler_params=params(8, 1),
        name="sage",
    )(enc, mean, table, wtrans, marks, inverse)

    enc_grad, benc = pl.pallas_call(
        backward_kernel,
        out_shape=(pltpu.VMEM((HALF, F), f32), pltpu.VMEM((HALF, HALF), f32)),
        in_specs=[SM, VM, VM, VM, VM, VM, VM],
        out_specs=(VM,) * 2,
        scratch_shapes=[pltpu.VMEM((local + 1, HALF, B), f32)],
        compiler_params=params(6),
        name="backward",
    )(lists, tiles, sums, self_back, fbuf, table, wtrans)

    packed, loss = pl.pallas_call(
        functools.partial(reduce_kernel, ng),
        out_shape=(pltpu.VMEM((sp, HALF), f32), pltpu.VMEM((8, HALF), f32)),
        in_specs=[VM] * 8,
        out_specs=(VM,) * 2,
        scratch_shapes=[
            pltpu.VMEM((TROWS, HALF), bf16),
            pltpu.VMEM((TROWS, HALF), bf16),
            pltpu.VMEM((ng, sp, HALF), bf16),
            pltpu.VMEM((ng, sp, HALF), bf16),
            pltpu.VMEM((8, HALF), f32),
            pltpu.VMEM((8, HALF), f32),
            pltpu.VMEM((ng, 8, HALF), f32),
            pltpu.SemaphoreType.REGULAR,
            pltpu.SemaphoreType.REGULAR,
            DMA((2,)),
            DMA((2,)),
            DMA((ng,)),
            DMA((ng,)),
            DMA((ng,)),
            DMA((ng,)),
        ],
        compiler_params=params(12, 2),
        name="reduce",
    )(enc_grad, benc, self_grad, neigh_grad, head_grad, bsage, srow, stats)

    shape = (PR, width, slots)
    new_master, new_first, new_second, low, mean_loss = pl.pallas_call(
        update_kernel,
        out_shape=(sds(shape, f32), sds(shape, f32), sds(shape, f32), sds(shape, bf16), sds((1, 1), f32)),
        in_specs=[VM] * 6,
        out_specs=(VM,) * 4 + (SM,),
        compiler_params=params(4),
        name="update",
    )(packed, loss, slot_piece, master_t, first_t, second_t)

    def back(v):
        return jnp.transpose(v, (2, 0, 1))

    return mean_loss[0, 0], back(new_master), back(new_first), back(new_second), back(low)


def solution(mesh):
    in_specs = (
        P(("grp", "col"), None),
        P("grp", None, None),
        P("grp", None, None),
        P("grp"),
        P("grp"),
        P(("grp", "col")),
        P(("grp", "col")),
        P(),
        P("grp", None, "col"),
        P("grp", None, "col"),
        P("grp", None, "col"),
    )
    out_specs = (
        P(),
        P("grp", None, "col"),
        P("grp", None, "col"),
        P("grp", None, "col"),
        P("grp", None, "col"),
    )
    return jax.shard_map(body, mesh=mesh, in_specs=in_specs, out_specs=out_specs, check_vma=False)
```

```python
import functools
import jax
import jax.numpy as jnp
from jax import lax
from jax.experimental import pallas as pl
from jax.experimental.pallas import tpu as pltpu
from jax.sharding import PartitionSpec as P

F = 256
HID = 256
CLS = 64
B = 256
PR = 2
STEP = 7
PROWS = 834
TROWS = 848
HALF = 128
WIDE = 8

learn_rate = 0.01
beta_one = 0.5
beta_two = 0.5
adam_epsilon = 1e-08
decay_rate = 0.1

f32 = jnp.float32
bf16 = jnp.bfloat16
MESH = pl.DeviceIdType.MESH
VM = pl.BlockSpec(memory_space=pltpu.VMEM)
SM = pl.BlockSpec(memory_space=pltpu.SMEM)
HBM = pl.BlockSpec(memory_space=pltpu.HBM)


def sds(shape, dtype):
    return jax.ShapeDtypeStruct(shape, dtype)


def dot_nn(a, b):
    return lax.dot_general(a, b, (((1,), (0,)), ((), ())), preferred_element_type=f32)


def dot_nt(a, b):
    return lax.dot_general(a, b, (((1,), (1,)), ((), ())), preferred_element_type=f32)


def dot_tn(a, b):
    return lax.dot_general(a, b, (((0,), (0,)), ((), ())), preferred_element_type=f32)


def column_of(rows16, row):
    pick = (lax.broadcasted_iota(jnp.int32, (16, HALF), 0) == row).astype(bf16)
    return dot_tn(rows16, pick)


def place():
    g = lax.axis_index("grp")
    q = lax.axis_index("col")
    k = q % 2
    x = q // 2
    partner = q + 1 - 2 * k
    across = q + 2 - 4 * x
    return g, q, k, x, partner, across


def sigmoid(v):
    return jax.nn.sigmoid(v)


def remote(src, dst, send, recv, dev):
    return pltpu.make_async_remote_copy(
        src_ref=src, dst_ref=dst, send_sem=send, recv_sem=recv, device_id=dev, device_id_type=MESH
    )


def enter(ng, g, q, others):
    barrier = pltpu.get_barrier_semaphore()
    line, last = g // 2, ng // 2 - 1
    for c in others:
        pl.semaphore_signal(barrier, inc=1, device_id=(g, c), device_id_type=MESH)
    pair = g + 1 - 2 * (g % 2)
    pl.semaphore_signal(barrier, inc=1, device_id=(pair, q), device_id_type=MESH)

    @pl.when(line > 0)
    def _():
        pl.semaphore_signal(barrier, inc=1, device_id=(g - 2, q), device_id_type=MESH)

    @pl.when(line < last)
    def _():
        pl.semaphore_signal(barrier, inc=1, device_id=(g + 2, q), device_id_type=MESH)

    ends = jnp.minimum(line, 1) + jnp.minimum(last - line, 1)
    return lambda: pl.semaphore_wait(barrier, len(others) + 1 + ends)


def all_in(ng, g, q, up, down):
    line, last = g // 2, ng // 2 - 1

    @pl.when(line == last)
    def _():
        @pl.when(line > 0)
        def _():
            pl.semaphore_signal(down, inc=1, device_id=(g - 2, q), device_id_type=MESH)

    @pl.when(line > 0)
    def _():
        pl.semaphore_wait(up, 1)

    @pl.when(line < last)
    def _():
        pl.semaphore_signal(up, inc=1, device_id=(g + 2, q), device_id_type=MESH)
        pl.semaphore_wait(down, 1)

        @pl.when(line > 0)
        def _():
            pl.semaphore_signal(down, inc=1, device_id=(g - 2, q), device_id_type=MESH)


def gather_kernel(
    ng,
    feat,
    master,
    pieces,
    labels,
    mask,
    pairs,
    degree,
    adj,
    tcount,
    tiles,
    fbuf,
    enc,
    table,
    wtrans,
    srow,
    marks,
    inverse,
    lists,
    mbuf,
    pcs,
    lab,
    msk,
    prs,
    deg,
    lbuf,
    wmsg,
    pmsg,
    wbuf,
    hot,
    up,
    down,
    local_sem,
    put_sem,
    tile_sem,
    small_sem,
    mark_sem,
    ws_core,
    ws_x,
    ws_send,
    ws_recv,
    wr_send,
    wr_recv,
    xs_send,
    xs_recv,
    en_send,
    en_recv,
):
    g, q, k, x, partner, across = place()
    rows = feat.shape[0]
    blocks = rows // B
    sp = wmsg.shape[1]
    slots = pieces.shape[1]
    count = pairs.shape[2]
    tpad = lists.shape[1]
    width = master.shape[1]

    load = pltpu.make_async_copy(feat, fbuf.at[x], local_sem)
    load.start()
    small = [
        pltpu.make_async_copy(a, b, small_sem.at[i])
        for i, (a, b) in enumerate(
            [
                (master, mbuf),
                (pieces, pcs),
                (labels, lab),
                (mask, msk),
                (pairs, prs),
                (degree.at[k], deg.at[0]),
                (degree.at[2 + k], deg.at[1]),
            ]
        )
    ]
    for copy in small:
        copy.start()

    entered = enter(ng, g, q, (across, partner))
    def cross(i):
        at = pl.ds(pl.multiple_of(i * B, B), B)
        return remote(feat.at[at], fbuf.at[x, at], xs_send.at[i], xs_recv.at[i], (g, across))

    entered()
    cross(0).start()
    cross(1).start()
    for copy in small:
        copy.wait()
    for j in range(PR):
        cols = jnp.concatenate(
            [mbuf[j], jnp.zeros((width, HALF - slots), f32)], axis=1
        )
        turned = jnp.transpose(jnp.concatenate([cols, jnp.zeros_like(cols)], axis=0))
        other = pltpu.roll(turned, width, 1)
        wmsg[j] = jnp.where(k == 0, turned, other)[:sp].astype(bf16)
    first = remote(wmsg, pmsg, ws_core.at[0], ws_core.at[1], (g, partner))
    first.start()
    marks[x] = jnp.where(msk[...] > 0, lab[...], -1)
    mark_copy = remote(marks.at[x], marks.at[x], mark_sem.at[0], mark_sem.at[1], (g, across))
    mark_copy.start()
    first.wait()
    wbuf[k, g, x] = wmsg[k] + pmsg[k]
    second = remote(wbuf.at[k, g, x], wbuf.at[k, g, x], ws_x.at[0], ws_x.at[1], (g, across))
    second.start()

    def cross_all(i, c):
        cross(i).start()
        return c

    lax.fori_loop(2, blocks, cross_all, 0)
    fetch = pltpu.make_async_copy(adj, tiles, tile_sem)
    fetch.start()
    all_in(ng, g, q, up, down)
    second.wait()

    def to_group(d):
        return remote(
            wbuf.at[k, g], wbuf.at[k, g], ws_send.at[d], ws_recv.at[d], ((g + d) % ng, q)
        )

    def from_group(d):
        src = (g + ng - d) % ng
        return remote(wbuf.at[k, src], wbuf.at[k, src], ws_send.at[d], ws_recv.at[d], (src, q))

    def hand_over(d):
        src = (g + ng - d) % ng
        return remote(
            wbuf.at[k, src], wbuf.at[k, src], wr_send.at[d], wr_recv.at[d], (g, partner)
        )

    def handed(d):
        src = (g + ng - d) % ng
        return remote(
            wbuf.at[1 - k, src], wbuf.at[1 - k, src], wr_send.at[d], wr_recv.at[d], (g, partner)
        )

    def send_group(d, c):
        to_group(d).start()
        return c

    lax.fori_loop(1, ng, send_group, 0)
    hand_over(0).start()

    shift = blocks.bit_length() - 1
    fill = jnp.zeros((2, tpad - count), jnp.int32)
    both = jnp.concatenate([prs[0], fill], axis=1)
    rvec = both[0:1]
    cvec = both[1:2]
    tvec = lax.broadcasted_iota(jnp.int32, (1, tpad), 1)
    live = tvec < tcount[0]

    def split(v):
        quarter = lax.shift_right_logical(v, shift)
        local = lax.shift_right_logical(quarter, 1) * blocks + (v & (blocks - 1))
        return (quarter & 1) == k, local

    fmine, frow = split(rvec)
    bmine, bcol = split(cvec)
    diagonal = fmine & live & (rvec == cvec)
    fmine = fmine & live & (rvec != cvec)
    bmine = bmine & live & (rvec != cvec)
    upto = (
        lax.broadcasted_iota(jnp.int32, (tpad, tpad), 0)
        <= lax.broadcasted_iota(jnp.int32, (tpad, tpad), 1)
    ).astype(bf16)
    order = lax.broadcasted_iota(jnp.int32, (tpad, tpad), 0)
    zero = jnp.zeros((1, tpad), jnp.int32)

    def compact(mine, one, two):
        flag = mine.astype(f32)
        seen = dot_nn(jnp.broadcast_to(flag, (8, tpad)).astype(bf16), upto)[0:1].astype(jnp.int32)
        spot = jnp.where(mine, seen - 1, -1)
        chosen = (order == spot).astype(f32).astype(bf16)
        values = jnp.concatenate([tvec, one, two, zero, zero, zero, zero, zero], axis=0)
        packed = dot_nt(values.astype(f32).astype(bf16), chosen).astype(jnp.int32)
        total = jnp.sum(flag, axis=1, keepdims=True).astype(jnp.int32)
        past = tvec >= total
        return packed[0:1], jnp.where(past, 2 * blocks, packed[1:2]), packed[2:3], zero + total

    ft, fr, fc, fn = compact(fmine, frow, cvec)
    bt, bc, br, bn = compact(bmine, bcol, rvec)
    chosen = (order == jnp.where(diagonal, frow, -1)).astype(f32).astype(bf16)
    index = jnp.broadcast_to(tvec.astype(f32), (8, tpad)).astype(bf16)
    first_tile = dot_nt(index, chosen)[0:1].astype(jnp.int32)
    counts = jnp.where(tvec == 0, fn, bn)
    lbuf[...] = jnp.concatenate([ft, fr, fc, bt, bc, br, counts, first_tile], axis=0)
    put = pltpu.make_async_copy(lbuf, lists, put_sem)
    put.start()
    inverse[...] = 1.0 / deg[...].astype(f32)

    lanes = ng * sp
    piece = jnp.concatenate([pcs[...], jnp.full((ng, HALF - slots), -1, jnp.int32)], axis=1)
    high = lax.shift_right_logical(piece + 1, 4).astype(f32).astype(bf16)
    low = ((piece + 1) & 15).astype(f32).astype(bf16)
    lane = lax.broadcasted_iota(jnp.int32, (1, lanes), 1)
    owner = jnp.floor((lane.astype(f32) + 0.5) * (1.0 / sp)).astype(jnp.int32)
    within = lane - owner * sp
    pick = (lax.broadcasted_iota(jnp.int32, (HALF, lanes), 0) == within).astype(f32).astype(bf16)
    wide = dot_nn(high, pick) * 16.0 + dot_nn(low, pick)
    keep = lax.broadcasted_iota(jnp.int32, (ng, lanes), 0) == owner
    flat = jnp.sum(jnp.where(keep, wide, 0.0), axis=0, keepdims=True).astype(jnp.int32) - 1
    line = lax.broadcasted_iota(jnp.int32, (TROWS, lanes), 0)
    for j in range(PR):
        at = jnp.where(flat >= 0, flat * PR + j, -1)
        srow[:, j * lanes : (j + 1) * lanes] = at
        hot[:, j * lanes : (j + 1) * lanes] = (line == at).astype(f32).astype(bf16)

    def pass_on(d, c):
        from_group(d).wait_recv()
        hand_over(d).start()
        return c

    lax.fori_loop(1, ng, pass_on, 0)

    def take(d, c):
        handed(d).wait_recv()
        return c

    lax.fori_loop(0, ng, take, 0)

    left = wbuf[:, :, 0].reshape(2 * ng * sp, HALF)
    right = wbuf[:, :, 1].reshape(2 * ng * sp, HALF)
    full = dot_nn(hot[...], jnp.concatenate([left, right], axis=1))
    table[...] = full.astype(bf16)
    for i in range(3):
        wtrans[i] = jnp.transpose(full[i * B : (i + 1) * B]).astype(bf16)
    bias = column_of(table[PROWS - 2 : PROWS + 14], 0)

    def share(i, core):
        away = i // blocks
        quarter = (x + away * (1 - 2 * x)) * 2 + core
        piece = enc.at[quarter * blocks + i % blocks]
        return remote(piece, piece, en_send.at[i], en_recv.at[i], (g, partner))

    def encode(i, many):
        away = i // blocks
        side = x + away * (1 - 2 * x)
        base = i % blocks
        piece = fbuf[side, pl.ds(pl.multiple_of(base * B, B), many * B)]
        pre = dot_nt(wtrans[0], piece) + jnp.concatenate([bias] * (2 * many), axis=1)
        out = (pre * sigmoid(pre)).astype(bf16)
        at = (side * 2 + k) * blocks + base
        for n in range(many):
            enc[at + n] = out[:, n * B : (n + 1) * B]
        for n in range(many):
            share(i + n, k).start()

    load.wait()

    def own(i, c):
        encode(i * 4, 4)
        return c

    lax.fori_loop(0, blocks // 4, own, 0)

    def crossed(i):
        at = pl.ds(pl.multiple_of(i * B, B), B)
        return remote(feat.at[at], fbuf.at[1 - x, at], xs_send.at[i], xs_recv.at[i], (g, across))

    def far_block(i, c):
        crossed(i).wait_recv()
        encode(blocks + i, 1)
        return c

    lax.fori_loop(0, blocks, far_block, 0)

    def settle(i, c):
        for n in (i, blocks + i):
            share(n, 1 - k).wait_recv()
            share(n, k).wait_send()
        cross(i).wait_send()
        return c

    lax.fori_loop(0, blocks, settle, 0)
    mark_copy.wait()

    def drain_group(d, c):
        to_group(d).wait_send()
        hand_over(d).wait_send()
        return c

    lax.fori_loop(1, ng, drain_group, 0)
    hand_over(0).wait_send()
    put.wait()
    fetch.wait()


def each_tile(count, use):
    done = 0

    def step0(i, c, start=done):
        for u in range(32):
            use(start + i * 32 + u)
        return c

    trips0 = (count - done) // 32
    lax.fori_loop(0, trips0, step0, 0)
    done = done + trips0 * 32

    def step1(i, c, start=done):
        for u in range(16):
            use(start + i * 16 + u)
        return c

    trips1 = (count - done) // 16
    lax.fori_loop(0, trips1, step1, 0)
    done = done + trips1 * 16

    def step2(i, c, start=done):
        for u in range(8):
            use(start + i * 8 + u)
        return c

    trips2 = (count - done + 7) // 8
    lax.fori_loop(0, trips2, step2, 0)
    done = done + trips2 * 8


def forward_kernel(lists, tiles, enc, inverse, mean, acc):
    local = mean.shape[0]
    blocks = local // 2

    def use(j):
        acc[lists[1, j]] += dot_nt(enc[lists[2, j]], tiles[lists[0, j]])

    k = lax.axis_index("col") % 2
    for i in range(local):
        at = (i // blocks) * 2 * blocks + k * blocks + i % blocks
        acc[i] = dot_nt(enc[at], tiles[lists[7, i]])
    each_tile(lists[6, 0], use)

    def finish(i, c):
        scale = inverse[i // blocks, :, pl.ds(pl.multiple_of((i % blocks) * B, B), B)]
        mean[i] = (acc[i] * scale).astype(bf16)
        return c

    lax.fori_loop(0, local, finish, 0)


def sage_kernel(
    enc,
    mean,
    table,
    wtrans,
    marks,
    inverse,
    sums,
    self_back,
    self_grad,
    neigh_grad,
    head_grad,
    bias_grad,
    stats,
    sage,
    hid,
    lgrad,
    send,
    recv,
):
    g, q, k, x, partner, across = place()
    local = mean.shape[0]
    blocks = local // 2
    width = 2 * B
    steps = local // WIDE
    side = steps // 2
    barrier = pltpu.get_barrier_semaphore()
    pl.semaphore_signal(barrier, inc=1, device_id=(g, partner), device_id_type=MESH)
    head = table[F + 2 * HID : F + 2 * HID + CLS]
    bias = column_of(table[PROWS - 2 : PROWS + 14], 1)
    bias = jnp.concatenate([bias] * 4, axis=1)
    both_half = jnp.concatenate(
        [
            table[pl.ds(pl.multiple_of(F + HID + x * HALF, HALF), HALF)],
            table[pl.ds(pl.multiple_of(F + x * HALF, HALF), HALF)],
        ],
        axis=0,
    )

    def slot(i, core):
        return (i // side) * 2 * blocks + core * blocks + (i % side) * WIDE

    def exchange(i, core):
        piece = sums.at[pl.ds(slot(i, core), WIDE)]
        return remote(piece, piece, send.at[i], recv.at[i], (g, partner))

    loss_rows = jnp.zeros((1, width), f32)
    valid_rows = jnp.zeros((1, width), f32)
    bias_sum = jnp.zeros((HALF, HALF), f32)
    parts = range(WIDE // 2)
    grads = []

    def weight_grads(i):
        total = [None, None, None]
        for b in range(WIDE):
            n = i * WIDE + b
            here = (
                dot_nt(sage[n], enc[slot(i, k) + b]),
                dot_nt(sage[n], mean[n]),
                dot_nt(lgrad[n], hid[n]),
            )
            total = [h if t is None else t + h for t, h in zip(total, here)]
        for ref, t in zip((self_grad, neigh_grad, head_grad), total):
            ref[...] = t if i == 0 else ref[...] + t

    for i in range(steps):
        at = slot(i, k)
        pre, sig, hidden, grad = {}, {}, {}, {}
        for p in parts:
            e = jnp.concatenate([enc[at + 2 * p], enc[at + 2 * p + 1]], axis=1)
            n = i * WIDE + 2 * p
            m = jnp.concatenate([mean[n], mean[n + 1]], axis=1)
            pre[p] = dot_nn(wtrans[1], e) + dot_nn(wtrans[2], m) + bias
        for p in parts:
            sig[p] = sigmoid(pre[p])
            hidden[p] = (pre[p] * sig[p]).astype(bf16)
        if i > 0:
            weight_grads(i - 1)
        for p in parts:
            logits = dot_nn(head, hidden[p])
            top = jnp.max(logits, axis=0, keepdims=True)
            expd = jnp.exp(logits - top)
            total = jnp.sum(expd, axis=0, keepdims=True)
            base = (i % side) * WIDE * B + p * width
            mark = marks[i // side, :, base : base + width]
            valid = (mark >= 0).astype(f32)
            hot = lax.broadcasted_iota(jnp.int32, (CLS, width), 0) == mark
            onehot = hot.astype(f32)
            target = jnp.sum(logits * onehot, axis=0, keepdims=True)
            loss_rows = loss_rows + valid * (top + jnp.log(total) - target)
            valid_rows = valid_rows + valid
            grad[p] = ((expd * (1.0 / total) - onehot) * valid).astype(bf16)
        outs = {}
        for p in parts:
            back = dot_tn(head, grad[p]) * (sig[p] * (1.0 + pre[p] * (1.0 - sig[p])))
            sgrad = back.astype(bf16)
            base = (i % side) * WIDE * B + p * width
            outs[p] = dot_nn(both_half, sgrad)
            scale = inverse[i // side, :, base : base + width]
            out = (outs[p][:HALF] * scale).astype(bf16)
            mine = jnp.where(x == 0, sgrad[:HALF], sgrad[HALF:])
            own = jnp.where(x == 0, hidden[p][:HALF], hidden[p][HALF:])
            fine = mine.astype(f32)
            for v in range(4):
                bias_sum = bias_sum + fine[:, v * HALF : (v + 1) * HALF]
            for b in range(2):
                lanes = slice(b * B, (b + 1) * B)
                n = i * WIDE + 2 * p + b
                sums[at + 2 * p + b] = out[:, lanes]
                self_back[n] = outs[p][HALF:, lanes]
                sage[n] = mine[:, lanes]
                hid[n] = own[:, lanes]
                lgrad[n] = grad[p][:, lanes]
        if i == 0:
            pl.semaphore_wait(barrier, 1)
        exchange(i, k).start()

    weight_grads(steps - 1)
    bias_grad[...] = bias_sum
    stats[...] = jnp.concatenate([loss_rows, valid_rows, jnp.zeros((6, width), f32)], axis=0)
    for i in range(steps):
        exchange(i, 1 - k).wait_recv()
        exchange(i, k).wait_send()


def backward_kernel(lists, tiles, sums, self_back, fbuf, table, wtrans, enc_grad, bias_grad, acc):
    x = lax.axis_index("col") // 2
    local = self_back.shape[0]
    blocks = local // 2

    def use(j):
        acc[lists[4, j]] += dot_nn(sums[lists[5, j]], tiles[lists[3, j]])

    k = lax.axis_index("col") % 2
    for i in range(local):
        at = (i // blocks) * 2 * blocks + k * blocks + i % blocks
        acc[i] = dot_nn(sums[at], tiles[lists[7, i]])
    each_tile(lists[6, 1], use)
    half = pl.ds(pl.multiple_of(x * HALF, HALF), HALF)
    wide = column_of(table[PROWS - 2 : PROWS + 14, half], 0)
    wide = jnp.concatenate([wide, wide], axis=1)
    weight = wtrans[0, half]
    eg = bg = None
    for b in range(local):
        piece = fbuf[b // blocks, (b % blocks) * B : (b % blocks + 1) * B]
        pre = dot_nt(weight, piece) + wide
        sig = sigmoid(pre)
        grad = ((self_back[b] + acc[b]) * (sig * (1.0 + pre * (1.0 - sig)))).astype(bf16)
        t1 = dot_nn(grad, piece)
        gf = grad.astype(f32)
        t2 = gf[:, :HALF] + gf[:, HALF:]
        eg = t1 if eg is None else eg + t1
        bg = t2 if bg is None else bg + t2
    enc_grad[...] = eg
    bias_grad[...] = bg


def reduce_kernel(
    ng,
    enc_grad,
    benc_grad,
    self_grad,
    neigh_grad,
    head_grad,
    bsage_grad,
    srow,
    stats,
    slot_grad,
    loss,
    gtab,
    rtab,
    qbuf,
    inbox,
    sbuf,
    srecv,
    sbox,
    up,
    down,
    core_sem,
    stat_sem,
    g_send,
    g_recv,
    s_send,
    s_recv,
):
    g, q, k, x, partner, across = place()
    entered = enter(ng, g, q, (partner,))
    sp = inbox.shape[1]
    slots = ng * sp

    both = jnp.sum(stats[...], axis=1, keepdims=True)
    sbuf[...] = jnp.broadcast_to(both, sbuf.shape)
    gtab[0:B] = jnp.transpose(enc_grad[...]).astype(bf16)
    gtab[B : 2 * B] = jnp.transpose(self_grad[...]).astype(bf16)
    gtab[2 * B : 3 * B] = jnp.transpose(neigh_grad[...]).astype(bf16)
    gtab[3 * B : 3 * B + CLS] = head_grad[...].astype(bf16)
    tail = lax.broadcasted_iota(jnp.int32, (16, HALF), 0)
    row_one = jnp.sum(jnp.transpose(benc_grad[...]), axis=0, keepdims=True)
    row_two = jnp.sum(jnp.transpose(bsage_grad[...]), axis=0, keepdims=True)
    last = jnp.where(tail == 0, row_one, jnp.where(tail == 1, row_two, 0.0))
    gtab[PROWS - 2 : PROWS + 14] = last.astype(bf16)
    entered()
    one = remote(gtab, rtab, core_sem.at[0], core_sem.at[1], (g, partner))
    one.start()
    two = remote(sbuf, srecv, stat_sem.at[0], stat_sem.at[1], (g, partner))
    two.start()
    all_in(ng, g, q, up, down)
    one.wait()
    two.wait()
    sbox[g] = sbuf[...] + srecv[...]

    def stat_out(d):
        to = (g + d) % ng
        return remote(sbox.at[g], sbox.at[g], s_send.at[d], s_recv.at[d], (to, q))

    def stat_got(d):
        src = (g + ng - d) % ng
        return remote(sbox.at[src], sbox.at[src], s_send.at[d], s_recv.at[d], (src, q))

    def start_stat(d, c):
        stat_out(d).start()
        return c

    lax.fori_loop(1, ng, start_stat, 0)

    whole = gtab[...].astype(f32) + rtab[...].astype(f32)
    rolled = pltpu.roll(whole, HALF // 2, 1)
    low = lax.broadcasted_iota(jnp.int32, (TROWS, HALF), 1) < HALF // 2
    line = lax.broadcasted_iota(jnp.int32, (TROWS, slots), 0)
    even = jnp.where(low, jnp.where(k == 0, whole, rolled), 0.0).astype(bf16)
    odd = jnp.where(low, 0.0, jnp.where(k == 0, rolled, whole)).astype(bf16)
    hot_even = (line == srow[:, :slots]).astype(f32).astype(bf16)
    hot_odd = (line == srow[:, slots:]).astype(f32).astype(bf16)
    spread = dot_tn(hot_even, even) + dot_tn(hot_odd, odd)
    qbuf[...] = spread.astype(bf16).reshape(ng, sp, HALF)

    def out(d):
        to = (g + d) % ng
        return remote(qbuf.at[to], inbox.at[g], g_send.at[d], g_recv.at[d], (to, q))

    def got(d):
        src = (g + ng - d) % ng
        return remote(qbuf.at[src], inbox.at[src], g_send.at[d], g_recv.at[d], (src, q))

    def start(d, c):
        out(d).start()
        return c

    lax.fori_loop(1, ng, start, 0)
    inbox[g] = qbuf[g]

    def arrive(d, c):
        stat_got(d).wait_recv()
        got(d).wait_recv()
        return c

    lax.fori_loop(1, ng, arrive, 0)

    def add_stat(i, c):
        return c + sbox[i]

    sums = lax.fori_loop(0, ng, add_stat, jnp.zeros(sbuf.shape, f32))
    loss_sum = sums[0:1]
    count = sums[1:2]
    loss[...] = jnp.broadcast_to(loss_sum / count, loss.shape)

    def add(i, c):
        return c + inbox[i].astype(f32)

    total = lax.fori_loop(0, ng, add, jnp.zeros((sp, HALF), f32))
    slot_grad[...] = total / count

    def finish(d, c):
        stat_out(d).wait_send()
        out(d).wait_send()
        return c

    lax.fori_loop(1, ng, finish, 0)


def update_kernel(packed, loss, pieces, master, first, second, new_master, new_first, new_second, low, mean_loss):
    g = lax.axis_index("grp")
    slots = pieces.shape[1]
    width = master.shape[1]
    sp = packed.shape[0]
    rows = packed[...]
    if sp < HALF:
        rows = jnp.concatenate([rows, jnp.zeros((HALF - sp, HALF), f32)], axis=0)
    turned = jnp.transpose(rows)
    piece = pieces[pl.ds(g, 1), :]
    owned = piece >= 0
    for j in range(PR):
        grad = turned[j * width : (j + 1) * width, :slots]
        decay = jnp.where(piece * PR + j < PROWS - 2, decay_rate, 0.0)
        old = master[j]
        one = beta_one * first[j] + (1.0 - beta_one) * grad
        two = beta_two * second[j] + (1.0 - beta_two) * grad * grad
        one_hat = one / (1.0 - beta_one**STEP)
        two_hat = two / (1.0 - beta_two**STEP)
        new = old - learn_rate * (one_hat / (jnp.sqrt(two_hat) + adam_epsilon) + decay * old)
        new = jnp.where(owned, new, 0.0)
        new_master[j] = new
        new_first[j] = jnp.where(owned, one, 0.0)
        new_second[j] = jnp.where(owned, two, 0.0)
        low[j] = new.astype(bf16)
    mean_loss[0, 0] = loss[0, 0]


def far(v):
    return pltpu.with_memory_space_constraint(v, pltpu.HBM)


def params(limit, collective=None):
    return pltpu.CompilerParams(
        vmem_limit_bytes=limit << 20, collective_id=collective, has_side_effects=collective is not None
    )


DMA = pltpu.SemaphoreType.DMA


def body(
    features,
    adj_tiles,
    block_pairs,
    tile_count,
    degree,
    labels,
    loss_mask,
    slot_piece,
    master,
    moment_one,
    moment_two,
):
    nc = lax.axis_size("col")
    ng = lax.axis_size("grp")
    rows = features.shape[0]
    blocks = rows // B
    nb = nc * blocks
    local = 2 * blocks
    count = adj_tiles.shape[0]
    tpad = -(-count // HALF) * HALF
    slots = slot_piece.shape[1]
    sp = -(-slots // 16) * 16
    width = master.shape[2]
    master_t = jnp.transpose(master, (1, 2, 0))
    first_t = jnp.transpose(moment_one, (1, 2, 0))
    second_t = jnp.transpose(moment_two, (1, 2, 0))

    tiles, fbuf, enc, table, wtrans, srow, marks, inverse, lists = pl.pallas_call(
        functools.partial(gather_kernel, ng),
        out_shape=(
            pltpu.VMEM((count, B, B), bf16),
            pltpu.VMEM((2, rows, F), bf16),
            pltpu.VMEM((nb, HID, B), bf16),
            pltpu.VMEM((TROWS, HID), bf16),
            pltpu.VMEM((3, HID, HID), bf16),
            pltpu.VMEM((1, 2 * ng * sp), jnp.int32),
            pltpu.VMEM((2, 1, rows), jnp.int32),
            pltpu.VMEM((2, 1, rows), f32),
            pltpu.SMEM((8, tpad), jnp.int32),
        ),
        in_specs=[HBM] * 8 + [SM],
        out_specs=(VM,) * 8 + (SM,),
        scratch_shapes=[
            pltpu.VMEM((PR, width, slots), f32),
            pltpu.VMEM((ng, slots), jnp.int32),
            pltpu.VMEM((1, rows), jnp.int32),
            pltpu.VMEM((1, rows), jnp.int32),
            pltpu.VMEM((1, 2, count), jnp.int32),
            pltpu.VMEM((2, 1, rows), jnp.int32),
            pltpu.VMEM((8, tpad), jnp.int32),
            pltpu.VMEM((2, sp, HALF), bf16),
            pltpu.VMEM((2, sp, HALF), bf16),
            pltpu.VMEM((2, ng, 2, sp, HALF), bf16),
            pltpu.VMEM((TROWS, 2 * ng * sp), bf16),
            pltpu.SemaphoreType.REGULAR,
            pltpu.SemaphoreType.REGULAR,
            DMA,
            DMA,
            DMA,
            DMA((7,)),
            DMA((2,)),
            DMA((2,)),
            DMA((2,)),
            DMA((ng,)),
            DMA((ng,)),
            DMA((ng,)),
            DMA((ng,)),
            DMA((blocks,)),
            DMA((blocks,)),
            DMA((2 * blocks,)),
            DMA((2 * blocks,)),
        ],
        compiler_params=params(6, 0),
        name="gather",
    )(
        far(features),
        far(master_t),
        far(slot_piece),
        far(labels.reshape(1, rows)),
        far(loss_mask.reshape(1, rows)),
        far(jnp.transpose(block_pairs, (0, 2, 1))),
        far(degree.reshape(nc, 1, rows)),
        far(adj_tiles),
        tile_count,
    )

    mean = pl.pallas_call(
        forward_kernel,
        out_shape=pltpu.VMEM((local, HID, B), bf16),
        in_specs=[SM, VM, VM, VM],
        out_specs=VM,
        scratch_shapes=[pltpu.VMEM((local + 1, HID, B), f32)],
        compiler_params=params(7),
        name="forward",
    )(lists, tiles, enc, inverse)

    sums, self_back, self_grad, neigh_grad, head_grad, bsage, stats = pl.pallas_call(
        sage_kernel,
        out_shape=(
            pltpu.VMEM((nb, HALF, B), bf16),
            pltpu.VMEM((local, HALF, B), f32),
            pltpu.VMEM((HALF, HID), f32),
            pltpu.VMEM((HALF, HID), f32),
            pltpu.VMEM((CLS, HALF), f32),
            pltpu.VMEM((HALF, HALF), f32),
            pltpu.VMEM((8, 2 * B), f32),
        ),
        in_specs=[VM] * 6,
        out_specs=(VM,) * 7,
        scratch_shapes=[
            pltpu.VMEM((local, HALF, B), bf16),
            pltpu.VMEM((local, HALF, B), bf16),
            pltpu.VMEM((local, CLS, B), bf16),
            DMA((local // WIDE,)),
            DMA((local // WIDE,)),
        ],
        compiler_params=params(8, 1),
        name="sage",
    )(enc, mean, table, wtrans, marks, inverse)

    enc_grad, benc = pl.pallas_call(
        backward_kernel,
        out_shape=(pltpu.VMEM((HALF, F), f32), pltpu.VMEM((HALF, HALF), f32)),
        in_specs=[SM, VM, VM, VM, VM, VM, VM],
        out_specs=(VM,) * 2,
        scratch_shapes=[pltpu.VMEM((local + 1, HALF, B), f32)],
        compiler_params=params(6),
        name="backward",
    )(lists, tiles, sums, self_back, fbuf, table, wtrans)

    packed, loss = pl.pallas_call(
        functools.partial(reduce_kernel, ng),
        out_shape=(pltpu.VMEM((sp, HALF), f32), pltpu.VMEM((8, HALF), f32)),
        in_specs=[VM] * 8,
        out_specs=(VM,) * 2,
        scratch_shapes=[
            pltpu.VMEM((TROWS, HALF), bf16),
            pltpu.VMEM((TROWS, HALF), bf16),
            pltpu.VMEM((ng, sp, HALF), bf16),
            pltpu.VMEM((ng, sp, HALF), bf16),
            pltpu.VMEM((8, HALF), f32),
            pltpu.VMEM((8, HALF), f32),
            pltpu.VMEM((ng, 8, HALF), f32),
            pltpu.SemaphoreType.REGULAR,
            pltpu.SemaphoreType.REGULAR,
            DMA((2,)),
            DMA((2,)),
            DMA((ng,)),
            DMA((ng,)),
            DMA((ng,)),
            DMA((ng,)),
        ],
        compiler_params=params(12, 2),
        name="reduce",
    )(enc_grad, benc, self_grad, neigh_grad, head_grad, bsage, srow, stats)

    shape = (PR, width, slots)
    new_master, new_first, new_second, low, mean_loss = pl.pallas_call(
        update_kernel,
        out_shape=(sds(shape, f32), sds(shape, f32), sds(shape, f32), sds(shape, bf16), sds((1, 1), f32)),
        in_specs=[VM] * 6,
        out_specs=(VM,) * 4 + (SM,),
        compiler_params=params(4),
        name="update",
    )(packed, loss, slot_piece, master_t, first_t, second_t)

    def back(v):
        return jnp.transpose(v, (2, 0, 1))

    return mean_loss[0, 0], back(new_master), back(new_first), back(new_second), back(low)


def solution(mesh):
    in_specs = (
        P(("grp", "col"), None),
        P("grp", None, None),
        P("grp", None, None),
        P("grp"),
        P("grp"),
        P(("grp", "col")),
        P(("grp", "col")),
        P(),
        P("grp", None, "col"),
        P("grp", None, "col"),
        P("grp", None, "col"),
    )
    out_specs = (
        P(),
        P("grp", None, "col"),
        P("grp", None, "col"),
        P("grp", None, "col"),
        P("grp", None, "col"),
    )
    return jax.shard_map(body, mesh=mesh, in_specs=in_specs, out_specs=out_specs, check_vma=False)
```

```python
import functools
import jax
import jax.numpy as jnp
from jax import lax
from jax.experimental import pallas as pl
from jax.experimental.pallas import tpu as pltpu
from jax.sharding import PartitionSpec as P

F = 256
HID = 256
CLS = 64
B = 256
PR = 2
STEP = 7
PROWS = 834
TROWS = 848
HALF = 128
WIDE = 8

learn_rate = 0.01
beta_one = 0.5
beta_two = 0.5
adam_epsilon = 1e-08
decay_rate = 0.1

f32 = jnp.float32
bf16 = jnp.bfloat16
MESH = pl.DeviceIdType.MESH
VM = pl.BlockSpec(memory_space=pltpu.VMEM)
SM = pl.BlockSpec(memory_space=pltpu.SMEM)
HBM = pl.BlockSpec(memory_space=pltpu.HBM)


def sds(shape, dtype):
    return jax.ShapeDtypeStruct(shape, dtype)


def dot_nn(a, b):
    return lax.dot_general(a, b, (((1,), (0,)), ((), ())), preferred_element_type=f32)


def dot_nt(a, b):
    return lax.dot_general(a, b, (((1,), (1,)), ((), ())), preferred_element_type=f32)


def dot_tn(a, b):
    return lax.dot_general(a, b, (((0,), (0,)), ((), ())), preferred_element_type=f32)


def column_of(rows16, row):
    pick = (lax.broadcasted_iota(jnp.int32, (16, HALF), 0) == row).astype(bf16)
    return dot_tn(rows16, pick)


def place():
    g = lax.axis_index("grp")
    q = lax.axis_index("col")
    k = q % 2
    x = q // 2
    partner = q + 1 - 2 * k
    across = q + 2 - 4 * x
    return g, q, k, x, partner, across


def sigmoid(v):
    return jax.nn.sigmoid(v)


def remote(src, dst, send, recv, dev):
    return pltpu.make_async_remote_copy(
        src_ref=src, dst_ref=dst, send_sem=send, recv_sem=recv, device_id=dev, device_id_type=MESH
    )


def enter(ng, g, q, others):
    barrier = pltpu.get_barrier_semaphore()
    line, last = g // 2, ng // 2 - 1
    for c in others:
        pl.semaphore_signal(barrier, inc=1, device_id=(g, c), device_id_type=MESH)
    pair = g + 1 - 2 * (g % 2)
    pl.semaphore_signal(barrier, inc=1, device_id=(pair, q), device_id_type=MESH)

    @pl.when(line > 0)
    def _():
        pl.semaphore_signal(barrier, inc=1, device_id=(g - 2, q), device_id_type=MESH)

    @pl.when(line < last)
    def _():
        pl.semaphore_signal(barrier, inc=1, device_id=(g + 2, q), device_id_type=MESH)

    ends = jnp.minimum(line, 1) + jnp.minimum(last - line, 1)
    return lambda: pl.semaphore_wait(barrier, len(others) + 1 + ends)


def all_in(ng, g, q, up, down):
    line, last = g // 2, ng // 2 - 1

    @pl.when(line == last)
    def _():
        @pl.when(line > 0)
        def _():
            pl.semaphore_signal(down, inc=1, device_id=(g - 2, q), device_id_type=MESH)

    @pl.when(line > 0)
    def _():
        pl.semaphore_wait(up, 1)

    @pl.when(line < last)
    def _():
        pl.semaphore_signal(up, inc=1, device_id=(g + 2, q), device_id_type=MESH)
        pl.semaphore_wait(down, 1)

        @pl.when(line > 0)
        def _():
            pl.semaphore_signal(down, inc=1, device_id=(g - 2, q), device_id_type=MESH)


def gather_kernel(
    ng,
    feat,
    master,
    pieces,
    labels,
    mask,
    pairs,
    degree,
    adj,
    tcount,
    tiles,
    fbuf,
    enc,
    table,
    wtrans,
    srow,
    marks,
    inverse,
    lists,
    mbuf,
    pcs,
    lab,
    msk,
    prs,
    deg,
    lbuf,
    wmsg,
    pmsg,
    wbuf,
    hot,
    up,
    down,
    local_sem,
    put_sem,
    tile_sem,
    small_sem,
    mark_sem,
    ws_core,
    ws_x,
    ws_send,
    ws_recv,
    wr_send,
    wr_recv,
    xs_send,
    xs_recv,
    en_send,
    en_recv,
):
    g, q, k, x, partner, across = place()
    rows = feat.shape[0]
    blocks = rows // B
    sp = wmsg.shape[1]
    slots = pieces.shape[1]
    count = pairs.shape[2]
    tpad = lists.shape[1]
    width = master.shape[1]

    load = pltpu.make_async_copy(feat, fbuf.at[x], local_sem)
    load.start()
    small = [
        pltpu.make_async_copy(a, b, small_sem.at[i])
        for i, (a, b) in enumerate(
            [
                (master, mbuf),
                (pieces, pcs),
                (labels, lab),
                (mask, msk),
                (pairs, prs),
                (degree.at[k], deg.at[0]),
                (degree.at[2 + k], deg.at[1]),
            ]
        )
    ]
    for copy in small:
        copy.start()

    entered = enter(ng, g, q, (across, partner))
    def cross(i):
        at = pl.ds(pl.multiple_of(i * B, B), B)
        return remote(feat.at[at], fbuf.at[x, at], xs_send.at[i], xs_recv.at[i], (g, across))

    entered()
    cross(0).start()
    cross(1).start()
    for copy in small:
        copy.wait()
    for j in range(PR):
        cols = jnp.concatenate(
            [mbuf[j], jnp.zeros((width, HALF - slots), f32)], axis=1
        )
        turned = jnp.transpose(jnp.concatenate([cols, jnp.zeros_like(cols)], axis=0))
        other = pltpu.roll(turned, width, 1)
        wmsg[j] = jnp.where(k == 0, turned, other)[:sp].astype(bf16)
    first = remote(wmsg, pmsg, ws_core.at[0], ws_core.at[1], (g, partner))
    first.start()
    marks[x] = jnp.where(msk[...] > 0, lab[...], -1)
    mark_copy = remote(marks.at[x], marks.at[x], mark_sem.at[0], mark_sem.at[1], (g, across))
    mark_copy.start()
    first.wait()
    wbuf[k, g, x] = wmsg[k] + pmsg[k]
    second = remote(wbuf.at[k, g, x], wbuf.at[k, g, x], ws_x.at[0], ws_x.at[1], (g, across))
    second.start()

    def cross_all(i, c):
        cross(i).start()
        return c

    lax.fori_loop(2, blocks, cross_all, 0)
    fetch = pltpu.make_async_copy(adj, tiles, tile_sem)
    fetch.start()
    all_in(ng, g, q, up, down)
    second.wait()

    def to_group(d):
        return remote(
            wbuf.at[k, g], wbuf.at[k, g], ws_send.at[d], ws_recv.at[d], ((g + d) % ng, q)
        )

    def from_group(d):
        src = (g + ng - d) % ng
        return remote(wbuf.at[k, src], wbuf.at[k, src], ws_send.at[d], ws_recv.at[d], (src, q))

    def hand_over(d):
        src = (g + ng - d) % ng
        return remote(
            wbuf.at[k, src], wbuf.at[k, src], wr_send.at[d], wr_recv.at[d], (g, partner)
        )

    def handed(d):
        src = (g + ng - d) % ng
        return remote(
            wbuf.at[1 - k, src], wbuf.at[1 - k, src], wr_send.at[d], wr_recv.at[d], (g, partner)
        )

    def send_group(d, c):
        to_group(d).start()
        return c

    lax.fori_loop(1, ng, send_group, 0)
    hand_over(0).start()

    shift = blocks.bit_length() - 1
    fill = jnp.zeros((2, tpad - count), jnp.int32)
    both = jnp.concatenate([prs[0], fill], axis=1)
    rvec = both[0:1]
    cvec = both[1:2]
    tvec = lax.broadcasted_iota(jnp.int32, (1, tpad), 1)
    live = tvec < tcount[0]

    def split(v):
        quarter = lax.shift_right_logical(v, shift)
        local = lax.shift_right_logical(quarter, 1) * blocks + (v & (blocks - 1))
        return (quarter & 1) == k, local

    fmine, frow = split(rvec)
    bmine, bcol = split(cvec)
    diagonal = fmine & live & (rvec == cvec)
    fmine = fmine & live & (rvec != cvec)
    bmine = bmine & live & (rvec != cvec)
    upto = (
        lax.broadcasted_iota(jnp.int32, (tpad, tpad), 0)
        <= lax.broadcasted_iota(jnp.int32, (tpad, tpad), 1)
    ).astype(bf16)
    order = lax.broadcasted_iota(jnp.int32, (tpad, tpad), 0)
    zero = jnp.zeros((1, tpad), jnp.int32)

    def compact(mine, one, two):
        flag = mine.astype(f32)
        seen = dot_nn(jnp.broadcast_to(flag, (8, tpad)).astype(bf16), upto)[0:1].astype(jnp.int32)
        spot = jnp.where(mine, seen - 1, -1)
        chosen = (order == spot).astype(f32).astype(bf16)
        values = jnp.concatenate([tvec, one, two, zero, zero, zero, zero, zero], axis=0)
        packed = dot_nt(values.astype(f32).astype(bf16), chosen).astype(jnp.int32)
        total = jnp.sum(flag, axis=1, keepdims=True).astype(jnp.int32)
        past = tvec >= total
        return packed[0:1], jnp.where(past, 2 * blocks, packed[1:2]), packed[2:3], zero + total

    ft, fr, fc, fn = compact(fmine, frow, cvec)
    bt, bc, br, bn = compact(bmine, bcol, rvec)
    chosen = (order == jnp.where(diagonal, frow, -1)).astype(f32).astype(bf16)
    index = jnp.broadcast_to(tvec.astype(f32), (8, tpad)).astype(bf16)
    first_tile = dot_nt(index, chosen)[0:1].astype(jnp.int32)
    counts = jnp.where(tvec == 0, fn, bn)
    lbuf[...] = jnp.concatenate([ft, fr, fc, bt, bc, br, counts, first_tile], axis=0)
    put = pltpu.make_async_copy(lbuf, lists, put_sem)
    put.start()
    inverse[...] = 1.0 / deg[...].astype(f32)

    lanes = ng * sp
    piece = jnp.concatenate([pcs[...], jnp.full((ng, HALF - slots), -1, jnp.int32)], axis=1)
    high = lax.shift_right_logical(piece + 1, 4).astype(f32).astype(bf16)
    low = ((piece + 1) & 15).astype(f32).astype(bf16)
    lane = lax.broadcasted_iota(jnp.int32, (1, lanes), 1)
    owner = jnp.floor((lane.astype(f32) + 0.5) * (1.0 / sp)).astype(jnp.int32)
    within = lane - owner * sp
    pick = (lax.broadcasted_iota(jnp.int32, (HALF, lanes), 0) == within).astype(f32).astype(bf16)
    wide = dot_nn(high, pick) * 16.0 + dot_nn(low, pick)
    keep = lax.broadcasted_iota(jnp.int32, (ng, lanes), 0) == owner
    flat = jnp.sum(jnp.where(keep, wide, 0.0), axis=0, keepdims=True).astype(jnp.int32) - 1
    line = lax.broadcasted_iota(jnp.int32, (TROWS, lanes), 0)
    for j in range(PR):
        at = jnp.where(flat >= 0, flat * PR + j, -1)
        srow[:, j * lanes : (j + 1) * lanes] = at
        hot[:, j * lanes : (j + 1) * lanes] = (line == at).astype(f32).astype(bf16)

    def pass_on(d, c):
        from_group(d).wait_recv()
        hand_over(d).start()
        return c

    lax.fori_loop(1, ng, pass_on, 0)

    def take(d, c):
        handed(d).wait_recv()
        return c

    lax.fori_loop(0, ng, take, 0)

    left = wbuf[:, :, 0].reshape(2 * ng * sp, HALF)
    right = wbuf[:, :, 1].reshape(2 * ng * sp, HALF)
    full = dot_nn(hot[...], jnp.concatenate([left, right], axis=1))
    table[...] = full.astype(bf16)
    for i in range(3):
        wtrans[i] = jnp.transpose(full[i * B : (i + 1) * B]).astype(bf16)
    bias = column_of(table[PROWS - 2 : PROWS + 14], 0)

    def share(i, core):
        away = i // blocks
        quarter = (x + away * (1 - 2 * x)) * 2 + core
        piece = enc.at[quarter * blocks + i % blocks]
        return remote(piece, piece, en_send.at[i], en_recv.at[i], (g, partner))

    def encode(i, many):
        away = i // blocks
        side = x + away * (1 - 2 * x)
        base = i % blocks
        piece = fbuf[side, pl.ds(pl.multiple_of(base * B, B), many * B)]
        pre = dot_nt(wtrans[0], piece) + jnp.concatenate([bias] * (2 * many), axis=1)
        out = (pre * sigmoid(pre)).astype(bf16)
        at = (side * 2 + k) * blocks + base
        for n in range(many):
            enc[at + n] = out[:, n * B : (n + 1) * B]
        for n in range(many):
            share(i + n, k).start()

    load.wait()

    def own(i, c):
        encode(i * 4, 4)
        return c

    lax.fori_loop(0, blocks // 4, own, 0)

    def crossed(i):
        at = pl.ds(pl.multiple_of(i * B, B), B)
        return remote(feat.at[at], fbuf.at[1 - x, at], xs_send.at[i], xs_recv.at[i], (g, across))

    def far_block(i, c):
        crossed(i).wait_recv()
        encode(blocks + i, 1)
        return c

    lax.fori_loop(0, blocks, far_block, 0)

    def settle(i, c):
        for n in (i, blocks + i):
            share(n, 1 - k).wait_recv()
            share(n, k).wait_send()
        cross(i).wait_send()
        return c

    lax.fori_loop(0, blocks, settle, 0)
    mark_copy.wait()

    def drain_group(d, c):
        to_group(d).wait_send()
        hand_over(d).wait_send()
        return c

    lax.fori_loop(1, ng, drain_group, 0)
    hand_over(0).wait_send()
    put.wait()
    fetch.wait()


def each_tile(count, use):
    done = 0

    def step0(i, c, start=done):
        for u in range(32):
            use(start + i * 32 + u)
        return c

    trips0 = (count - done) // 32
    lax.fori_loop(0, trips0, step0, 0)
    done = done + trips0 * 32

    def step1(i, c, start=done):
        for u in range(16):
            use(start + i * 16 + u)
        return c

    trips1 = (count - done) // 16
    lax.fori_loop(0, trips1, step1, 0)
    done = done + trips1 * 16

    def step2(i, c, start=done):
        for u in range(8):
            use(start + i * 8 + u)
        return c

    trips2 = (count - done + 7) // 8
    lax.fori_loop(0, trips2, step2, 0)
    done = done + trips2 * 8


def forward_kernel(lists, tiles, enc, inverse, mean, acc):
    local = mean.shape[0]
    blocks = local // 2

    def use(j):
        acc[lists[1, j]] += dot_nt(enc[lists[2, j]], tiles[lists[0, j]])

    k = lax.axis_index("col") % 2
    for i in range(local):
        at = (i // blocks) * 2 * blocks + k * blocks + i % blocks
        acc[i] = dot_nt(enc[at], tiles[lists[7, i]])
    each_tile(lists[6, 0], use)

    def finish(i, c):
        scale = inverse[i // blocks, :, pl.ds(pl.multiple_of((i % blocks) * B, B), B)]
        mean[i] = (acc[i] * scale).astype(bf16)
        return c

    lax.fori_loop(0, local, finish, 0)


def sage_kernel(
    enc,
    mean,
    table,
    wtrans,
    marks,
    inverse,
    sums,
    self_back,
    self_grad,
    neigh_grad,
    head_grad,
    bias_grad,
    stats,
    sage,
    hid,
    lgrad,
    send,
    recv,
):
    g, q, k, x, partner, across = place()
    local = mean.shape[0]
    blocks = local // 2
    width = 2 * B
    steps = local // WIDE
    side = steps // 2
    barrier = pltpu.get_barrier_semaphore()
    pl.semaphore_signal(barrier, inc=1, device_id=(g, partner), device_id_type=MESH)
    head = table[F + 2 * HID : F + 2 * HID + CLS]
    bias = column_of(table[PROWS - 2 : PROWS + 14], 1)
    bias = jnp.concatenate([bias] * 4, axis=1)
    both_half = jnp.concatenate(
        [
            table[pl.ds(pl.multiple_of(F + HID + x * HALF, HALF), HALF)],
            table[pl.ds(pl.multiple_of(F + x * HALF, HALF), HALF)],
        ],
        axis=0,
    )

    def slot(i, core):
        return (i // side) * 2 * blocks + core * blocks + (i % side) * WIDE

    def exchange(i, core):
        piece = sums.at[pl.ds(slot(i, core), WIDE)]
        return remote(piece, piece, send.at[i], recv.at[i], (g, partner))

    loss_rows = jnp.zeros((1, width), f32)
    valid_rows = jnp.zeros((1, width), f32)
    bias_sum = jnp.zeros((HALF, HALF), f32)
    parts = range(WIDE // 2)
    grads = []

    def weight_grads(i):
        total = [None, None, None]
        for b in range(WIDE):
            n = i * WIDE + b
            here = (
                dot_nt(sage[n], enc[slot(i, k) + b]),
                dot_nt(sage[n], mean[n]),
                dot_nt(lgrad[n], hid[n]),
            )
            total = [h if t is None else t + h for t, h in zip(total, here)]
        for ref, t in zip((self_grad, neigh_grad, head_grad), total):
            ref[...] = t if i == 0 else ref[...] + t

    for i in range(steps):
        at = slot(i, k)
        pre, sig, hidden, grad = {}, {}, {}, {}
        for p in parts:
            e = jnp.concatenate([enc[at + 2 * p], enc[at + 2 * p + 1]], axis=1)
            n = i * WIDE + 2 * p
            m = jnp.concatenate([mean[n], mean[n + 1]], axis=1)
            pre[p] = dot_nn(wtrans[1], e) + dot_nn(wtrans[2], m) + bias
        for p in parts:
            sig[p] = sigmoid(pre[p])
            hidden[p] = (pre[p] * sig[p]).astype(bf16)
        if i > 0:
            weight_grads(i - 1)
        for p in parts:
            logits = dot_nn(head, hidden[p])
            top = jnp.max(logits, axis=0, keepdims=True)
            expd = jnp.exp(logits - top)
            total = jnp.sum(expd, axis=0, keepdims=True)
            base = (i % side) * WIDE * B + p * width
            mark = marks[i // side, :, base : base + width]
            valid = (mark >= 0).astype(f32)
            hot = lax.broadcasted_iota(jnp.int32, (CLS, width), 0) == mark
            onehot = hot.astype(f32)
            target = jnp.sum(logits * onehot, axis=0, keepdims=True)
            loss_rows = loss_rows + valid * (top + jnp.log(total) - target)
            valid_rows = valid_rows + valid
            grad[p] = ((expd * (1.0 / total) - onehot) * valid).astype(bf16)
        outs = {}
        for p in parts:
            back = dot_tn(head, grad[p]) * (sig[p] * (1.0 + pre[p] * (1.0 - sig[p])))
            sgrad = back.astype(bf16)
            base = (i % side) * WIDE * B + p * width
            outs[p] = dot_nn(both_half, sgrad)
            scale = inverse[i // side, :, base : base + width]
            out = (outs[p][:HALF] * scale).astype(bf16)
            mine = jnp.where(x == 0, sgrad[:HALF], sgrad[HALF:])
            own = jnp.where(x == 0, hidden[p][:HALF], hidden[p][HALF:])
            fine = mine.astype(f32)
            for v in range(4):
                bias_sum = bias_sum + fine[:, v * HALF : (v + 1) * HALF]
            for b in range(2):
                lanes = slice(b * B, (b + 1) * B)
                n = i * WIDE + 2 * p + b
                sums[at + 2 * p + b] = out[:, lanes]
                self_back[n] = outs[p][HALF:, lanes]
                sage[n] = mine[:, lanes]
                hid[n] = own[:, lanes]
                lgrad[n] = grad[p][:, lanes]
        if i == 0:
            pl.semaphore_wait(barrier, 1)
        exchange(i, k).start()

    weight_grads(steps - 1)
    bias_grad[...] = bias_sum
    stats[...] = jnp.concatenate([loss_rows, valid_rows, jnp.zeros((6, width), f32)], axis=0)
    for i in range(steps):
        exchange(i, 1 - k).wait_recv()
        exchange(i, k).wait_send()


def backward_kernel(lists, tiles, sums, self_back, fbuf, table, wtrans, enc_grad, bias_grad, acc):
    x = lax.axis_index("col") // 2
    local = self_back.shape[0]
    blocks = local // 2

    def use(j):
        acc[lists[4, j]] += dot_nn(sums[lists[5, j]], tiles[lists[3, j]])

    k = lax.axis_index("col") % 2
    for i in range(local):
        at = (i // blocks) * 2 * blocks + k * blocks + i % blocks
        acc[i] = dot_nn(sums[at], tiles[lists[7, i]])
    each_tile(lists[6, 1], use)
    half = pl.ds(pl.multiple_of(x * HALF, HALF), HALF)
    wide = column_of(table[PROWS - 2 : PROWS + 14, half], 0)
    wide = jnp.concatenate([wide, wide], axis=1)
    weight = wtrans[0, half]
    eg = bg = None
    for b in range(local):
        piece = fbuf[b // blocks, (b % blocks) * B : (b % blocks + 1) * B]
        pre = dot_nt(weight, piece) + wide
        sig = sigmoid(pre)
        grad = ((self_back[b] + acc[b]) * (sig * (1.0 + pre * (1.0 - sig)))).astype(bf16)
        t1 = dot_nn(grad, piece)
        gf = grad.astype(f32)
        t2 = gf[:, :HALF] + gf[:, HALF:]
        eg = t1 if eg is None else eg + t1
        bg = t2 if bg is None else bg + t2
    enc_grad[...] = eg
    bias_grad[...] = bg


def reduce_kernel(
    ng,
    enc_grad,
    benc_grad,
    self_grad,
    neigh_grad,
    head_grad,
    bsage_grad,
    srow,
    stats,
    slot_grad,
    loss,
    gtab,
    rtab,
    qbuf,
    inbox,
    sbuf,
    srecv,
    sbox,
    up,
    down,
    core_sem,
    stat_sem,
    g_send,
    g_recv,
    s_send,
    s_recv,
):
    g, q, k, x, partner, across = place()
    entered = enter(ng, g, q, (partner,))
    sp = inbox.shape[1]
    slots = ng * sp

    both = jnp.sum(stats[...], axis=1, keepdims=True)
    sbuf[...] = jnp.broadcast_to(both, sbuf.shape)
    gtab[0:B] = jnp.transpose(enc_grad[...]).astype(bf16)
    gtab[B : 2 * B] = jnp.transpose(self_grad[...]).astype(bf16)
    gtab[2 * B : 3 * B] = jnp.transpose(neigh_grad[...]).astype(bf16)
    gtab[3 * B : 3 * B + CLS] = head_grad[...].astype(bf16)
    tail = lax.broadcasted_iota(jnp.int32, (16, HALF), 0)
    row_one = jnp.sum(jnp.transpose(benc_grad[...]), axis=0, keepdims=True)
    row_two = jnp.sum(jnp.transpose(bsage_grad[...]), axis=0, keepdims=True)
    last = jnp.where(tail == 0, row_one, jnp.where(tail == 1, row_two, 0.0))
    gtab[PROWS - 2 : PROWS + 14] = last.astype(bf16)
    entered()
    one = remote(gtab, rtab, core_sem.at[0], core_sem.at[1], (g, partner))
    one.start()
    two = remote(sbuf, srecv, stat_sem.at[0], stat_sem.at[1], (g, partner))
    two.start()
    all_in(ng, g, q, up, down)
    one.wait()
    two.wait()
    sbox[g] = sbuf[...] + srecv[...]

    def stat_out(d):
        to = (g + d) % ng
        return remote(sbox.at[g], sbox.at[g], s_send.at[d], s_recv.at[d], (to, q))

    def stat_got(d):
        src = (g + ng - d) % ng
        return remote(sbox.at[src], sbox.at[src], s_send.at[d], s_recv.at[d], (src, q))

    def start_stat(d, c):
        stat_out(d).start()
        return c

    lax.fori_loop(1, ng, start_stat, 0)

    whole = gtab[...].astype(f32) + rtab[...].astype(f32)
    rolled = pltpu.roll(whole, HALF // 2, 1)
    low = lax.broadcasted_iota(jnp.int32, (TROWS, HALF), 1) < HALF // 2
    line = lax.broadcasted_iota(jnp.int32, (TROWS, slots), 0)
    even = jnp.where(low, jnp.where(k == 0, whole, rolled), 0.0).astype(bf16)
    odd = jnp.where(low, 0.0, jnp.where(k == 0, rolled, whole)).astype(bf16)
    hot_even = (line == srow[:, :slots]).astype(f32).astype(bf16)
    hot_odd = (line == srow[:, slots:]).astype(f32).astype(bf16)
    spread = dot_tn(hot_even, even) + dot_tn(hot_odd, odd)
    qbuf[...] = spread.astype(bf16).reshape(ng, sp, HALF)

    def out(d):
        to = (g + d) % ng
        return remote(qbuf.at[to], inbox.at[g], g_send.at[d], g_recv.at[d], (to, q))

    def got(d):
        src = (g + ng - d) % ng
        return remote(qbuf.at[src], inbox.at[src], g_send.at[d], g_recv.at[d], (src, q))

    def start(i, c):
        out(ng // 2 + (i // 2) * (1 - 2 * (i % 2))).start()
        return c

    lax.fori_loop(1, ng, start, 0)
    inbox[g] = qbuf[g]

    def arrive(d, c):
        stat_got(d).wait_recv()
        got(d).wait_recv()
        return c

    lax.fori_loop(1, ng, arrive, 0)

    def add_stat(i, c):
        return c + sbox[i]

    sums = lax.fori_loop(0, ng, add_stat, jnp.zeros(sbuf.shape, f32))
    loss_sum = sums[0:1]
    count = sums[1:2]
    loss[...] = jnp.broadcast_to(loss_sum / count, loss.shape)

    def add(i, c):
        return c + inbox[i].astype(f32)

    total = lax.fori_loop(0, ng, add, jnp.zeros((sp, HALF), f32))
    slot_grad[...] = total / count

    def finish(d, c):
        stat_out(d).wait_send()
        out(d).wait_send()
        return c

    lax.fori_loop(1, ng, finish, 0)


def update_kernel(packed, loss, pieces, master, first, second, new_master, new_first, new_second, low, mean_loss):
    g = lax.axis_index("grp")
    slots = pieces.shape[1]
    width = master.shape[1]
    sp = packed.shape[0]
    rows = packed[...]
    if sp < HALF:
        rows = jnp.concatenate([rows, jnp.zeros((HALF - sp, HALF), f32)], axis=0)
    turned = jnp.transpose(rows)
    piece = pieces[pl.ds(g, 1), :]
    owned = piece >= 0
    for j in range(PR):
        grad = turned[j * width : (j + 1) * width, :slots]
        decay = jnp.where(piece * PR + j < PROWS - 2, decay_rate, 0.0)
        old = master[j]
        one = beta_one * first[j] + (1.0 - beta_one) * grad
        two = beta_two * second[j] + (1.0 - beta_two) * grad * grad
        one_hat = one / (1.0 - beta_one**STEP)
        two_hat = two / (1.0 - beta_two**STEP)
        new = old - learn_rate * (one_hat / (jnp.sqrt(two_hat) + adam_epsilon) + decay * old)
        new = jnp.where(owned, new, 0.0)
        new_master[j] = new
        new_first[j] = jnp.where(owned, one, 0.0)
        new_second[j] = jnp.where(owned, two, 0.0)
        low[j] = new.astype(bf16)
    mean_loss[0, 0] = loss[0, 0]


def far(v):
    return pltpu.with_memory_space_constraint(v, pltpu.HBM)


def params(limit, collective=None):
    return pltpu.CompilerParams(
        vmem_limit_bytes=limit << 20, collective_id=collective, has_side_effects=collective is not None
    )


DMA = pltpu.SemaphoreType.DMA


def body(
    features,
    adj_tiles,
    block_pairs,
    tile_count,
    degree,
    labels,
    loss_mask,
    slot_piece,
    master,
    moment_one,
    moment_two,
):
    nc = lax.axis_size("col")
    ng = lax.axis_size("grp")
    rows = features.shape[0]
    blocks = rows // B
    nb = nc * blocks
    local = 2 * blocks
    count = adj_tiles.shape[0]
    tpad = -(-count // HALF) * HALF
    slots = slot_piece.shape[1]
    sp = -(-slots // 16) * 16
    width = master.shape[2]
    master_t = jnp.transpose(master, (1, 2, 0))
    first_t = jnp.transpose(moment_one, (1, 2, 0))
    second_t = jnp.transpose(moment_two, (1, 2, 0))

    tiles, fbuf, enc, table, wtrans, srow, marks, inverse, lists = pl.pallas_call(
        functools.partial(gather_kernel, ng),
        out_shape=(
            pltpu.VMEM((count, B, B), bf16),
            pltpu.VMEM((2, rows, F), bf16),
            pltpu.VMEM((nb, HID, B), bf16),
            pltpu.VMEM((TROWS, HID), bf16),
            pltpu.VMEM((3, HID, HID), bf16),
            pltpu.VMEM((1, 2 * ng * sp), jnp.int32),
            pltpu.VMEM((2, 1, rows), jnp.int32),
            pltpu.VMEM((2, 1, rows), f32),
            pltpu.SMEM((8, tpad), jnp.int32),
        ),
        in_specs=[HBM] * 8 + [SM],
        out_specs=(VM,) * 8 + (SM,),
        scratch_shapes=[
            pltpu.VMEM((PR, width, slots), f32),
            pltpu.VMEM((ng, slots), jnp.int32),
            pltpu.VMEM((1, rows), jnp.int32),
            pltpu.VMEM((1, rows), jnp.int32),
            pltpu.VMEM((1, 2, count), jnp.int32),
            pltpu.VMEM((2, 1, rows), jnp.int32),
            pltpu.VMEM((8, tpad), jnp.int32),
            pltpu.VMEM((2, sp, HALF), bf16),
            pltpu.VMEM((2, sp, HALF), bf16),
            pltpu.VMEM((2, ng, 2, sp, HALF), bf16),
            pltpu.VMEM((TROWS, 2 * ng * sp), bf16),
            pltpu.SemaphoreType.REGULAR,
            pltpu.SemaphoreType.REGULAR,
            DMA,
            DMA,
            DMA,
            DMA((7,)),
            DMA((2,)),
            DMA((2,)),
            DMA((2,)),
            DMA((ng,)),
            DMA((ng,)),
            DMA((ng,)),
            DMA((ng,)),
            DMA((blocks,)),
            DMA((blocks,)),
            DMA((2 * blocks,)),
            DMA((2 * blocks,)),
        ],
        compiler_params=params(6, 0),
        name="gather",
    )(
        far(features),
        far(master_t),
        far(slot_piece),
        far(labels.reshape(1, rows)),
        far(loss_mask.reshape(1, rows)),
        far(jnp.transpose(block_pairs, (0, 2, 1))),
        far(degree.reshape(nc, 1, rows)),
        far(adj_tiles),
        tile_count,
    )

    mean = pl.pallas_call(
        forward_kernel,
        out_shape=pltpu.VMEM((local, HID, B), bf16),
        in_specs=[SM, VM, VM, VM],
        out_specs=VM,
        scratch_shapes=[pltpu.VMEM((local + 1, HID, B), f32)],
        compiler_params=params(7),
        name="forward",
    )(lists, tiles, enc, inverse)

    sums, self_back, self_grad, neigh_grad, head_grad, bsage, stats = pl.pallas_call(
        sage_kernel,
        out_shape=(
            pltpu.VMEM((nb, HALF, B), bf16),
            pltpu.VMEM((local, HALF, B), f32),
            pltpu.VMEM((HALF, HID), f32),
            pltpu.VMEM((HALF, HID), f32),
            pltpu.VMEM((CLS, HALF), f32),
            pltpu.VMEM((HALF, HALF), f32),
            pltpu.VMEM((8, 2 * B), f32),
        ),
        in_specs=[VM] * 6,
        out_specs=(VM,) * 7,
        scratch_shapes=[
            pltpu.VMEM((local, HALF, B), bf16),
            pltpu.VMEM((local, HALF, B), bf16),
            pltpu.VMEM((local, CLS, B), bf16),
            DMA((local // WIDE,)),
            DMA((local // WIDE,)),
        ],
        compiler_params=params(8, 1),
        name="sage",
    )(enc, mean, table, wtrans, marks, inverse)

    enc_grad, benc = pl.pallas_call(
        backward_kernel,
        out_shape=(pltpu.VMEM((HALF, F), f32), pltpu.VMEM((HALF, HALF), f32)),
        in_specs=[SM, VM, VM, VM, VM, VM, VM],
        out_specs=(VM,) * 2,
        scratch_shapes=[pltpu.VMEM((local + 1, HALF, B), f32)],
        compiler_params=params(6),
        name="backward",
    )(lists, tiles, sums, self_back, fbuf, table, wtrans)

    packed, loss = pl.pallas_call(
        functools.partial(reduce_kernel, ng),
        out_shape=(pltpu.VMEM((sp, HALF), f32), pltpu.VMEM((8, HALF), f32)),
        in_specs=[VM] * 8,
        out_specs=(VM,) * 2,
        scratch_shapes=[
            pltpu.VMEM((TROWS, HALF), bf16),
            pltpu.VMEM((TROWS, HALF), bf16),
            pltpu.VMEM((ng, sp, HALF), bf16),
            pltpu.VMEM((ng, sp, HALF), bf16),
            pltpu.VMEM((8, HALF), f32),
            pltpu.VMEM((8, HALF), f32),
            pltpu.VMEM((ng, 8, HALF), f32),
            pltpu.SemaphoreType.REGULAR,
            pltpu.SemaphoreType.REGULAR,
            DMA((2,)),
            DMA((2,)),
            DMA((ng,)),
            DMA((ng,)),
            DMA((ng,)),
            DMA((ng,)),
        ],
        compiler_params=params(12, 2),
        name="reduce",
    )(enc_grad, benc, self_grad, neigh_grad, head_grad, bsage, srow, stats)

    shape = (PR, width, slots)
    new_master, new_first, new_second, low, mean_loss = pl.pallas_call(
        update_kernel,
        out_shape=(sds(shape, f32), sds(shape, f32), sds(shape, f32), sds(shape, bf16), sds((1, 1), f32)),
        in_specs=[VM] * 6,
        out_specs=(VM,) * 4 + (SM,),
        compiler_params=params(4),
        name="update",
    )(packed, loss, slot_piece, master_t, first_t, second_t)

    def back(v):
        return jnp.transpose(v, (2, 0, 1))

    return mean_loss[0, 0], back(new_master), back(new_first), back(new_second), back(low)


def solution(mesh):
    in_specs = (
        P(("grp", "col"), None),
        P("grp", None, None),
        P("grp", None, None),
        P("grp"),
        P("grp"),
        P(("grp", "col")),
        P(("grp", "col")),
        P(),
        P("grp", None, "col"),
        P("grp", None, "col"),
        P("grp", None, "col"),
    )
    out_specs = (
        P(),
        P("grp", None, "col"),
        P("grp", None, "col"),
        P("grp", None, "col"),
        P("grp", None, "col"),
    )
    return jax.shard_map(body, mesh=mesh, in_specs=in_specs, out_specs=out_specs, check_vma=False)
```
